32 devices in a mesh: dp: 2 (over x), tp: 4 (over z), cp: 4 (over y, core).
Axes of the slice: x: 2, y: 2, z: 4, core: 2. Of those that a mesh axis runs over, the one named last changes fastest.
Arguments:
- x_suffix: bfloat16 [8192, 4096], P(('dp', 'cp')), parts along dimension 0
- k_prefix: bfloat16 [16384, 8, 128], P(('dp', 'cp'), 'tp'), parts along dimension 0
- v_prefix: bfloat16 [16384, 8, 128], P(('dp', 'cp'), 'tp'), parts along dimension 0
- norm_attn: bfloat16 [4096], replicated
- w_query: bfloat16 [4096, 4096], P(None, 'tp')
- w_key: bfloat16 [4096, 1024], P(None, 'tp')
- w_value: bfloat16 [4096, 1024], P(None, 'tp')
- w_out: bfloat16 [4096, 4096], P('tp')
- norm_mlp: bfloat16 [4096], replicated
- w_gate: bfloat16 [4096, 14336], P(None, 'tp')
- w_up: bfloat16 [4096, 14336], P(None, 'tp')
- w_down: bfloat16 [14336, 4096], P('tp')
Outputs:
- output 1: bfloat16 [8192, 4096], P(('dp', 'cp')), parts along dimension 0
- output 2: bfloat16 [8192, 8, 128], P(('dp', 'cp'), 'tp'), parts along dimension 0
- output 3: bfloat16 [8192, 8, 128], P(('dp', 'cp'), 'tp'), parts along dimension 0
There are 2 independent parts. The reference program is written for one: setup_inputs(seed, part) draws one part's arguments, and reference() takes and returns one part's arrays. A program takes and returns all parts, laid end to end along the dimension named above; an argument that names none is the same for every part.
All inputs are finite; a program needn't handle non-finite values.
Results may differ from the reference program's by a relative error of at most 0.0109479.
Values are sent between devices in bfloat16 or wider.
A program may use at most 1 GiB of HBM per device.

```python
import jax
import jax.numpy as jnp
from jax import lax

D = 4096
HEADS = 32
KV_HEADS = 8
HEAD = 128
FF = 14336
SEQ_GROUPS = 4
PREFIX_DEV = 2048
SUFFIX_BLK = 512

PREFIX = SEQ_GROUPS * PREFIX_DEV
SUFFIX = 2 * SEQ_GROUPS * SUFFIX_BLK
GROUP_RATIO = HEADS // KV_HEADS
ROPE_THETA = 500000.0
NORM_EPS = 1e-5


def setup_inputs(seed: int = 0, part: int = 0) -> dict:
    shared_keys = jax.random.split(jax.random.key(seed), 9)
    part_keys = jax.random.split(jax.random.fold_in(jax.random.key(seed + 1), part), 3)
    out_std = 2.0 * ((PREFIX + SUFFIX // 2) / (HEADS * HEAD)) ** 0.5

    def normal_draw(rng_key, dims, std_dev):
        return (jax.random.normal(rng_key, dims, jnp.float32) * std_dev).astype(jnp.bfloat16)

    def gain_draw(rng_key):
        return jax.random.uniform(rng_key, (D,), jnp.float32, 0.5, 1.5).astype(jnp.bfloat16)

    return {
        'x_suffix': normal_draw(part_keys[0], (SUFFIX, D), 1.0),
        'k_prefix': normal_draw(part_keys[1], (PREFIX, KV_HEADS, HEAD), 1.0),
        'v_prefix': normal_draw(part_keys[2], (PREFIX, KV_HEADS, HEAD), 1.0),
        'norm_attn': gain_draw(shared_keys[0]),
        'w_query': normal_draw(shared_keys[1], (D, HEADS * HEAD), D ** -0.5),
        'w_key': normal_draw(shared_keys[2], (D, KV_HEADS * HEAD), D ** -0.5),
        'w_value': normal_draw(shared_keys[3], (D, KV_HEADS * HEAD), D ** -0.5),
        'w_out': normal_draw(shared_keys[4], (HEADS * HEAD, D), out_std),
        'norm_mlp': gain_draw(shared_keys[5]),
        'w_gate': normal_draw(shared_keys[6], (D, FF), D ** -0.5),
        'w_up': normal_draw(shared_keys[7], (D, FF), D ** -0.5),
        'w_down': normal_draw(shared_keys[8], (FF, D), 2.0 * FF ** -0.5),
    }


def suffix_positions():
    row_ids = jnp.arange(SUFFIX, dtype=jnp.int32)
    owner_dev = row_ids // (2 * SUFFIX_BLK)
    local_row = row_ids % (2 * SUFFIX_BLK)
    blk_idx = jnp.where(local_row < SUFFIX_BLK, owner_dev, 2 * SEQ_GROUPS - 1 - owner_dev)
    return PREFIX + blk_idx * SUFFIX_BLK + local_row % SUFFIX_BLK


def rope_tables(positions):
    inv_freq = ROPE_THETA ** (-jnp.arange(0, HEAD, 2, dtype=jnp.float32) / HEAD)
    angles = positions.astype(jnp.float32)[:, None] * inv_freq[None, :]
    return jnp.cos(angles), jnp.sin(angles)


def apply_rope(values, cos_tab, sin_tab):
    half_dim = HEAD // 2
    first_half = values[..., :half_dim]
    second_half = values[..., half_dim:]
    cos_rows = cos_tab[:, None, :]
    sin_rows = sin_tab[:, None, :]
    return jnp.concatenate([first_half * cos_rows - second_half * sin_rows, second_half * cos_rows + first_half * sin_rows], axis=-1)


def rms_norm(values, gain_vec):
    vals32 = values.astype(jnp.float32)
    inv_rms = lax.rsqrt(jnp.mean(vals32 * vals32, axis=-1, keepdims=True) + NORM_EPS)
    return (vals32 * inv_rms * gain_vec.astype(jnp.float32)).astype(jnp.bfloat16)


def reference(x_suffix, k_prefix, v_prefix, norm_attn, w_query, w_key, w_value, w_out, norm_mlp, w_gate, w_up, w_down):
    positions = suffix_positions()
    cos_tab, sin_tab = rope_tables(positions)
    hidden = rms_norm(x_suffix, norm_attn)
    q_proj = jnp.dot(hidden, w_query, preferred_element_type=jnp.float32).reshape(SUFFIX, HEADS, HEAD)
    q_rot = apply_rope(q_proj, cos_tab, sin_tab).astype(jnp.bfloat16)
    k_proj = jnp.dot(hidden, w_key, preferred_element_type=jnp.float32).reshape(SUFFIX, KV_HEADS, HEAD)
    k_suffix = apply_rope(k_proj, cos_tab, sin_tab).astype(jnp.bfloat16)
    v_suffix = jnp.dot(hidden, w_value, preferred_element_type=jnp.float32).astype(jnp.bfloat16).reshape(SUFFIX, KV_HEADS, HEAD)
    keys_all = jnp.moveaxis(jnp.concatenate([k_prefix, k_suffix], axis=0), 1, 0)
    vals_all = jnp.moveaxis(jnp.concatenate([v_prefix, v_suffix], axis=0), 1, 0)
    key_pos = jnp.concatenate([jnp.arange(PREFIX, dtype=jnp.int32), positions])
    q_blocks = jnp.moveaxis(q_rot.reshape(2 * SEQ_GROUPS, SUFFIX_BLK, KV_HEADS, GROUP_RATIO, HEAD), 2, 1)
    pos_blocks = positions.reshape(2 * SEQ_GROUPS, SUFFIX_BLK)
    score_scale = HEAD ** -0.5

    def attend_block(blk_args):
        q_blk, q_pos = blk_args
        visible = (key_pos[None, :] <= q_pos[:, None])[:, None, :]

        def attend_head(head_args):
            q_head, k_head, v_head = head_args
            scores = jnp.einsum('brd,kd->brk', q_head.astype(jnp.float32), k_head.astype(jnp.float32)) * score_scale
            scores = jnp.where(visible, scores, -jnp.inf)
            row_max = jnp.max(scores, axis=-1, keepdims=True)
            weights = jnp.exp(scores - row_max)
            denom_sum = jnp.sum(weights, axis=-1, keepdims=True)
            numer_sum = jnp.einsum('brk,kd->brd', weights.astype(jnp.bfloat16).astype(jnp.float32), v_head.astype(jnp.float32))
            return (numer_sum / denom_sum).astype(jnp.bfloat16)

        return lax.map(attend_head, (q_blk, keys_all, vals_all))

    attn_heads = lax.map(attend_block, (q_blocks, pos_blocks))
    attn_heads = jnp.moveaxis(attn_heads, 1, 2).reshape(SUFFIX, HEADS * HEAD)
    resid_mid = x_suffix.astype(jnp.float32) + jnp.dot(attn_heads, w_out, preferred_element_type=jnp.float32)
    hidden_mlp = rms_norm(resid_mid, norm_mlp)
    gate_proj = jnp.dot(hidden_mlp, w_gate, preferred_element_type=jnp.float32)
    up_proj = jnp.dot(hidden_mlp, w_up, preferred_element_type=jnp.float32)
    act_mid = (jax.nn.silu(gate_proj) * up_proj).astype(jnp.bfloat16)
    x_out = (resid_mid + jnp.dot(act_mid, w_down, preferred_element_type=jnp.float32)).astype(jnp.bfloat16)
    return (x_out, k_suffix, v_suffix)
```

```python
import functools
import math

import jax
import jax.numpy as jnp
from jax import lax
from jax.experimental import pallas as pl
from jax.experimental.pallas import tpu as pltpu
from jax.sharding import PartitionSpec as P

ROPE_THETA = 500000.0
NORM_EPS = 1e-5
F32 = jnp.float32
BF16 = jnp.bfloat16
ANY = pl.BlockSpec(memory_space=pl.ANY)
VMEM = pl.BlockSpec(memory_space=pltpu.VMEM)
NT = (((1,), (1,)), ((), ()))


def block_positions(owner, groups, blk_len, prefix_len):
    local_row = jnp.arange(2 * blk_len, dtype=jnp.int32)
    blk_idx = jnp.where(local_row < blk_len, owner, 2 * groups - 1 - owner)
    return prefix_len + blk_idx * blk_len + local_row % blk_len


def rope_tables(positions, head_dim):
    inv_freq = ROPE_THETA ** (-jnp.arange(0, head_dim, 2, dtype=F32) / head_dim)
    angles = positions.astype(F32)[:, None] * inv_freq[None, :]
    cos_tab, sin_tab = jnp.cos(angles), jnp.sin(angles)
    return jnp.concatenate([cos_tab, cos_tab], axis=1), jnp.concatenate([-sin_tab, sin_tab], axis=1)


def qkv_kernel(x_ref, g_ref, wq_ref, wk_ref, wv_ref, cos_ref, sin_ref, q_ref, k_ref, vt_ref, kf_ref, vf_ref, h_ref, *, nq):
    step = pl.program_id(0)
    rows = x_ref.shape[0]
    rt = 128

    @pl.when(step == 0)
    def _():
        @pl.loop(0, rows // rt)
        def _(i):
            sl = pl.ds(pl.multiple_of(i * rt, rt), rt)
            xv = x_ref[sl, :].astype(F32)
            inv = lax.rsqrt(jnp.mean(xv * xv, axis=-1, keepdims=True) + NORM_EPS)
            h_ref[sl, :] = (xv * inv * g_ref[...].astype(F32)).astype(BF16)

    def rope(block, sl):
        return (block * cos_ref[sl, :] + pltpu.roll(block, 64, axis=1) * sin_ref[sl, :]).astype(BF16)

    mt = 512

    def project(w_ref, store):
        @pl.loop(0, rows // mt)
        def _(i):
            sl = pl.ds(pl.multiple_of(i * mt, mt), mt)
            acc = jnp.dot(h_ref[sl, :], w_ref[...], preferred_element_type=F32)
            store(acc, sl)

    def store_q(acc, sl):
        for t in range(2):
            cs = slice(t * 128, (t + 1) * 128)
            q_ref[sl, cs] = rope(acc[:, cs], sl)

    def store_k(acc, sl):
        for t in range(2):
            cs = slice(t * 128, (t + 1) * 128)
            kv = rope(acc[:, cs], sl)
            k_ref[t, sl, :] = kv
            kf_ref[sl, cs] = kv

    def store_v(acc, sl):
        vf_ref[sl, :] = acc.astype(BF16)
        for t in range(2):
            vt_ref[t, :, sl] = acc[:, t * 128:(t + 1) * 128].T.astype(BF16)

    pl.when(step < nq)(lambda: project(wq_ref, store_q))
    pl.when(step == nq)(lambda: project(wk_ref, store_k))
    pl.when(step == nq + 1)(lambda: project(wv_ref, store_v))


def qkv(x, gain, wq, wk, wv, cos_tab, sin_tab):
    rows, depth = x.shape
    nq = wq.shape[1] // 256
    whole = lambda shape: pl.BlockSpec(shape, lambda j: (0,) * len(shape), pipeline_mode=pl.Buffered(1))
    return pl.pallas_call(
        functools.partial(qkv_kernel, nq=nq),
        grid=(nq + 2,),
        in_specs=[
            whole((rows, depth)), whole((1, depth)),
            pl.BlockSpec((depth, 256), lambda j: (0, jnp.minimum(j, nq - 1))),
            pl.BlockSpec((depth, 256), lambda j: (0, 0)),
            pl.BlockSpec((depth, 256), lambda j: (0, 0)),
            whole((rows, 128)), whole((rows, 128)),
        ],
        out_specs=[
            pl.BlockSpec((rows, 256), lambda j: (0, jnp.minimum(j, nq - 1))),
            pl.BlockSpec((2, rows, 128), lambda j: (0, 0, 0)),
            pl.BlockSpec((2, 128, rows), lambda j: (0, 0, 0)),
            pl.BlockSpec((rows, 256), lambda j: (0, 0)),
            pl.BlockSpec((rows, 256), lambda j: (0, 0)),
        ],
        out_shape=[
            jax.ShapeDtypeStruct((rows, nq * 256), BF16),
            jax.ShapeDtypeStruct((2, rows, 128), BF16),
            jax.ShapeDtypeStruct((2, 128, rows), BF16),
            jax.ShapeDtypeStruct((rows, 256), BF16),
            jax.ShapeDtypeStruct((rows, 256), BF16),
        ],
        scratch_shapes=[pltpu.VMEM((rows, depth), BF16)],
        compiler_params=pltpu.CompilerParams(dimension_semantics=("arbitrary",), vmem_limit_bytes=56 * 2**20),
        cost_estimate=pl.CostEstimate(flops=2 * rows * depth * (nq + 2) * 256, bytes_accessed=2 * depth * (rows + 1536), transcendentals=0),
        name="qkv",
    )(x, gain.reshape(1, depth), wq, wk, wv, cos_tab, sin_tab)


NQ = 512


def fetch_pieces(refs, bufs, sems, start):
    for i, (kr, vr) in enumerate(refs):
        n = kr.shape[1]
        for j, (src, dst) in enumerate(((kr, bufs[0].at[:, pl.ds(i * n, n), :]), (vr, bufs[1].at[:, :, pl.ds(i * n, n)]))):
            copy = pltpu.make_async_copy(src, dst, sems.at[i, j])
            copy.start() if start else copy.wait()


def q_block(q_ref, head, half):
    return q_ref[pl.ds(pl.multiple_of(half * NQ, NQ), NQ), pl.ds(pl.multiple_of(head * 128, 128), 128)]


def attend_items(q_ref, kb_ref, vb_ref, acc_ref, m_ref, l_ref, pbufs, n_items, item, bk, c2, diag):
    depth = len(pbufs)

    def scores(i, pb):
        head, half, start = item(i)
        n = head * 2 + half
        ks = kb_ref[head // 4, pl.ds(pl.multiple_of(start, bk), bk), :]
        s = lax.dot_general(ks, q_block(q_ref, head, half), NT, preferred_element_type=F32)
        e = jnp.exp2(s * c2 - m_ref[n])
        if diag:
            seen = lax.broadcasted_iota(jnp.int32, (bk, NQ), 0) <= lax.broadcasted_iota(jnp.int32, (bk, NQ), 1)
            e = jnp.where(seen, e, 0.0)
        pb[...] = e.astype(BF16)
        l_ref[n] += jnp.sum(e.reshape(bk // 8, 8, NQ), axis=0)

    def values(i, pb):
        head, half, start = item(i)
        vt = vb_ref[head // 4, :, pl.ds(pl.multiple_of(start, bk), bk)]
        acc_ref[head * 2 + half] += jnp.dot(vt, pb[...], preferred_element_type=F32)

    scores(0, pbufs[0])

    def body(g, carry):
        for u in range(depth):
            i = g * depth + u
            scores(i + 1, pbufs[(u + 1) % depth])
            values(i, pbufs[u])
        return carry

    trips = n_items // depth - 1
    lax.fori_loop(0, trips, body, 0)
    for u in range(depth):
        if u + 1 < depth:
            scores(trips * depth + u + 1, pbufs[u + 1])
        values(trips * depth + u, pbufs[u])


def prefix_kernel(*refs, first, heads, c2):
    refs = list(refs)
    q_ref, ka, va, kb, vb = refs[:5]
    refs = refs[5:]
    state_in = None
    if not first:
        state_in, refs = refs[:3], refs[3:]
    acc_ref, m_ref, l_ref, kbuf, vbuf, pa, pb, ksem, ssem = refs
    pieces = ((ka, va), (kb, vb))
    fetch_pieces(pieces, (kbuf, vbuf), ksem, True)
    copies = []
    if not first:
        copies = [pltpu.make_async_copy(src, dst, ssem.at[i]) for i, (src, dst) in enumerate(zip(state_in, (acc_ref, m_ref, l_ref)))]
        for copy in copies:
            copy.start()
    fetch_pieces(pieces, (kbuf, vbuf), ksem, False)
    for copy in copies:
        copy.wait()
    if first:
        @pl.loop(0, heads * 2)
        def _(n):
            head, half = n // 2, n % 2
            s = lax.dot_general(kbuf[head // 4, 0:128, :], q_block(q_ref, head, half), NT, preferred_element_type=F32)
            m_ref[n] = jnp.max(s, axis=0, keepdims=True) * c2
            acc_ref[n] = jnp.zeros((128, NQ), F32)
            l_ref[n] = jnp.zeros((8, NQ), F32)
    bk = 1024
    per = kbuf.shape[1] // bk

    def item(i):
        n = i // per
        return n // 2, n % 2, (i % per) * bk

    attend_items(q_ref, kbuf, vbuf, acc_ref, m_ref, l_ref, (pa, pb), heads * 2 * per, item, bk, c2, False)


def state_shapes(heads):
    return [
        jax.ShapeDtypeStruct((heads * 2, 128, NQ), F32),
        jax.ShapeDtypeStruct((heads * 2, 1, NQ), F32),
        jax.ShapeDtypeStruct((heads * 2, 8, NQ), F32),
    ]


def attend_prefix(q, pieces, state, c2):
    heads = q.shape[1] // 128
    n = pieces[0][0].shape[1]
    first = state is None
    flops = 4 * q.shape[0] * heads * 128 * 2 * n
    return pl.pallas_call(
        functools.partial(prefix_kernel, first=first, heads=heads, c2=c2),
        in_specs=[VMEM] + [ANY] * (4 if first else 7),
        out_specs=[VMEM] * 3,
        out_shape=state_shapes(heads),
        scratch_shapes=[
            pltpu.VMEM((2, 2 * n, 128), BF16), pltpu.VMEM((2, 128, 2 * n), BF16),
            pltpu.VMEM((1024, NQ), BF16), pltpu.VMEM((1024, NQ), BF16),
            pltpu.SemaphoreType.DMA((2, 2)), pltpu.SemaphoreType.DMA((3,)),
        ],
        compiler_params=pltpu.CompilerParams(vmem_limit_bytes=40 * 2**20),
        cost_estimate=pl.CostEstimate(flops=flops, bytes_accessed=8 * n * 256 + 8 * q.size, transcendentals=0),
        name="attend_prefix",
    )(q, *pieces[0], *pieces[1], *(() if first else state))


def suffix_kernel(*refs, heads, groups, c2, axis):
    refs = list(refs)
    q_ref = refs[0]
    pre = [(refs[1 + 2 * i], refs[2 + 2 * i]) for i in range(groups)]
    suf = [(refs[1 + 2 * groups + 2 * i], refs[2 + 2 * groups + 2 * i]) for i in range(groups)]
    state_in = refs[1 + 4 * groups:4 + 4 * groups]
    o_ref, kbuf, vbuf, acc_ref, m_ref, l_ref, bad_ref, ksem, ssem, *pbufs = refs[4 + 4 * groups:]
    me = lax.axis_index(axis)
    fetch_pieces(suf, (kbuf, vbuf), ksem, True)
    copies = [pltpu.make_async_copy(src, dst, ssem.at[i]) for i, (src, dst) in enumerate(zip(state_in, (acc_ref, m_ref, l_ref)))]
    for copy in copies:
        copy.start()
    fetch_pieces(suf, (kbuf, vbuf), ksem, False)
    for copy in copies:
        copy.wait()
    bk = NQ
    last = 2 * groups - 1

    def locate(blk):
        late = (blk >= groups).astype(jnp.int32)
        owner = jnp.where(blk < groups, blk, last - blk)
        diff = (owner % 2 != me % 2).astype(jnp.int32) + 2 * (owner // 2 != me // 2).astype(jnp.int32)
        return (diff * 2 + late) * bk

    def full_item(i):
        head, r = i // last, i % last
        half = (r >= me).astype(jnp.int32)
        blk = jnp.where(r < me, r, r - me)
        return head, half, locate(blk)

    def diag_item(i):
        half = i % 2
        return i // 2, half, locate(jnp.where(half == 0, me, last - me))

    attend_items(q_ref, kbuf, vbuf, acc_ref, m_ref, l_ref, pbufs[:4], heads * last, full_item, bk, c2, False)
    attend_items(q_ref, kbuf, vbuf, acc_ref, m_ref, l_ref, pbufs[:2], heads * 2, diag_item, bk, c2, True)

    bad_ref[...] = jnp.zeros_like(bad_ref)

    def write(n, acc, total):
        head, half = n // 2, n % 2
        out = (acc * (1.0 / total)).T.astype(BF16)
        o_ref[pl.ds(pl.multiple_of(half * NQ, NQ), NQ), pl.ds(pl.multiple_of(head * 128, 128), 128)] = out

    @pl.loop(0, heads * 2)
    def _(n):
        acc = acc_ref[n]
        total = jnp.sum(l_ref[n], axis=0, keepdims=True)
        fine = (jnp.abs(acc) < jnp.inf) & (total < jnp.inf)
        bad = jnp.where(fine, 0.0, 1.0)
        for j in range(NQ // 128):
            bad_ref[...] = jnp.maximum(bad_ref[...], jnp.max(bad[:, j * 128:(j + 1) * 128].reshape(16, 8, 128), axis=0))
        write(n, acc, total)

    @pl.when(jnp.max(bad_ref[...]) > 0.0)
    def _():
        n_pre = pre[0][0].shape[1]

        @pl.loop(0, heads * 2)
        def _(n):
            head, half = n // 2, n % 2
            q = q_block(q_ref, head, half)
            m_ref[n] = jnp.full((1, NQ), -jnp.inf, F32)
            l_ref[n] = jnp.zeros((8, NQ), F32)
            acc_ref[n] = jnp.zeros((128, NQ), F32)

            def update(ks, vt, seen):
                s = lax.dot_general(ks, q, NT, preferred_element_type=F32) * c2
                if seen is not None:
                    s = jnp.where(seen, s, -jnp.inf)
                m_old = m_ref[n]
                m_new = jnp.maximum(m_old, jnp.max(s, axis=0, keepdims=True))
                alpha = jnp.exp2(m_old - m_new)
                e = jnp.exp2(s - m_new)
                m_ref[n] = m_new
                l_ref[n] = l_ref[n] * alpha + jnp.sum(e.reshape(bk // 8, 8, NQ), axis=0)
                acc_ref[n] = acc_ref[n] * alpha + jnp.dot(vt, e.astype(BF16), preferred_element_type=F32)

            kpre, vpre = pbufs[0].at[:, 0:128], pbufs[1].at[0:128, :]
            for kr, vr in pre:
                @pl.loop(0, n_pre // bk)
                def _(j):
                    sl = pl.ds(pl.multiple_of(j * bk, bk), bk)
                    c0 = pltpu.make_async_copy(kr.at[head // 4, sl, :], kpre, ksem.at[0, 0])
                    c1 = pltpu.make_async_copy(vr.at[head // 4, :, sl], vpre, ksem.at[0, 1])
                    c0.start()
                    c1.start()
                    c0.wait()
                    c1.wait()
                    update(kpre[...], vpre[...], None)

            mine = jnp.where(half == 0, me, last - me)

            @pl.loop(0, 2 * groups)
            def _(blk):
                @pl.when(blk <= mine)
                def _():
                    start = pl.multiple_of(locate(blk), bk)
                    seen = (lax.broadcasted_iota(jnp.int32, (bk, NQ), 0) <= lax.broadcasted_iota(jnp.int32, (bk, NQ), 1)) | (blk < mine)
                    update(kbuf[head // 4, pl.ds(start, bk), :], vbuf[head // 4, :, pl.ds(start, bk)], seen)

            write(n, acc_ref[n], jnp.sum(l_ref[n], axis=0, keepdims=True))


def attend_suffix(q, pre, suf, state, c2, axis):
    rows = q.shape[0]
    heads, groups = q.shape[1] // 128, len(suf)
    n = suf[0][0].shape[1]
    flat = [a for p in list(pre) + list(suf) for a in p]
    st = state_shapes(heads)
    return pl.pallas_call(
        functools.partial(suffix_kernel, heads=heads, groups=groups, c2=c2, axis=axis),
        in_specs=[VMEM] + [ANY] * (len(flat) + 3),
        out_specs=VMEM,
        out_shape=jax.ShapeDtypeStruct(q.shape, BF16),
        scratch_shapes=[
            pltpu.VMEM((2, groups * n, 128), BF16), pltpu.VMEM((2, 128, groups * n), BF16),
            *(pltpu.VMEM(s.shape, F32) for s in st), pltpu.VMEM((8, 128), F32),
            pltpu.SemaphoreType.DMA((groups, 2)), pltpu.SemaphoreType.DMA((3,)),
            *(pltpu.VMEM((NQ, NQ), BF16) for _ in range(4)),
        ],
        compiler_params=pltpu.CompilerParams(vmem_limit_bytes=40 * 2**20),
        cost_estimate=pl.CostEstimate(flops=4 * heads * 128 * NQ * NQ * (2 * groups + 1), bytes_accessed=8 * n * 512, transcendentals=0),
        name="attend_suffix",
    )(q, *flat, *state)


def swap(arrays, axis, groups, bit):
    return tuple(lax.ppermute(a, axis, [(i, i ^ bit) for i in range(groups)]) for a in arrays)


def attend(q, own_pre, near_pre, far_pre, own_suf, near_suf, far_suf, c2, axis, groups):
    state = attend_prefix(q, (own_pre, near_pre), None, c2)
    far_pre, state = lax.optimization_barrier((far_pre, state))
    cross_pre = swap(far_pre, axis, groups, 1)
    state = attend_prefix(q, (far_pre, cross_pre), state, c2)
    far_suf, state = lax.optimization_barrier((far_suf, state))
    cross_suf = swap(far_suf, axis, groups, 1)
    return attend_suffix(q, (own_pre, near_pre, far_pre, cross_pre), (own_suf, near_suf, far_suf, cross_suf), state, c2, axis)


def solution(mesh):
    groups = mesh.shape['cp']
    tps = mesh.shape['tp']

    def local_layer(x_loc, kp_loc, vp_loc, norm_attn, w_query, w_key, w_value, w_out, norm_mlp, w_gate, w_up, w_down):
        rows = x_loc.shape[0]
        pre_dev, kv_loc, head_dim = kp_loc.shape
        c2 = head_dim ** -0.5 * math.log2(math.e)
        me = lax.axis_index('cp')
        z = lax.axis_index('tp')
        q_pos = block_positions(me, groups, rows // 2, pre_dev * groups)
        cos_tab, sin_tab = rope_tables(q_pos, head_dim)
        own_pre = (kp_loc.transpose(1, 0, 2), vp_loc.transpose(1, 2, 0))
        far_pre, near_pre = swap(own_pre, 'cp', groups, 2), swap(own_pre, 'cp', groups, 1)
        q, k_new, vt_new, k_flat, v_flat = qkv(x_loc, norm_attn, w_query, w_key, w_value, cos_tab, sin_tab)
        own_suf = (k_new, vt_new)
        far_suf, near_suf = swap(own_suf, 'cp', groups, 2), swap(own_suf, 'cp', groups, 1)
        o = attend(q, own_pre, near_pre, far_pre, own_suf, near_suf, far_suf, c2, 'cp', groups)

        n_chunks = 2
        ch = rows // n_chunks
        own = ch // tps
        outs = []
        for c in range(n_chunks):
            part = jnp.dot(o[c * ch:(c + 1) * ch], w_out, preferred_element_type=F32)
            y = lax.psum_scatter(part, 'tp', scatter_dimension=0, tiled=True)
            y = y + lax.dynamic_slice_in_dim(x_loc, c * ch + z * own, own, 0).astype(F32)
            inv = lax.rsqrt(jnp.mean(y * y, axis=-1, keepdims=True) + NORM_EPS)
            h2 = (y * inv * norm_mlp.astype(F32)).astype(BF16)
            h2 = lax.all_gather(h2, 'tp', axis=0, tiled=True)
            gate = jnp.dot(h2, w_gate, preferred_element_type=F32)
            up = jnp.dot(h2, w_up, preferred_element_type=F32)
            act = (jax.nn.silu(gate) * up).astype(BF16)
            part = jnp.dot(act, w_down, preferred_element_type=F32)
            fin = lax.psum_scatter(part, 'tp', scatter_dimension=0, tiled=True)
            outs.append(lax.all_gather((y + fin).astype(BF16), 'tp', axis=0, tiled=True))
        x_out = jnp.concatenate(outs, axis=0)
        return x_out, k_flat.reshape(rows, kv_loc, head_dim), v_flat.reshape(rows, kv_loc, head_dim)

    row_spec = P(('dp', 'cp'), None)
    kv_spec = P(('dp', 'cp'), 'tp', None)
    col_spec = P(None, 'tp')
    row_split = P('tp', None)
    vec_spec = P(None)
    return jax.shard_map(local_layer, mesh=mesh, in_specs=(row_spec, kv_spec, kv_spec, vec_spec, col_spec, col_spec, col_spec, row_split, vec_spec, col_spec, col_spec, row_split), out_specs=(row_spec, kv_spec, kv_spec), check_vma=False)
```

```python
import functools
import math

import jax
import jax.numpy as jnp
from jax import lax
from jax.experimental import pallas as pl
from jax.experimental.pallas import tpu as pltpu
from jax.sharding import PartitionSpec as P


ROPE_THETA = 500000.0
NORM_EPS = 1e-5
F32 = jnp.float32
BF16 = jnp.bfloat16
ANY = pl.BlockSpec(memory_space=pl.ANY)
VMEM = pl.BlockSpec(memory_space=pltpu.VMEM)
LANES = 128
PAIR = 2 * LANES
NT = (((1,), (1,)), ((), ()))
each = functools.partial(pl.loop, 0)


def tile(i, n):
    return pl.ds(pl.multiple_of(i * n, n), n)


def params(mib, **more):
    return pltpu.CompilerParams(vmem_limit_bytes=mib * 2**20, **more)


def cost(flops, moved):
    return pl.CostEstimate(flops=flops, bytes_accessed=moved, transcendentals=0)


def struct(shape, dtype):
    return jax.ShapeDtypeStruct(shape, dtype)


def block_positions(owner, groups, blk_len, prefix_len):
    local_row = jnp.arange(2 * blk_len, dtype=jnp.int32)
    blk_idx = jnp.where(local_row < blk_len, owner, 2 * groups - 1 - owner)
    return prefix_len + blk_idx * blk_len + local_row % blk_len


def rope_tables(positions, head_dim):
    inv_freq = ROPE_THETA ** (-jnp.arange(0, head_dim, 2, dtype=F32) / head_dim)
    angles = positions.astype(F32)[:, None] * inv_freq[None, :]
    cos_tab, sin_tab = jnp.cos(angles), jnp.sin(angles)
    return jnp.concatenate([cos_tab, cos_tab], axis=1), jnp.concatenate([-sin_tab, sin_tab], axis=1)


def qkv_kernel(x_ref, g_ref, wq_ref, wk_ref, wv_ref, cos_ref, sin_ref, q_ref, k_ref, vt_ref, kf_ref, vf_ref, h_ref, *, nq):
    step = pl.program_id(0)
    rows = x_ref.shape[0]
    rt = 128

    @pl.when(step == 0)
    def _():
        @each(rows // rt)
        def _(i):
            sl = tile(i, rt)
            xv = x_ref[sl, :].astype(F32)
            inv = lax.rsqrt(jnp.mean(xv * xv, axis=-1, keepdims=True) + NORM_EPS)
            h_ref[sl, :] = (xv * inv * g_ref[...].astype(F32)).astype(BF16)

    def rope(block, sl):
        return (block * cos_ref[sl, :] + pltpu.roll(block, 64, axis=1) * sin_ref[sl, :]).astype(BF16)

    mt = 512

    def project(w_ref, store):
        @each(rows // mt)
        def _(i):
            sl = tile(i, mt)
            acc = jnp.dot(h_ref[sl, :], w_ref[...], preferred_element_type=F32)
            store(acc, sl)

    def heads_of(acc):
        return [(t, slice(t * LANES, (t + 1) * LANES), acc[:, t * LANES:(t + 1) * LANES]) for t in range(2)]

    def store_q(acc, sl):
        for _, cs, part in heads_of(acc):
            q_ref[sl, cs] = rope(part, sl)

    def store_k(acc, sl):
        for t, cs, part in heads_of(acc):
            kf_ref[sl, cs] = rope(part, sl)
            k_ref[t, sl, :] = kf_ref[sl, cs]

    def store_v(acc, sl):
        vf_ref[sl, :] = acc.astype(BF16)
        for t, _, part in heads_of(acc):
            vt_ref[t, :, sl] = part.T.astype(BF16)

    pl.when(step < nq)(lambda: project(wq_ref, store_q))
    pl.when(step == nq)(lambda: project(wk_ref, store_k))
    pl.when(step == nq + 1)(lambda: project(wv_ref, store_v))


def qkv(x, gain, wq, wk, wv, cos_tab, sin_tab):
    rows, depth = x.shape
    nq = wq.shape[1] // PAIR

    def fixed(shape):
        return pl.BlockSpec(shape, lambda j: tuple(0 for _ in shape))

    def whole(shape):
        return pl.BlockSpec(shape, lambda j: tuple(0 for _ in shape), pipeline_mode=pl.Buffered(1))

    def columns(n):
        return pl.BlockSpec((n, PAIR), lambda j: (0, jnp.minimum(j, nq - 1)))

    flat, by_head, by_head_t = (rows, PAIR), (2, rows, LANES), (2, LANES, rows)
    return pl.pallas_call(
        functools.partial(qkv_kernel, nq=nq),
        grid=(nq + 2,),
        in_specs=[whole(x.shape), whole((1, depth)), columns(depth), fixed(wk.shape), fixed(wv.shape), whole(cos_tab.shape), whole(sin_tab.shape)],
        out_specs=[columns(rows), fixed(by_head), fixed(by_head_t), fixed(flat), fixed(flat)],
        out_shape=[struct(s, BF16) for s in ((rows, nq * PAIR), by_head, by_head_t, flat, flat)],
        scratch_shapes=[pltpu.VMEM((rows, depth), BF16)],
        compiler_params=params(56, dimension_semantics=("arbitrary",)),
        cost_estimate=cost(2 * rows * depth * (nq + 2) * PAIR, 2 * depth * rows),
        name="qkv",
    )(x, gain.reshape(1, depth), wq, wk, wv, cos_tab, sin_tab)


NQ = 512


def fetch_pieces(refs, bufs, sems, start):
    for i, (kr, vr) in enumerate(refs):
        n = kr.shape[1]
        for j, (src, dst) in enumerate(((kr, bufs[0].at[:, pl.ds(i * n, n), :]), (vr, bufs[1].at[:, :, pl.ds(i * n, n)]))):
            copy = pltpu.make_async_copy(src, dst, sems.at[i, j])
            copy.start() if start else copy.wait()


def q_block(q_ref, head, half):
    return q_ref[tile(half, NQ), tile(head, 128)]


def attend_items(q_ref, kb_ref, vb_ref, acc_ref, m_ref, l_ref, pbufs, n_items, item, bk, c2, diag):
    depth = len(pbufs)

    def scores(i, pb):
        head, half, start = item(i)
        n = head * 2 + half
        ks = kb_ref[head // 4, pl.ds(pl.multiple_of(start, bk), bk), :]
        s = lax.dot_general(ks, q_block(q_ref, head, half), NT, preferred_element_type=F32)
        e = jnp.exp2(s * c2 - m_ref[n])
        if diag:
            seen = lax.broadcasted_iota(jnp.int32, (bk, NQ), 0) <= lax.broadcasted_iota(jnp.int32, (bk, NQ), 1)
            e = jnp.where(seen, e, 0.0)
        pb[...] = e.astype(BF16)
        l_ref[n] += jnp.sum(e.reshape(-1, *l_ref.shape[1:]), axis=0)

    def values(i, pb):
        head, half, start = item(i)
        vt = vb_ref[head // 4, :, pl.ds(pl.multiple_of(start, bk), bk)]
        acc_ref[head * 2 + half] += jnp.dot(vt, pb[...], preferred_element_type=F32)

    scores(0, pbufs[0])

    def body(g, carry):
        for u in range(depth):
            i = g * depth + u
            scores(i + 1, pbufs[(u + 1) % depth])
            values(i, pbufs[u])
        return carry

    trips = n_items // depth - 1
    lax.fori_loop(0, trips, body, 0)
    for u in range(depth):
        if u + 1 < depth:
            scores(trips * depth + u + 1, pbufs[u + 1])
        values(trips * depth + u, pbufs[u])


def prefix_kernel(*refs, first, heads, c2):
    refs = list(refs)
    q_ref, ka, va, kb, vb = refs[:5]
    refs = refs[5:]
    state_in, refs = (None, refs) if first else (refs[:3], refs[3:])
    acc_ref, m_ref, l_ref, kbuf, vbuf, pa, pb, ksem, ssem = refs
    pieces = ((ka, va), (kb, vb))
    fetch_pieces(pieces, (kbuf, vbuf), ksem, True)
    copies = []
    if not first:
        copies = [pltpu.make_async_copy(src, dst, ssem.at[i]) for i, (src, dst) in enumerate(zip(state_in, (acc_ref, m_ref, l_ref)))]
        for copy in copies:
            copy.start()
    fetch_pieces(pieces, (kbuf, vbuf), ksem, False)
    for copy in copies:
        copy.wait()
    if first:
        @each(heads * 2)
        def _(n):
            head, half = n // 2, n % 2
            s = lax.dot_general(kbuf[head // 4, tile(0, LANES), :], q_block(q_ref, head, half), NT, preferred_element_type=F32)
            m_ref[n] = jnp.max(s, axis=0, keepdims=True) * c2
            for ref in (acc_ref, l_ref):
                ref[n] = jnp.zeros(ref.shape[1:], F32)
    bk = 2 * NQ
    per = kbuf.shape[1] // bk

    def item(i):
        n = i // per
        return n // 2, n % 2, (i % per) * bk

    attend_items(q_ref, kbuf, vbuf, acc_ref, m_ref, l_ref, (pa, pb), heads * 2 * per, item, bk, c2, False)


def state_shapes(heads):
    return [struct((heads * 2, n, NQ), F32) for n in (LANES, 1, 8)]


def attend_prefix(q, pieces, state, c2):
    heads = q.shape[1] // LANES
    flat = [a for p in pieces for a in p] + list(state or ())
    n = 2 * pieces[0][0].shape[1]
    dma = pltpu.SemaphoreType.DMA
    return pl.pallas_call(
        functools.partial(prefix_kernel, first=state is None, heads=heads, c2=c2),
        in_specs=[VMEM] + [ANY] * len(flat),
        out_specs=[VMEM] * 3,
        out_shape=state_shapes(heads),
        scratch_shapes=[pltpu.VMEM((2, n, LANES), BF16), pltpu.VMEM((2, LANES, n), BF16), *[pltpu.VMEM((2 * NQ, NQ), BF16)] * 2, dma((2, 2)), dma((3,))],
        compiler_params=params(40),
        cost_estimate=cost(4 * q.size * n, 4 * q.size),
        name="attend_prefix",
    )(q, *flat)


def suffix_kernel(*refs, heads, groups, c2, axis):
    q_ref, *refs = refs
    flat, refs = refs[:4 * groups], refs[4 * groups:]
    pairs = list(zip(flat[::2], flat[1::2]))
    pre, suf = pairs[:groups], pairs[groups:]
    *state_in, o_ref, kbuf, vbuf, acc_ref, m_ref, l_ref, bad_ref, ksem, ssem, pa, pb, pc, pd = refs
    pbufs = (pa, pb, pc, pd)
    me = lax.axis_index(axis)
    fetch_pieces(suf, (kbuf, vbuf), ksem, True)
    copies = [pltpu.make_async_copy(src, dst, ssem.at[i]) for i, (src, dst) in enumerate(zip(state_in, (acc_ref, m_ref, l_ref)))]
    for copy in copies:
        copy.start()
    fetch_pieces(suf, (kbuf, vbuf), ksem, False)
    for copy in copies:
        copy.wait()
    bk = NQ
    last = 2 * groups - 1

    def locate(blk):
        late = (blk >= groups).astype(jnp.int32)
        owner = jnp.where(blk < groups, blk, last - blk)
        diff = (owner % 2 != me % 2).astype(jnp.int32) + 2 * (owner // 2 != me // 2).astype(jnp.int32)
        return (diff * 2 + late) * bk

    def full_item(i):
        head, r = i // last, i % last
        half = (r >= me).astype(jnp.int32)
        blk = jnp.where(r < me, r, r - me)
        return head, half, locate(blk)

    def diag_item(i):
        half = i % 2
        return i // 2, half, locate(jnp.where(half == 0, me, last - me))

    attend_items(q_ref, kbuf, vbuf, acc_ref, m_ref, l_ref, pbufs, heads * last, full_item, bk, c2, False)
    attend_items(q_ref, kbuf, vbuf, acc_ref, m_ref, l_ref, (pa, pb), heads * 2, diag_item, bk, c2, True)

    bad_ref[...] = jnp.zeros_like(bad_ref)

    def write(n, acc, total):
        head, half = n // 2, n % 2
        out = (acc * (1.0 / total)).T.astype(BF16)
        o_ref[tile(half, NQ), tile(head, 128)] = out

    @each(heads * 2)
    def _(n):
        acc = acc_ref[n]
        total = jnp.sum(l_ref[n], axis=0, keepdims=True)
        fine = (jnp.abs(acc) < jnp.inf) & (total < jnp.inf)
        bad = jnp.where(fine, 0.0, 1.0)
        for j in range(NQ // LANES):
            part = bad[:, j * LANES:(j + 1) * LANES]
            bad_ref[...] = jnp.maximum(bad_ref[...], jnp.max(part.reshape(-1, *bad_ref.shape), axis=0))
        write(n, acc, total)

    @pl.when(jnp.max(bad_ref[...]) > 0.0)
    def _():
        n_pre = pre[0][0].shape[1]

        @each(heads * 2)
        def _(n):
            head, half = n // 2, n % 2
            q = q_block(q_ref, head, half)
            m_ref[n] = jnp.full((1, NQ), -jnp.inf, F32)
            for ref in (acc_ref, l_ref):
                ref[n] = jnp.zeros(ref.shape[1:], F32)

            def update(ks, vt, seen):
                s = lax.dot_general(ks, q, NT, preferred_element_type=F32) * c2
                if seen is not None:
                    s = jnp.where(seen, s, -jnp.inf)
                m_old = m_ref[n]
                m_new = jnp.maximum(m_old, jnp.max(s, axis=0, keepdims=True))
                alpha = jnp.exp2(m_old - m_new)
                e = jnp.exp2(s - m_new)
                m_ref[n] = m_new
                l_ref[n] = l_ref[n] * alpha + jnp.sum(e.reshape(-1, *l_ref.shape[1:]), axis=0)
                acc_ref[n] = acc_ref[n] * alpha + jnp.dot(vt, e.astype(BF16), preferred_element_type=F32)

            kpre, vpre = pa.at[:, tile(0, LANES)], pb.at[tile(0, LANES), :]
            for kr, vr in pre:
                @each(n_pre // bk)
                def _(j):
                    sl = tile(j, bk)
                    pltpu.sync_copy(kr.at[head // 4, sl, :], kpre)
                    pltpu.sync_copy(vr.at[head // 4, :, sl], vpre)
                    update(kpre[...], vpre[...], None)

            mine = jnp.where(half == 0, me, last - me)

            @each(2 * groups)
            def _(blk):
                @pl.when(blk <= mine)
                def _():
                    start = pl.multiple_of(locate(blk), bk)
                    seen = (lax.broadcasted_iota(jnp.int32, (bk, NQ), 0) <= lax.broadcasted_iota(jnp.int32, (bk, NQ), 1)) | (blk < mine)
                    update(kbuf[head // 4, pl.ds(start, bk), :], vbuf[head // 4, :, pl.ds(start, bk)], seen)

            write(n, acc_ref[n], jnp.sum(l_ref[n], axis=0, keepdims=True))


def attend_suffix(q, pre, suf, state, c2, axis):
    heads, groups = q.shape[1] // LANES, len(suf)
    n = groups * suf[0][0].shape[1]
    flat = [a for p in list(pre) + list(suf) for a in p]
    dma = pltpu.SemaphoreType.DMA
    return pl.pallas_call(
        functools.partial(suffix_kernel, heads=heads, groups=groups, c2=c2, axis=axis),
        in_specs=[VMEM] + [ANY] * (len(flat) + 3),
        out_specs=VMEM,
        out_shape=struct(q.shape, BF16),
        scratch_shapes=[
            pltpu.VMEM((2, n, LANES), BF16), pltpu.VMEM((2, LANES, n), BF16), *(pltpu.VMEM(s.shape, F32) for s in state_shapes(heads)),
            pltpu.VMEM((8, LANES), F32), dma((groups, 2)), dma((3,)), *[pltpu.VMEM((NQ, NQ), BF16)] * 4,
        ],
        compiler_params=params(40),
        cost_estimate=cost(2 * q.size * n, 4 * q.size),
        name="attend_suffix",
    )(q, *flat, *state)


def swap(arrays, axis, groups, bit):
    return tuple(lax.ppermute(a, axis, [(i, i ^ bit) for i in range(groups)]) for a in arrays)


def attend(q, own_pre, near_pre, far_pre, own_suf, near_suf, far_suf, wo_z, wo_x, c2, groups, dps):
    state = attend_prefix(q, (own_pre, near_pre), None, c2)
    far_pre, wo_z, wo_x, state = lax.optimization_barrier((far_pre, wo_z, wo_x, state))
    cross_pre = swap(far_pre, 'cp', groups, 1)
    wo_x = wo_x + swap(wo_z[1:], 'dp', dps, 1)
    state = attend_prefix(q, (far_pre, cross_pre), state, c2)
    far_suf, wo_x, state = lax.optimization_barrier((far_suf, wo_x, state))
    cross_suf = swap(far_suf, 'cp', groups, 1)
    wo_mate = swap(wo_z + wo_x, 'cp', groups, 1)
    o = attend_suffix(q, (own_pre, near_pre, far_pre, cross_pre), (own_suf, near_suf, far_suf, cross_suf), state, c2, 'cp')
    return o, wo_z + wo_x + wo_mate


MESH = pl.DeviceIdType.MESH
ROWS_CH = 256
DOT_N = 512


def side_of(z):
    return lax.div(z, 2)


def colhalf_of(z):
    return lax.rem(lax.div(z + 1, 2), 2)


def line_kernel(o_ref, x_ref, wo_ref, *refs, nc, heads_k):
    wo_pieces, refs = refs[:12], refs[12:]
    wg_ref, wu_ref, wd_ref, gain_ref, xout_ref, land_ref = refs[:6]
    (obuf, h2, ybuf, ring, psum, act, stage, xs, xo, sstat, rstat,
     ring_sem, loc_sem, o_send, o_recv, st_send, st_recv, a1_send, a1_recv, rs_send, rs_recv, a2_send, a2_recv) = refs[6:]
    R, H = ROWS_CH, ROWS_CH // 2
    depth = wg_ref.shape[0]
    ff = wg_ref.shape[1]
    half = depth // 2
    kz = heads_k
    n_ct = half // DOT_N
    nd, ne = ff // PAIR, depth // DOT_N
    per = 4 + nd + ne
    total_loads = nc * per
    big = 1024

    z = lax.axis_index('tp')
    dp = lax.axis_index('dp')
    core = lax.rem(lax.axis_index('cp'), 2)
    side, q = side_of(z), colhalf_of(z)
    is_mid = q == 1
    is_end = q != 1
    near = 1 + side
    outer = 3 * side
    inner = 2 - side
    far_end = 3 - 3 * side
    peers = {1: z + 1 - 2 * lax.rem(z, 2), 2: lax.rem(z + 2, 4), 3: 3 - z}
    mate = peers[1]

    def rdma(src, dst, ssem, rsem, dev):
        return pltpu.make_async_remote_copy(src_ref=src, dst_ref=dst, send_sem=ssem, recv_sem=rsem, device_id={'tp': dev}, device_id_type=MESH)

    def rows_at(zz):
        return tile(side_of(zz), H)

    def cols_at(zz):
        return tile(colhalf_of(zz), half)

    barrier = pltpu.get_barrier_semaphore()
    for d in (1, 2, 3):
        pl.semaphore_signal(barrier, inc=1, device_id={'tp': peers[d]}, device_id_type=MESH)
    pl.semaphore_wait(barrier, 3)

    def load_kind(ld):
        u = ld + (per - 4)
        i1 = lax.div(u, per)
        a = lax.div(i1 + big - 1, big)
        t = lax.rem(u, per) + 4 * lax.div(i1, nc)
        return a * t + (1 - a) * ld

    def issue(ld):
        slot = lax.rem(ld, 3)
        sem = ring_sem.at[slot]
        t = load_kind(ld)

        def start(src, dst):
            pltpu.make_async_copy(src, dst, sem).start()

        for d in range(4):
            @pl.when(t == d)
            def _():
                @each(n_ct)
                def _(ct):
                    c0 = pl.multiple_of(ct * DOT_N, DOT_N)
                    if d == 0:
                        cs = tile(q * n_ct + ct, DOT_N)
                        start(wo_ref.at[:, cs], ring.at[slot, tile(ct, kz), :])
                    else:
                        for dpx in range(2):
                            for cx in range(2):
                                piece = wo_pieces[(dpx + 2 * cx) * 3 + d - 1]
                                n = piece.shape[0]
                                j = (dp + dpx - 2 * dp * dpx) * 2 + (core + cx - 2 * core * cx)
                                r0 = pl.multiple_of(ct * kz + j * n, n)
                                start(piece.at[:, pl.ds(c0, DOT_N)], ring.at[slot, pl.ds(r0, n), :])

        @pl.when((t >= 4) & (t < 4 + nd))
        def _():
            cs = pl.ds(pl.multiple_of((t - 4) * 256, 256), 256)
            start(wg_ref.at[:, cs], ring.at[slot, :depth, :PAIR])
            start(wu_ref.at[:, cs], ring.at[slot, :depth, PAIR:])

        @pl.when(t >= 4 + nd)
        def _():
            cs = pl.ds(pl.multiple_of((t - 4 - nd) * DOT_N, DOT_N), DOT_N)
            start(wd_ref.at[:, cs], ring.at[slot, :ff, :])

    def take(ld, n_rows):
        slot = lax.rem(ld, 3)
        whole = ring.at[slot, :n_rows, :]
        pltpu.make_async_copy(whole, whole, ring_sem.at[slot]).wait()
        pl.when(ld + 2 < total_loads)(lambda: issue(ld + 2))
        return slot

    def o_rows(c, zz):
        return tile(c * 2 + side_of(zz), H)

    def o_copy(c, d):
        return rdma(o_ref.at[o_rows(c, peers[d]), :], obuf.at[c, d], o_send.at[c, d - 1], o_recv.at[c, d - 1], peers[d])

    def o_start(c):
        for d in (1, 2, 3):
            o_copy(c, d).start()

    def project(c, ld0):
        own_o = pltpu.make_async_copy(o_ref.at[o_rows(c, z), :], obuf.at[c, 0], loc_sem.at[0])
        own_x = pltpu.make_async_copy(x_ref.at[o_rows(c, z), cols_at(z)], xs, loc_sem.at[1])
        own_o.start()
        own_x.start()
        for d in (1, 2, 3):
            o_copy(c, d).wait_recv()
        own_o.wait()
        own_x.wait()

        @each(n_ct)
        def _(ct):
            cs = tile(ct, DOT_N)
            ybuf[c, :, cs] = xs[:, cs].astype(F32)

        @each(4)
        def _(d):
            slot = take(ld0 + d, n_ct * kz)

            @each(n_ct)
            def _(ct):
                cs = tile(ct, DOT_N)
                w = ring[slot, tile(ct, kz), :]
                ybuf[c, :, cs] += jnp.dot(obuf[c, d], w, preferred_element_type=F32)

        sstat[c] = jnp.zeros((H, LANES), F32)

        @each(n_ct)
        def _(ct):
            yv = ybuf[c, :, tile(ct, DOT_N)]
            sstat[c] += jnp.broadcast_to(jnp.sum(yv * yv, axis=-1, keepdims=True), (H, LANES))

        swap_stat = rdma(sstat.at[c], rstat.at[c], st_send.at[c, 0], st_recv.at[c, 0], mate)
        swap_stat.start()
        swap_stat.wait_recv()
        inv = lax.rsqrt((sstat[c] + rstat[c])[:, 0:1] * (1.0 / depth) + NORM_EPS)

        @each(n_ct)
        def _(ct):
            cs = tile(ct, DOT_N)
            gs = tile(q * n_ct + ct, DOT_N)
            h2[c, rows_at(z), gs] = (ybuf[c, :, cs] * inv * gain_ref[:, gs].astype(F32)).astype(BF16)

    class Spread:
        def __init__(self, block, send, recv, own=None):
            self.block, self.send, self.recv, self.own = block, send, recv, own

        def copy(self, c, zz, s, r, dev, own=False):
            src = self.own(c) if own and self.own is not None else self.block(c, zz)
            return rdma(src, self.block(c, zz), self.send.at[c, s], self.recv.at[c, r], dev)

        def to_near(self, c):
            return self.copy(c, z, 0, 0, near, own=True)

        def to_outer(self, c):
            return self.copy(c, z, 0, 0, outer, own=True)

        def to_inner(self, c):
            return self.copy(c, z, 1, 1, inner, own=True)

        def end_to_inner(self, c):
            return self.copy(c, outer, 2, 2, inner)

        def inner_to_outer(self, c):
            return self.copy(c, inner, 3, 1, outer)

        def far_to_outer(self, c):
            return self.copy(c, far_end, 4, 2, outer)

        def start(self, c):
            pl.when(is_end)(lambda: self.to_near(c).start())

            @pl.when(is_mid)
            def _():
                self.to_outer(c).start()
                self.to_inner(c).start()

        def wait(self, c, r):
            self.copy(c, z, 0, r, mate).wait_recv()

        def serve1(self, c):
            self.wait(c, 0)
            self.end_to_inner(c).start()
            self.wait(c, 1)
            self.inner_to_outer(c).start()

        def serve2(self, c):
            self.wait(c, 2)
            self.far_to_outer(c).start()

        def drain(self, c):
            @pl.when(is_end)
            def _():
                self.to_near(c).wait_send()

            @pl.when(is_mid)
            def _():
                for copy in (self.to_outer(c), self.to_inner(c), self.end_to_inner(c), self.inner_to_outer(c), self.far_to_outer(c)):
                    copy.wait_send()

    hidden = Spread(lambda c, zz: h2.at[c, rows_at(zz), cols_at(zz)], a1_send, a1_recv)

    def out_block(c, zz):
        return xout_ref.at[tile(c * 2 + side_of(zz), H), cols_at(zz)]

    done = Spread(out_block, a2_send, a2_recv, own=lambda c: xo.at[c])

    def gate_up(c, ld0):
        @each(nd)
        def _(i):
            slot = take(ld0 + i, depth)
            gu = jnp.dot(h2[c], ring[slot, :depth, :], preferred_element_type=F32)
            g, u = gu[:, :PAIR], gu[:, PAIR:]
            a = g * (1.0 / (1.0 + jnp.exp(-g))) * u
            act[:, tile(i, PAIR)] = a.astype(BF16)

    def ps_copy(c, k_send, zz, k_recv, dev):
        return rdma(psum.at[lax.rem(c, 2), zz], land_ref.at[c, k_recv], rs_send.at[c, k_send], rs_recv.at[c, k_recv], dev)

    def sums_out(c):
        ends = (ps_copy(c, 0, far_end, 0, near), ps_copy(c, 1, inner, 2, near), ps_copy(c, 2, near, 3, near))
        mids = (ps_copy(c, 0, far_end, 1, inner), ps_copy(c, 1, outer, 0, outer), ps_copy(c, 2, inner, 4, inner))
        return ends, mids

    def wait_sums_out(c):
        ends, mids = sums_out(c)
        for flag, copies in ((is_end, ends), (is_mid, mids)):
            @pl.when(flag)
            def _():
                for copy in copies:
                    copy.wait_send()

    def down(c, ld0):
        ps = lax.rem(c, 2)
        ends, _ = sums_out(c)
        pl.when(c >= 2)(lambda: wait_sums_out(c - 2))
        for part in range(2):
            @each(ne // 2)
            def _(i):
                slot = take(ld0 + part * (ne // 2) + i, ff)
                pv = jnp.dot(act[...], ring[slot, :ff, :], preferred_element_type=F32)
                cs = tile(i, DOT_N)
                psum[ps, part, :, cs] = pv[:H]
                psum[ps, 3 - part, :, cs] = pv[H:R]

            @pl.when(is_end)
            def _():
                for copy in (ends[:1], ends[1:])[part]:
                    copy.start()

    def arrive(c, k, buf):
        ps_copy(c, 0, z, k, mate).wait_recv()
        copy = pltpu.make_async_copy(land_ref.at[c, k], stage.at[buf], loc_sem.at[2 + buf])
        copy.start()
        return copy

    def tiles(fn):
        @each(4)
        def _(i):
            fn(tile(i, H // 4))

    def pass_on(c, k, zz, send):
        arrive(c, k, 0).wait()

        def add(rs):
            psum[lax.rem(c, 2), zz, rs, :] += stage[0, rs, :]

        tiles(add)
        send.start()

    def finish(c, ks):
        for copy in [arrive(c, k, i) for i, k in enumerate(ks)]:
            copy.wait()

        def add(rs):
            v = psum[lax.rem(c, 2), z, rs, :] + stage[0, rs, :]
            if len(ks) == 2:
                v = v + stage[1, rs, :]
            xo[c, rs, :] = (ybuf[c, rs, :] + v).astype(BF16)

        tiles(add)
        done.start(c)
        pltpu.make_async_copy(xo.at[c], out_block(c, z), loc_sem.at[4]).start()
        pltpu.make_async_copy(xo.at[c], out_block(c, z), loc_sem.at[4]).wait()

    def relay(c):
        _, mids = sums_out(c)
        pass_on(c, 0, far_end, mids[0])
        pass_on(c, 1, outer, mids[1])
        pass_on(c, 2, inner, mids[2])
        finish(c, (3, 4))

    issue(jnp.int32(0))
    issue(jnp.int32(1))
    o_start(0)
    o_start(1)

    @each(nc + 3)
    def _(j):
        c = j - 1
        in_mlp = (j >= 1) & (j <= nc)
        ld_b = per * j - (per - 4) * lax.div(j + big - 1, big)
        ld_d = per * j - (per - 8) - 4 * lax.div(j, nc)
        pl.when((j >= 1) & (j + 1 < nc))(lambda: o_start(j + 1))

        @pl.when(j < nc)
        def _():
            project(j, ld_b)
            hidden.start(j)

        @pl.when(in_mlp & is_end)
        def _():
            for r in range(3):
                hidden.wait(c, r)

        pl.when(in_mlp)(lambda: gate_up(c, ld_d))
        pl.when((j < nc) & is_mid)(lambda: hidden.serve1(j))
        pl.when(in_mlp)(lambda: down(c, ld_d + nd))
        pl.when((j < nc) & is_mid)(lambda: hidden.serve2(j))
        pl.when(in_mlp & is_mid)(lambda: relay(c))
        pl.when((j >= 2) & (j <= nc + 1) & is_end)(lambda: finish(j - 2, (0,)))

        @pl.when((j >= 3) & is_mid)
        def _():
            done.serve1(j - 3)
            done.serve2(j - 3)

    @each(nc)
    def _(c):
        @pl.when(is_end)
        def _():
            for r in range(3):
                done.wait(c, r)

        for d in (1, 2, 3):
            o_copy(c, d).wait_send()
        rdma(sstat.at[c], rstat.at[c], st_send.at[c, 0], st_recv.at[c, 0], mate).wait_send()
        hidden.drain(c)
        done.drain(c)
        pl.when(c >= nc - 2)(lambda: wait_sums_out(c))


def line_block(o, x, w_out, pieces, w_gate, w_up, w_down, gain):
    rows, depth = x.shape
    ff = w_gate.shape[1]
    kz = o.shape[1]
    nc = rows // ROWS_CH
    h, half = ROWS_CH // 2, depth // 2
    ring_rows = max(depth, ff, half // DOT_N * kz)
    sems = [pltpu.SemaphoreType.DMA((nc, n)) for n in (3, 3, 1, 1, 5, 3, 3, 5, 5, 3)]
    xout, _ = pl.pallas_call(
        functools.partial(line_kernel, nc=nc, heads_k=kz),
        in_specs=[ANY] * (6 + len(pieces)) + [VMEM],
        out_specs=[ANY] * 2,
        out_shape=[struct(x.shape, BF16), struct((nc, 5, h, half), F32)],
        scratch_shapes=[
            pltpu.VMEM((nc, 4, h, kz), BF16), pltpu.VMEM((nc, ROWS_CH, depth), BF16), pltpu.VMEM((nc, h, half), F32),
            pltpu.VMEM((3, ring_rows, DOT_N), BF16), pltpu.VMEM((2, 4, h, half), F32), pltpu.VMEM((ROWS_CH, ff), BF16),
            pltpu.VMEM((2, h, half), F32), pltpu.VMEM((h, half), BF16), pltpu.VMEM((nc, h, half), BF16),
            *[pltpu.VMEM((nc, h, LANES), F32)] * 2, pltpu.SemaphoreType.DMA((3,)), pltpu.SemaphoreType.DMA((5,)), *sems,
        ],
        compiler_params=params(60, collective_id=1, has_side_effects=True),
        cost_estimate=cost(6 * x.size * ff, 2 * x.size),
        name="line_block",
    )(o, x, w_out, *pieces, w_gate, w_up, w_down, gain.reshape(1, depth))
    return xout


def gather_w_out(w_out, tps):
    z, dp, core = lax.axis_index('tp'), lax.axis_index('dp'), lax.axis_index('cp') % 2
    n, half = w_out.shape[0] // 4, w_out.shape[1] // 2
    q = (z + 1) // 2 % 2
    quarter = lax.dynamic_slice_in_dim(w_out, (dp * 2 + core) * n, n, 0)
    same = lax.dynamic_slice_in_dim(quarter, q * half, half, 1)
    other = lax.dynamic_slice_in_dim(quarter, (1 - q) * half, half, 1)
    return tuple(lax.ppermute(a, 'tp', [(i, i ^ d) for i in range(tps)]) for d, a in ((1, other), (2, other), (3, same)))


def solution(mesh):
    groups = mesh.shape['cp']
    tps = mesh.shape['tp']
    dps = mesh.shape['dp']

    def local_layer(x_loc, kp_loc, vp_loc, norm_attn, w_query, w_key, w_value, w_out, norm_mlp, w_gate, w_up, w_down):
        rows = x_loc.shape[0]
        pre_dev, kv_loc, head_dim = kp_loc.shape
        c2 = head_dim ** -0.5 * math.log2(math.e)
        me = lax.axis_index('cp')
        q_pos = block_positions(me, groups, rows // 2, pre_dev * groups)
        own_pre = (kp_loc.transpose(1, 0, 2), vp_loc.transpose(1, 2, 0))
        far_pre = swap(own_pre, 'cp', groups, 2)
        near_pre = swap(own_pre, 'cp', groups, 1)
        wo_z = gather_w_out(w_out, tps)
        cos_tab, sin_tab = rope_tables(q_pos, head_dim)
        q, k_new, vt_new, k_flat, v_flat = qkv(x_loc, norm_attn, w_query, w_key, w_value, cos_tab, sin_tab)
        own_suf = (k_new, vt_new)
        first, q = lax.optimization_barrier((wo_z[0], q))
        wo_z = (first,) + wo_z[1:]
        wo_x = swap(wo_z[:1], 'dp', dps, 1)
        far_suf = swap(own_suf, 'cp', groups, 2)
        near_suf = swap(own_suf, 'cp', groups, 1)
        o, wo_pieces = attend(q, own_pre, near_pre, far_pre, own_suf, near_suf, far_suf, wo_z, wo_x, c2, groups, dps)
        x_out = line_block(o, x_loc, w_out, wo_pieces, w_gate, w_up, w_down, norm_mlp)
        return x_out, k_flat.reshape(rows, kv_loc, head_dim), v_flat.reshape(rows, kv_loc, head_dim)

    row_spec = P(('dp', 'cp'), None)
    kv_spec = P(('dp', 'cp'), 'tp', None)
    col_spec = P(None, 'tp')
    row_split = P('tp', None)
    vec_spec = P(None)
    return jax.shard_map(local_layer, mesh=mesh, in_specs=(row_spec, kv_spec, kv_spec, vec_spec, col_spec, col_spec, col_spec, row_split, vec_spec, col_spec, col_spec, row_split), out_specs=(row_spec, kv_spec, kv_spec), check_vma=False)
```

```python
import functools
import math

import jax
import jax.numpy as jnp
from jax import lax
from jax.experimental import pallas as pl
from jax.experimental.pallas import tpu as pltpu
from jax.sharding import PartitionSpec as P


ROPE_THETA = 500000.0
NORM_EPS = 1e-5
ROWS_CH = 256
F32 = jnp.float32
BF16 = jnp.bfloat16
HBM = pl.BlockSpec(memory_space=pl.ANY)
VMEM = pl.BlockSpec(memory_space=pltpu.VMEM)
LANES = 128
PAIR = 2 * LANES
NT = (((1,), (1,)), ((), ()))
each = functools.partial(pl.loop, 0)


def tile(i, n):
    return pl.ds(pl.multiple_of(i * n, n), n)


def params(mib, **more):
    return pltpu.CompilerParams(vmem_limit_bytes=mib * 2**20, **more)


def cost(flops, moved):
    return pl.CostEstimate(flops=flops, bytes_accessed=moved, transcendentals=0)


def struct(shape, dtype):
    return jax.ShapeDtypeStruct(shape, dtype)


def block_positions(owner, groups, blk_len, prefix_len):
    local_row = jnp.arange(2 * blk_len, dtype=jnp.int32)
    blk_idx = jnp.where(local_row < blk_len, owner, 2 * groups - 1 - owner)
    return prefix_len + blk_idx * blk_len + local_row % blk_len


def rope_tables(positions, head_dim):
    inv_freq = ROPE_THETA ** (-jnp.arange(0, head_dim, 2, dtype=F32) / head_dim)
    angles = positions.astype(F32)[:, None] * inv_freq[None, :]
    cos_tab, sin_tab = jnp.cos(angles), jnp.sin(angles)
    return jnp.concatenate([cos_tab, cos_tab], axis=1), jnp.concatenate([-sin_tab, sin_tab], axis=1)


def qkv_kernel(x_hbm, g_ref, wq_ref, wk_ref, wv_ref, cos_ref, sin_ref, q_ref, k_ref, vt_ref, kf_ref, vf_ref, x_ref, h_ref, sems, *, nq):
    step = pl.program_id(0)
    rows = x_ref.shape[0]
    parts, rt = sems.shape[0], 32

    @pl.when(step == 0)
    def _():
        n = rows // parts
        copies = [pltpu.make_async_copy(x_hbm.at[tile(i, n), :], x_ref.at[tile(i, n), :], sems.at[i]) for i in range(parts)]
        for copy in copies:
            copy.start()
        for i, copy in enumerate(copies):
            copy.wait()

            @pl.loop(i * n // rt, (i + 1) * n // rt)
            def _(j):
                sl = tile(j, rt)
                xv = x_ref[sl, :].astype(F32)
                inv = lax.rsqrt(jnp.mean(xv * xv, axis=-1, keepdims=True) + NORM_EPS)
                h_ref[sl, :] = (xv * inv * g_ref[...].astype(F32)).astype(BF16)

    def rope(block, sl):
        return (block * cos_ref[sl, :] + pltpu.roll(block, 64, axis=1) * sin_ref[sl, :]).astype(BF16)

    mt = 512

    def project(w_ref, store):
        @each(rows // mt)
        def _(i):
            sl = tile(i, mt)
            acc = jnp.dot(h_ref[sl, :], w_ref[...], preferred_element_type=F32)
            store(acc, sl)

    def heads_of(acc):
        return [(t, slice(t * LANES, (t + 1) * LANES), acc[:, t * LANES:(t + 1) * LANES]) for t in range(2)]

    def store_q(acc, sl):
        for _, cs, part in heads_of(acc):
            q_ref[sl, cs] = rope(part, sl)

    def store_k(acc, sl):
        for t, cs, part in heads_of(acc):
            kf_ref[sl, cs] = rope(part, sl)
            k_ref[t, sl, :] = kf_ref[sl, cs]

    def store_v(acc, sl):
        vf_ref[sl, :] = acc.astype(BF16)
        for t, _, part in heads_of(acc):
            vt_ref[t, :, sl] = part.T.astype(BF16)

    pl.when(step < nq)(lambda: project(wq_ref, store_q))
    pl.when(step == nq)(lambda: project(wk_ref, store_k))
    pl.when(step == nq + 1)(lambda: project(wv_ref, store_v))


def qkv(x, gain, wq, wk, wv, cos_tab, sin_tab):
    rows, depth = x.shape
    nq = wq.shape[1] // PAIR

    def fixed(shape):
        return pl.BlockSpec(shape, lambda j: tuple(0 for _ in shape))

    def whole(shape):
        return pl.BlockSpec(shape, lambda j: tuple(0 for _ in shape), pipeline_mode=pl.Buffered(1))

    def columns(n):
        return pl.BlockSpec((n, PAIR), lambda j: (0, jnp.minimum(j, nq - 1)))

    flat, by_head, by_head_t = (rows, PAIR), (2, rows, LANES), (2, LANES, rows)
    return pl.pallas_call(
        functools.partial(qkv_kernel, nq=nq),
        grid=(nq + 2,),
        in_specs=[HBM, whole((1, depth)), columns(depth), fixed(wk.shape), fixed(wv.shape), whole(cos_tab.shape), whole(sin_tab.shape)],
        out_specs=[columns(rows), fixed(by_head), fixed(by_head_t), fixed(flat), fixed(flat)],
        out_shape=[struct(s, BF16) for s in ((rows, nq * PAIR), by_head, by_head_t, flat, flat)],
        scratch_shapes=[pltpu.VMEM((rows, depth), BF16), pltpu.VMEM((rows, depth), BF16), pltpu.SemaphoreType.DMA((4,))],
        compiler_params=params(40, dimension_semantics=("arbitrary",)),
        cost_estimate=cost(2 * rows * depth * (nq + 2) * PAIR, 2 * depth * rows),
        name="qkv",
    )(x, gain.reshape(1, depth), wq, wk, wv, cos_tab, sin_tab)


NQ = 512
PER_KV = 4


class Fetch:
    def __init__(self, sems):
        self.sems, self.used = sems, 0

    def start(self, pairs):
        copies = []
        for src, dst in pairs:
            copies.append(pltpu.make_async_copy(src, dst, self.sems.at[self.used]))
            self.used += 1
        for copy in copies:
            copy.start()
        return copies


def settle(copies):
    for copy in copies:
        copy.wait()


def q_block(q_ref, head, half):
    return q_ref[tile(half, NQ), tile(head, LANES)]


def attend_items(q_ref, kb_ref, vb_ref, acc_ref, m_ref, l_ref, pbufs, n_items, item, bk, c2, diag=False):
    depth = len(pbufs)

    def scores(i, pb):
        head, half, start = item(i)
        n = head * 2 + half
        ks = kb_ref[head // PER_KV, pl.ds(pl.multiple_of(start, bk), bk), :]
        s = lax.dot_general(ks, q_block(q_ref, head, half), NT, preferred_element_type=F32)
        e = jnp.exp2(s * c2 - m_ref[n])
        if diag:
            seen = lax.broadcasted_iota(jnp.int32, (bk, NQ), 0) <= lax.broadcasted_iota(jnp.int32, (bk, NQ), 1)
            e = jnp.where(seen, e, 0.0)
        pb[...] = e.astype(BF16)
        l_ref[n] += jnp.sum(e.reshape(-1, *l_ref.shape[1:]), axis=0)

    def values(i, pb):
        head, half, start = item(i)
        vt = vb_ref[head // PER_KV, :, pl.ds(pl.multiple_of(start, bk), bk)]
        acc_ref[head * 2 + half] += jnp.dot(vt, pb[...], preferred_element_type=F32)

    scores(0, pbufs[0])

    def body(g, carry):
        for u in range(depth):
            i = g * depth + u
            scores(i + 1, pbufs[(u + 1) % depth])
            values(i, pbufs[u])
        return carry

    trips = n_items // depth - 1
    lax.fori_loop(0, trips, body, 0)
    for u in range(depth):
        if u + 1 < depth:
            scores(trips * depth + u + 1, pbufs[u + 1])
        values(trips * depth + u, pbufs[u])


def prefix_kernel(q_ref, ka, va, kb, vb, acc_ref, m_ref, l_ref, kbuf, vbuf, pa, pb, sems, *, heads, c2):
    fetch = Fetch(sems)
    n = ka.shape[1]
    settle(fetch.start([(ka, kbuf.at[:, tile(0, n), :]), (va, vbuf.at[:, :, tile(0, n)]), (kb, kbuf.at[:, tile(1, n), :]), (vb, vbuf.at[:, :, tile(1, n)])]))

    @each(heads * 2)
    def _(i):
        head, half = i // 2, i % 2
        s = lax.dot_general(kbuf[head // PER_KV, tile(0, LANES), :], q_block(q_ref, head, half), NT, preferred_element_type=F32)
        m_ref[i] = jnp.max(s, axis=0, keepdims=True) * c2
        for ref in (acc_ref, l_ref):
            ref[i] = jnp.zeros(ref.shape[1:], F32)

    bk = 2 * NQ
    per = kbuf.shape[1] // bk

    def item(i):
        pair = i // per
        return pair // 2, pair % 2, (i % per) * bk

    attend_items(q_ref, kbuf, vbuf, acc_ref, m_ref, l_ref, (pa, pb), heads * 2 * per, item, bk, c2)


def state_shapes(heads):
    return [struct((heads * 2, n, NQ), F32) for n in (LANES, 1, 8)]


def vmem_like(shapes):
    return [pltpu.VMEM(s.shape, s.dtype) for s in shapes]


def attend_prefix(q, pieces, c2):
    heads = q.shape[1] // LANES
    flat = [a for p in pieces for a in p]
    n = 2 * pieces[0][0].shape[1]
    shapes = state_shapes(heads)
    return pl.pallas_call(
        functools.partial(prefix_kernel, heads=heads, c2=c2),
        in_specs=[VMEM] + [HBM] * len(flat),
        out_specs=[VMEM] * len(shapes),
        out_shape=shapes,
        scratch_shapes=[
            pltpu.VMEM((2, n, LANES), BF16), pltpu.VMEM((2, LANES, n), BF16),
            *[pltpu.VMEM((2 * NQ, NQ), BF16)] * 2, pltpu.SemaphoreType.DMA((8,)),
        ],
        compiler_params=params(20),
        cost_estimate=cost(4 * q.size * n, 4 * q.size),
        name="attend_prefix",
    )(q, *flat)


def rest_kernel(*refs, group, groups, c2, axis):
    q_hbm, *refs = refs
    flat, refs = refs[:4 * groups], refs[4 * groups:]
    pairs = list(zip(flat[::2], flat[1::2]))
    pre, suf = pairs[:groups], pairs[groups:]
    acc_in, m_in, l_in, o_out, q_ref, kbuf, vbuf, ksuf, vsuf, acc_ref, m_ref, l_ref, o_ref, bad_ref, sems, wa, wb, pa, pb, pc, pd = refs
    heads = PER_KV
    me = lax.axis_index(axis)
    fetch = Fetch(sems)
    mine = group * heads * 2
    n_pre, n_suf = pre[0][0].shape[1], suf[0][0].shape[1]
    first = fetch.start([(q_hbm.at[:, tile(group, heads * LANES)], q_ref)])
    for i, (kr, vr) in enumerate(pre[2:]):
        first += fetch.start([(kr.at[group], kbuf.at[0, tile(i, n_pre), :]), (vr.at[group], vbuf.at[0, :, tile(i, n_pre)])])
    second = []
    for i, (kr, vr) in enumerate(suf):
        second += fetch.start([(kr.at[group], ksuf.at[0, tile(i, n_suf), :]), (vr.at[group], vsuf.at[0, :, tile(i, n_suf)])])
    for ref, old in ((acc_ref, acc_in), (m_ref, m_in), (l_ref, l_in)):
        ref[...] = old[pl.ds(mine, heads * 2)]
    settle(first)
    bk = 2 * NQ
    per = kbuf.shape[1] // bk

    def pre_item(i):
        pair = i // per
        return pair // 2, pair % 2, (i % per) * bk

    attend_items(q_ref, kbuf, vbuf, acc_ref, m_ref, l_ref, (wa, wb), heads * 2 * per, pre_item, bk, c2)
    settle(second)
    last = 2 * groups - 1

    def locate(blk):
        late = (blk >= groups).astype(jnp.int32)
        owner = jnp.where(blk < groups, blk, last - blk)
        diff = (owner % 2 != me % 2).astype(jnp.int32) + 2 * (owner // 2 != me // 2).astype(jnp.int32)
        return (diff * 2 + late) * NQ

    def full_item(i):
        head, r = i // last, i % last
        half = (r >= me).astype(jnp.int32)
        return head, half, locate(jnp.where(r < me, r, r - me))

    def diag_item(i):
        half = i % 2
        return i // 2, half, locate(jnp.where(half == 0, me, last - me))

    attend_items(q_ref, ksuf, vsuf, acc_ref, m_ref, l_ref, (pa, pb, pc, pd), heads * last, full_item, NQ, c2)
    attend_items(q_ref, ksuf, vsuf, acc_ref, m_ref, l_ref, (pa, pb), heads * 2, diag_item, NQ, c2, diag=True)
    bad_ref[...] = jnp.zeros_like(bad_ref)
    chunk = ROWS_CH // 2

    def write(i, acc, total):
        head, half = i // 2, i % 2
        out = (acc * (1.0 / total)).T.astype(BF16)
        n_p = NQ // chunk
        for p in range(n_p):
            o_ref[p % 2, tile(half * (n_p // 2) + p // 2, chunk), tile(head, LANES)] = out[p * chunk:(p + 1) * chunk]

    @each(heads * 2)
    def _(i):
        acc = acc_ref[i]
        total = jnp.sum(l_ref[i], axis=0, keepdims=True)
        bad = jnp.where((jnp.abs(acc) < jnp.inf) & (total < jnp.inf), 0.0, 1.0)
        for j in range(NQ // LANES):
            part = bad[:, j * LANES:(j + 1) * LANES]
            bad_ref[...] = jnp.maximum(bad_ref[...], jnp.max(part.reshape(-1, *bad_ref.shape), axis=0))
        write(i, acc, total)

    @pl.when(jnp.max(bad_ref[...]) > 0.0)
    def _():
        @each(heads * 2)
        def _(i):
            head, half = i // 2, i % 2
            q = q_block(q_ref, head, half)
            m_ref[i] = jnp.full((1, NQ), -jnp.inf, F32)
            for ref in (acc_ref, l_ref):
                ref[i] = jnp.zeros(ref.shape[1:], F32)

            def update(ks, vt, seen):
                s = lax.dot_general(ks, q, NT, preferred_element_type=F32) * c2
                if seen is not None:
                    s = jnp.where(seen, s, -jnp.inf)
                m_old = m_ref[i]
                m_new = jnp.maximum(m_old, jnp.max(s, axis=0, keepdims=True))
                alpha = jnp.exp2(m_old - m_new)
                e = jnp.exp2(s - m_new)
                m_ref[i] = m_new
                l_ref[i] = l_ref[i] * alpha + jnp.sum(e.reshape(-1, *l_ref.shape[1:]), axis=0)
                acc_ref[i] = acc_ref[i] * alpha + jnp.dot(vt, e.astype(BF16), preferred_element_type=F32)

            kpre, vpre = pa.at[:, tile(0, LANES)], pb.at[tile(0, LANES), :]
            for kr, vr in pre:
                @each(n_pre // NQ)
                def _(j):
                    pltpu.sync_copy(kr.at[group, tile(j, NQ), :], kpre)
                    pltpu.sync_copy(vr.at[group, :, tile(j, NQ)], vpre)
                    update(kpre[...], vpre[...], None)

            mine_blk = jnp.where(half == 0, me, last - me)

            @each(2 * groups)
            def _(blk):
                @pl.when(blk <= mine_blk)
                def _():
                    start = pl.ds(pl.multiple_of(locate(blk), NQ), NQ)
                    seen = (lax.broadcasted_iota(jnp.int32, (NQ, NQ), 0) <= lax.broadcasted_iota(jnp.int32, (NQ, NQ), 1)) | (blk < mine_blk)
                    update(ksuf[0, start, :], vsuf[0, :, start], seen)

            write(i, acc_ref[i], jnp.sum(l_ref[i], axis=0, keepdims=True))

    pltpu.sync_copy(o_ref, o_out)


def attend_rest(q, pre, suf, state, c2, axis, group):
    rows, groups, width = q.shape[0], len(suf), PER_KV * LANES
    n_pre, n_suf = 2 * pre[0][0].shape[1], groups * suf[0][0].shape[1]
    flat = [a for p in list(pre) + list(suf) for a in p]
    acc, m, total = state_shapes(PER_KV)
    out = struct((2, rows // 2, width), BF16)
    return pl.pallas_call(
        functools.partial(rest_kernel, group=group, groups=groups, c2=c2, axis=axis),
        in_specs=[HBM] * (len(flat) + 1) + [VMEM] * 3,
        out_specs=HBM,
        out_shape=pltpu.HBM(out.shape, out.dtype),
        scratch_shapes=[
            pltpu.VMEM((rows, width), BF16), pltpu.VMEM((1, n_pre, LANES), BF16), pltpu.VMEM((1, LANES, n_pre), BF16),
            pltpu.VMEM((1, n_suf, LANES), BF16), pltpu.VMEM((1, LANES, n_suf), BF16), *vmem_like([acc, m, total, out]),
            pltpu.VMEM((8, LANES), F32), pltpu.SemaphoreType.DMA((20,)), *[pltpu.VMEM((2 * NQ, NQ), BF16)] * 2, *[pltpu.VMEM((NQ, NQ), BF16)] * 4,
        ],
        compiler_params=params(20),
        cost_estimate=cost(2 * rows * width * (2 * n_pre + n_suf), 4 * q.size),
        name="attend_rest",
    )(q, *flat, *state)


def swap(arrays, axis, groups, bit):
    return tuple(lax.ppermute(a, axis, [(i, i ^ bit) for i in range(groups)]) for a in arrays)


def attend(q, own_pre, near_pre, far_pre, own_suf, near_suf, far_suf, wo_z, c2, groups, tps, dps):
    state = attend_prefix(q, (own_pre, near_pre), c2)
    far_pre, far_suf, wo_z, state = lax.optimization_barrier((far_pre, far_suf, wo_z, state))
    cross_pre = swap(far_pre, 'cp', groups, 1)
    cross_suf = swap(far_suf, 'cp', groups, 1)
    wo_x = swap(wo_z, 'dp', dps, 1)
    wo_near = swap(wo_z, 'cp', groups, 1)
    pre, suf = (own_pre, near_pre, far_pre, cross_pre), (own_suf, near_suf, far_suf, cross_suf)
    o_first = attend_rest(q, pre, suf, state, c2, 'cp', 0)
    side = lax.axis_index('tp') // 2
    here, there = (lax.dynamic_index_in_dim(o_first, s, keepdims=False) for s in (side, 1 - side))
    o_got = tuple(lax.ppermute(a, 'tp', [(i, i ^ d) for i in range(tps)]) for d, a in ((1, here), (2, there), (3, there)))
    o_first, q = lax.optimization_barrier((o_first, q))
    o_last = attend_rest(q, pre, suf, state, c2, 'cp', 1)
    wo_x, o_last = lax.optimization_barrier((wo_x, o_last))
    wo_cross = swap(wo_x, 'cp', groups, 1)
    return (here,) + o_got, o_last, wo_z + wo_x + wo_near + wo_cross


MESH = pl.DeviceIdType.MESH
DOT_N = 512
MID_PLAN = ((), (('r2', -1), ('ha', 1), ('O', 3), ('xa', -2),), (('r4', -1),), (('xc', -2),), (('hb', 1),), (('xb', -1),), (('r1', 0), ('hc', 1), ('r3', 0),))
END_PLAN = ((('f', -2), ('hw', 0), ('O', 3),), (), (), (), (), (), ())
AHEAD, BEHIND = 3, 2


def side_of(z):
    return lax.div(z, 2)


def colhalf_of(z):
    return lax.rem(lax.div(z + 1, 2), 2)


def line_kernel(*refs, nc):
    o_first, o_ref, x_ref, wo_ref, *refs = refs[:4], *refs[4:]
    wo_pieces, refs = refs[:12], refs[12:]
    wg_ref, wu_ref, wd_ref, gain_ref, xout_ref, land_ref = refs[:6]
    (obuf, h2, ybuf, ring, psum, act, stage, xs, xo, sstat, rstat,
     ring_sem, loc_sem, o_send, o_recv, st_send, st_recv, a1_send, a1_recv, rs_send, rs_recv, a2_send, a2_recv) = refs[6:]
    R, H = ROWS_CH, ROWS_CH // 2
    depth = wg_ref.shape[0]
    ff = wg_ref.shape[1]
    half = depth // 2
    width = o_ref.shape[-1]
    kz = 2 * width
    n_ct = half // DOT_N
    nd, ne = ff // PAIR, depth // DOT_N
    per = 4 + nd + ne
    total_loads = nc * per
    big = 1024

    z = lax.axis_index('tp')
    dp = lax.axis_index('dp')
    core = lax.rem(lax.axis_index('cp'), 2)
    side, q = side_of(z), colhalf_of(z)
    is_mid = q == 1
    is_end = q != 1
    near = 1 + side
    outer = 3 * side
    inner = 2 - side
    far_end = 3 - 3 * side
    peers = {1: z + 1 - 2 * lax.rem(z, 2), 2: lax.rem(z + 2, 4), 3: 3 - z}
    mate = peers[1]

    def rdma(src, dst, ssem, rsem, dev):
        return pltpu.make_async_remote_copy(src_ref=src, dst_ref=dst, send_sem=ssem, recv_sem=rsem, device_id={'tp': dev}, device_id_type=MESH)

    def rows_at(zz):
        return tile(side_of(zz), H)

    def cols_at(zz):
        return tile(colhalf_of(zz), half)

    barrier = pltpu.get_barrier_semaphore()
    for d in (1, 2, 3):
        pl.semaphore_signal(barrier, inc=1, device_id={'tp': peers[d]}, device_id_type=MESH)
    pl.semaphore_wait(barrier, 3)

    def load_kind(ld):
        u = ld + (per - 4)
        i1 = lax.div(u, per)
        a = lax.div(i1 + big - 1, big)
        t = lax.rem(u, per) + 4 * lax.div(i1, nc)
        return a * t + (1 - a) * ld

    def issue(ld):
        slot = lax.rem(ld, 3)
        sem = ring_sem.at[slot]
        t = load_kind(ld)

        def start(src, dst):
            pltpu.make_async_copy(src, dst, sem).start()

        for d in range(4):
            @pl.when(t == d)
            def _():
                @each(n_ct)
                def _(ct):
                    c0 = pl.multiple_of(ct * DOT_N, DOT_N)
                    if d == 0:
                        cs = tile(q * n_ct + ct, DOT_N)
                        start(wo_ref.at[:, cs], ring.at[slot, tile(ct, kz), :])
                    else:
                        for dpx in range(2):
                            for cx in range(2):
                                piece = wo_pieces[(dpx + 2 * cx) * 3 + d - 1]
                                n = piece.shape[0]
                                j = (dp + dpx - 2 * dp * dpx) * 2 + (core + cx - 2 * core * cx)
                                r0 = pl.multiple_of(ct * kz + j * n, n)
                                start(piece.at[:, pl.ds(c0, DOT_N)], ring.at[slot, pl.ds(r0, n), :])

        @pl.when((t >= 4) & (t < 4 + nd))
        def _():
            cs = pl.ds(pl.multiple_of((t - 4) * 256, 256), 256)
            start(wg_ref.at[:, cs], ring.at[slot, :depth, :PAIR])
            start(wu_ref.at[:, cs], ring.at[slot, :depth, PAIR:])

        @pl.when(t >= 4 + nd)
        def _():
            cs = pl.ds(pl.multiple_of((t - 4 - nd) * DOT_N, DOT_N), DOT_N)
            start(wd_ref.at[:, cs], ring.at[slot, :ff, :])

    def take(ld, n_rows):
        slot = lax.rem(ld, 3)
        whole = ring.at[slot, :n_rows, :]
        pltpu.make_async_copy(whole, whole, ring_sem.at[slot]).wait()
        pl.when(ld + 2 < total_loads)(lambda: issue(ld + 2))
        return slot

    def late(c, d):
        return obuf.at[c, d, :, tile(1, width)]

    def o_copy(c, d):
        return rdma(o_ref.at[side_of(peers[d]), tile(c, H), :], late(c, d), o_send.at[c, d - 1], o_recv.at[c, d - 1], peers[d])

    def o_start(c):
        for d in (1, 2, 3):
            o_copy(c, d).start()

    def project(c, ld0):
        own_o = pltpu.make_async_copy(o_ref.at[side, tile(c, H), :], late(c, 0), loc_sem.at[0])
        own_x = pltpu.make_async_copy(x_ref.at[tile(c * 2 + side, H), cols_at(z)], xs, loc_sem.at[1])
        own_o.start()
        own_x.start()
        for d in (1, 2, 3):
            o_copy(c, d).wait_recv()
        own_o.wait()
        own_x.wait()

        @each(n_ct)
        def _(ct):
            cs = tile(ct, DOT_N)
            ybuf[c, :, cs] = xs[:, cs].astype(F32)

        @each(4)
        def _(d):
            slot = take(ld0 + d, n_ct * kz)

            @each(n_ct)
            def _(ct):
                cs = tile(ct, DOT_N)
                w = ring[slot, tile(ct, kz), :]
                ybuf[c, :, cs] += jnp.dot(obuf[c, d], w, preferred_element_type=F32)

        sstat[c] = jnp.zeros((H, LANES), F32)

        @each(n_ct)
        def _(ct):
            yv = ybuf[c, :, tile(ct, DOT_N)]
            sstat[c] += jnp.broadcast_to(jnp.sum(yv * yv, axis=-1, keepdims=True), (H, LANES))

        swap_stat = rdma(sstat.at[c], rstat.at[c], st_send.at[c, 0], st_recv.at[c, 0], mate)
        swap_stat.start()
        swap_stat.wait_recv()
        inv = lax.rsqrt((sstat[c] + rstat[c])[:, 0:1] * (1.0 / depth) + NORM_EPS)

        @each(n_ct)
        def _(ct):
            cs = tile(ct, DOT_N)
            gs = tile(q * n_ct + ct, DOT_N)
            h2[c, rows_at(z), gs] = (ybuf[c, :, cs] * inv * gain_ref[:, gs].astype(F32)).astype(BF16)

    class Spread:
        def __init__(self, block, send, recv, own=None):
            self.block, self.send, self.recv, self.own = block, send, recv, own

        def copy(self, c, zz, s, r, dev, own=False):
            src = self.own(c) if own and self.own is not None else self.block(c, zz)
            return rdma(src, self.block(c, zz), self.send.at[c, s], self.recv.at[c, r], dev)

        def to_near(self, c):
            return self.copy(c, z, 0, 0, near, own=True)

        def to_outer(self, c):
            return self.copy(c, z, 0, 0, outer, own=True)

        def to_inner(self, c):
            return self.copy(c, z, 1, 1, inner, own=True)

        def end_to_inner(self, c):
            return self.copy(c, outer, 2, 2, inner)

        def inner_to_outer(self, c):
            return self.copy(c, inner, 3, 1, outer)

        def far_to_outer(self, c):
            return self.copy(c, far_end, 4, 2, outer)

        def start(self, c):
            pl.when(is_end)(lambda: self.to_near(c).start())

            @pl.when(is_mid)
            def _():
                self.to_outer(c).start()
                self.to_inner(c).start()

        def wait(self, c, r):
            self.copy(c, z, 0, r, mate).wait_recv()

        def serve(self, r, c):
            self.wait(c, r)
            (self.end_to_inner, self.inner_to_outer, self.far_to_outer)[r](c).start()

        def drain(self, c):
            @pl.when(is_end)
            def _():
                self.to_near(c).wait_send()

            @pl.when(is_mid)
            def _():
                for copy in (self.to_outer(c), self.to_inner(c), self.end_to_inner(c), self.inner_to_outer(c), self.far_to_outer(c)):
                    copy.wait_send()

    hidden = Spread(lambda c, zz: h2.at[c, rows_at(zz), cols_at(zz)], a1_send, a1_recv)

    def out_block(c, zz):
        return xout_ref.at[tile(c * 2 + side_of(zz), H), cols_at(zz)]

    done = Spread(out_block, a2_send, a2_recv, own=lambda c: xo.at[c])

    def gate_up(c, ld0, active, after):
        @each(nd)
        def _(i):
            @pl.when(active)
            def _():
                slot = take(ld0 + i, depth)
                gu = jnp.dot(h2[c], ring[slot, :depth, :], preferred_element_type=F32)
                g, u = gu[:, :PAIR], gu[:, PAIR:]
                act[:, tile(i, PAIR)] = (g * (1.0 / (1.0 + jnp.exp(-g))) * u).astype(BF16)

            for k in range(4):
                pl.when(i == (k + 1) * nd // 4 - 1)(functools.partial(after, k + 1))

    def ps_copy(c, k_send, zz, k_recv, dev):
        return rdma(psum.at[lax.rem(c, 2), zz], land_ref.at[c, k_recv], rs_send.at[c, k_send], rs_recv.at[c, k_recv], dev)

    def sums_out(c):
        ends = (ps_copy(c, 0, far_end, 0, near), ps_copy(c, 1, inner, 2, near), ps_copy(c, 2, near, 3, near))
        mids = (ps_copy(c, 0, far_end, 1, inner), ps_copy(c, 1, outer, 0, outer), ps_copy(c, 2, inner, 4, inner))
        return ends, mids

    def wait_sums_out(c):
        ends, mids = sums_out(c)
        for flag, copies in ((is_end, ends), (is_mid, mids)):
            @pl.when(flag)
            def _():
                for copy in copies:
                    copy.wait_send()

    def down(c, ld0, part):
        ps = lax.rem(c, 2)
        ends, _ = sums_out(c)
        if part == 0:
            pl.when(c >= 2)(lambda: wait_sums_out(c - 2))

        @each(ne // 2)
        def _(i):
            slot = take(ld0 + part * (ne // 2) + i, ff)
            pv = jnp.dot(act[...], ring[slot, :ff, :], preferred_element_type=F32)
            cs = tile(i, DOT_N)
            psum[ps, part, :, cs] = pv[:H]
            psum[ps, 3 - part, :, cs] = pv[H:R]

        @pl.when(is_end)
        def _():
            for copy in (ends[:1], ends[1:])[part]:
                copy.start()

    def arrive(c, k, buf):
        ps_copy(c, 0, z, k, mate).wait_recv()
        copy = pltpu.make_async_copy(land_ref.at[c, k], stage.at[buf], loc_sem.at[2 + buf])
        copy.start()
        return copy

    def tiles(fn):
        @each(4)
        def _(i):
            fn(tile(i, H // 4))

    def pass_on(c, k, zz, send):
        arrive(c, k, 0).wait()

        def add(rs):
            psum[lax.rem(c, 2), zz, rs, :] += stage[0, rs, :]

        tiles(add)
        send.start()

    def finish(c, ks):
        for copy in [arrive(c, k, i) for i, k in enumerate(ks)]:
            copy.wait()

        def add(rs):
            v = psum[lax.rem(c, 2), z, rs, :] + stage[0, rs, :]
            if len(ks) == 2:
                v = v + stage[1, rs, :]
            xo[c, rs, :] = (ybuf[c, rs, :] + v).astype(BF16)

        tiles(add)
        done.start(c)
        pltpu.make_async_copy(xo.at[c], out_block(c, z), loc_sem.at[4]).start()
        pltpu.make_async_copy(xo.at[c], out_block(c, z), loc_sem.at[4]).wait()

    def relay(k, c):
        pass_on(c, k, (far_end, outer, inner)[k], sums_out(c)[1][k])

    def hidden_wait(c):
        for r in range(3):
            hidden.wait(c, r)

    steps = {'O': o_start, 'hw': hidden_wait, 'f': lambda c: finish(c, (0,)), 'r4': lambda c: finish(c, (3, 4))}
    for r in range(3):
        steps['h' + 'abc'[r]] = functools.partial(hidden.serve, r)
        steps['x' + 'abc'[r]] = functools.partial(done.serve, r)
        steps['r' + '123'[r]] = functools.partial(relay, r)

    early = [pltpu.make_async_copy(src, obuf.at[:, d, :, tile(0, width)], loc_sem.at[5 + d]) for d, src in enumerate(o_first)]
    for copy in early:
        copy.start()
    issue(jnp.int32(0))
    issue(jnp.int32(1))
    for copy in early:
        copy.wait()

    @each(AHEAD + nc + BEHIND)
    def _(t):
        j = t - AHEAD
        jj = j + 1
        active = (j >= 0) & (j < nc)

        def after(k):
            for flag, plan in ((is_mid, MID_PLAN[k]), (is_end, END_PLAN[k])):
                def run(plan=plan):
                    for name, ahead in plan:
                        c = j + ahead
                        pl.when((c >= 0) & (c < nc))(functools.partial(steps[name], c))

                if plan:
                    pl.when(flag)(run)

        @pl.when((jj >= 0) & (jj < nc))
        def _():
            project(jj, per * jj - (per - 4) * lax.div(jj + big - 1, big))
            hidden.start(jj)

        after(0)
        ld_d = per * jj - (per - 8) - 4 * lax.div(jj, nc)
        gate_up(j, ld_d, active, after)
        for part in range(2):
            pl.when(active)(lambda: down(j, ld_d + nd, part))
            after(5 + part)

    @each(nc)
    def _(c):
        @pl.when(is_end)
        def _():
            for r in range(3):
                done.wait(c, r)

        for d in (1, 2, 3):
            o_copy(c, d).wait_send()
        rdma(sstat.at[c], rstat.at[c], st_send.at[c, 0], st_recv.at[c, 0], mate).wait_send()
        hidden.drain(c)
        done.drain(c)
        pl.when(c >= nc - 2)(lambda: wait_sums_out(c))


def line_block(o_first, o_last, x, w_out, pieces, w_gate, w_up, w_down, gain):
    rows, depth = x.shape
    ff = w_gate.shape[1]
    width = o_last.shape[-1]
    kz = 2 * width
    nc = rows // ROWS_CH
    h, half = ROWS_CH // 2, depth // 2
    ring_rows = max(depth, ff, half // DOT_N * kz)
    sems = [pltpu.SemaphoreType.DMA((nc, n)) for n in (3, 3, 1, 1, 5, 3, 3, 5, 5, 3)]
    xout, _ = pl.pallas_call(
        functools.partial(line_kernel, nc=nc),
        in_specs=[HBM] * (10 + len(pieces)) + [VMEM],
        out_specs=[HBM] * 2,
        out_shape=[struct(x.shape, BF16), struct((nc, 5, h, half), F32)],
        scratch_shapes=[
            pltpu.VMEM((nc, 4, h, kz), BF16), pltpu.VMEM((nc, ROWS_CH, depth), BF16), pltpu.VMEM((nc, h, half), F32),
            pltpu.VMEM((3, ring_rows, DOT_N), BF16), pltpu.VMEM((2, 4, h, half), F32), pltpu.VMEM((ROWS_CH, ff), BF16),
            pltpu.VMEM((2, h, half), F32), pltpu.VMEM((h, half), BF16), pltpu.VMEM((nc, h, half), BF16),
            *[pltpu.VMEM((nc, h, LANES), F32)] * 2, pltpu.SemaphoreType.DMA((3,)), pltpu.SemaphoreType.DMA((9,)), *sems,
        ],
        compiler_params=params(60, collective_id=1, has_side_effects=True),
        cost_estimate=cost(6 * x.size * ff, 2 * x.size),
        name="line_block",
    )(*(a.reshape(nc, h, width) for a in o_first), o_last, x, w_out, *pieces, w_gate, w_up, w_down, gain.reshape(1, depth))
    return xout


def gather_w_out(w_out, tps):
    z, dp, core = lax.axis_index('tp'), lax.axis_index('dp'), lax.axis_index('cp') % 2
    n, half = w_out.shape[0] // 4, w_out.shape[1] // 2
    q = (z + 1) // 2 % 2
    quarter = lax.dynamic_slice_in_dim(w_out, (dp * 2 + core) * n, n, 0)
    same = lax.dynamic_slice_in_dim(quarter, q * half, half, 1)
    other = lax.dynamic_slice_in_dim(quarter, (1 - q) * half, half, 1)
    return tuple(lax.ppermute(a, 'tp', [(i, i ^ d) for i in range(tps)]) for d, a in ((1, other), (2, other), (3, same)))


def solution(mesh):
    groups = mesh.shape['cp']
    tps = mesh.shape['tp']
    dps = mesh.shape['dp']

    def local_layer(x_loc, kp_loc, vp_loc, norm_attn, w_query, w_key, w_value, w_out, norm_mlp, w_gate, w_up, w_down):
        rows = x_loc.shape[0]
        pre_dev, kv_loc, head_dim = kp_loc.shape
        c2 = head_dim ** -0.5 * math.log2(math.e)
        me = lax.axis_index('cp')
        q_pos = block_positions(me, groups, rows // 2, pre_dev * groups)
        own_pre = (kp_loc.transpose(1, 0, 2), vp_loc.transpose(1, 2, 0))
        far_pre = swap(own_pre, 'cp', groups, 2)
        near_pre = swap(own_pre, 'cp', groups, 1)
        wo_z = gather_w_out(w_out, tps)
        cos_tab, sin_tab = rope_tables(q_pos, head_dim)
        q, k_new, vt_new, k_flat, v_flat = qkv(x_loc, norm_attn, w_query, w_key, w_value, cos_tab, sin_tab)
        own_suf = (k_new, vt_new)
        far_suf = swap(own_suf, 'cp', groups, 2)
        near_suf = swap(own_suf, 'cp', groups, 1)
        o_first, o_last, wo_pieces = attend(q, own_pre, near_pre, far_pre, own_suf, near_suf, far_suf, wo_z, c2, groups, tps, dps)
        x_out = line_block(o_first, o_last, x_loc, w_out, wo_pieces, w_gate, w_up, w_down, norm_mlp)
        return x_out, k_flat.reshape(rows, kv_loc, head_dim), v_flat.reshape(rows, kv_loc, head_dim)

    row_spec = P(('dp', 'cp'), None)
    kv_spec = P(('dp', 'cp'), 'tp', None)
    col_spec = P(None, 'tp')
    row_split = P('tp', None)
    vec_spec = P(None)
    return jax.shard_map(local_layer, mesh=mesh, in_specs=(row_spec, kv_spec, kv_spec, vec_spec, col_spec, col_spec, col_spec, row_split, vec_spec, col_spec, col_spec, row_split), out_specs=(row_spec, kv_spec, kv_spec), check_vma=False)
```

```python
import functools
import math

import jax
import jax.numpy as jnp
from jax import lax
from jax.experimental import pallas as pl
from jax.experimental.pallas import tpu as pltpu
from jax.sharding import PartitionSpec as P


ROPE_THETA = 500000.0
NORM_EPS = 1e-5
ROWS_CH = 128
F32 = jnp.float32
BF16 = jnp.bfloat16
HBM = pl.BlockSpec(memory_space=pl.ANY)
VMEM = pl.BlockSpec(memory_space=pltpu.VMEM)
IN_HBM = pl.BlockSpec(memory_space=pltpu.HBM)
LANES = 128
PAIR = 2 * LANES
NT = (((1,), (1,)), ((), ()))
each = functools.partial(pl.loop, 0)


def tile(i, n):
    return pl.ds(pl.multiple_of(i * n, n), n)


def params(mib, **more):
    return pltpu.CompilerParams(vmem_limit_bytes=mib * 2**20, **more)


def cost(flops, moved):
    return pl.CostEstimate(flops=flops, bytes_accessed=moved, transcendentals=0)


def struct(shape, dtype):
    return jax.ShapeDtypeStruct(shape, dtype)


def block_positions(owner, groups, blk_len, prefix_len):
    local_row = jnp.arange(2 * blk_len, dtype=jnp.int32)
    blk_idx = jnp.where(local_row < blk_len, owner, 2 * groups - 1 - owner)
    return prefix_len + blk_idx * blk_len + local_row % blk_len


def rope_tables(positions, head_dim):
    inv_freq = ROPE_THETA ** (-jnp.arange(0, head_dim, 2, dtype=F32) / head_dim)
    angles = positions.astype(F32)[:, None] * inv_freq[None, :]
    cos_tab, sin_tab = jnp.cos(angles), jnp.sin(angles)
    return jnp.concatenate([cos_tab, cos_tab], axis=1), jnp.concatenate([-sin_tab, sin_tab], axis=1)


def qkv_kernel(x_hbm, g_ref, wq_ref, wk_ref, wv_ref, cos_ref, sin_ref, q_ref, k_ref, vt_ref, kf_ref, vf_ref, x_ref, h_ref, sems, *, nq):
    step = pl.program_id(0)
    rows = x_ref.shape[0]
    parts, rt = sems.shape[0], 32

    @pl.when(step == 0)
    def _():
        n = rows // parts
        copies = [pltpu.make_async_copy(x_hbm.at[tile(i, n), :], x_ref.at[tile(i, n), :], sems.at[i]) for i in range(parts)]
        for copy in copies:
            copy.start()
        for i, copy in enumerate(copies):
            copy.wait()

            @pl.loop(i * n // rt, (i + 1) * n // rt)
            def _(j):
                sl = tile(j, rt)
                xv = x_ref[sl, :].astype(F32)
                inv = lax.rsqrt(jnp.mean(xv * xv, axis=-1, keepdims=True) + NORM_EPS)
                h_ref[sl, :] = (xv * inv * g_ref[...].astype(F32)).astype(BF16)

    def rope(block, sl):
        return (block * cos_ref[sl, :] + pltpu.roll(block, 64, axis=1) * sin_ref[sl, :]).astype(BF16)

    mt = 512

    def project(w_ref, store):
        @each(rows // mt)
        def _(i):
            sl = tile(i, mt)
            acc = jnp.dot(h_ref[sl, :], w_ref[...], preferred_element_type=F32)
            store(acc, sl)

    def heads_of(acc):
        return [(t, slice(t * LANES, (t + 1) * LANES), acc[:, t * LANES:(t + 1) * LANES]) for t in range(2)]

    def store_q(acc, sl):
        for _, cs, part in heads_of(acc):
            q_ref[sl, cs] = rope(part, sl)

    def store_k(acc, sl):
        for t, cs, part in heads_of(acc):
            kf_ref[sl, cs] = rope(part, sl)
            k_ref[t, sl, :] = kf_ref[sl, cs]

    def store_v(acc, sl):
        vf_ref[sl, :] = acc.astype(BF16)
        for t, _, part in heads_of(acc):
            vt_ref[t, :, sl] = part.T.astype(BF16)

    pl.when(step < nq)(lambda: project(wq_ref, store_q))
    pl.when(step == nq)(lambda: project(wk_ref, store_k))
    pl.when(step == nq + 1)(lambda: project(wv_ref, store_v))


def qkv(x, gain, wq, wk, wv, cos_tab, sin_tab):
    rows, depth = x.shape
    nq = wq.shape[1] // PAIR

    def fixed(shape):
        return pl.BlockSpec(shape, lambda j: tuple(0 for _ in shape))

    def whole(shape):
        return pl.BlockSpec(shape, lambda j: tuple(0 for _ in shape), pipeline_mode=pl.Buffered(1))

    def columns(n):
        return pl.BlockSpec((n, PAIR), lambda j: (0, jnp.minimum(j, nq - 1)))

    flat, by_head, by_head_t = (rows, PAIR), (2, rows, LANES), (2, LANES, rows)
    return pl.pallas_call(
        functools.partial(qkv_kernel, nq=nq),
        grid=(nq + 2,),
        in_specs=[HBM, whole((1, depth)), columns(depth), fixed(wk.shape), fixed(wv.shape), whole(cos_tab.shape), whole(sin_tab.shape)],
        out_specs=[columns(rows), fixed(by_head), fixed(by_head_t), fixed(flat), fixed(flat)],
        out_shape=[struct(s, BF16) for s in ((rows, nq * PAIR), by_head, by_head_t, flat, flat)],
        scratch_shapes=[pltpu.VMEM((rows, depth), BF16), pltpu.VMEM((rows, depth), BF16), pltpu.SemaphoreType.DMA((4,))],
        compiler_params=params(56, dimension_semantics=("arbitrary",)),
        cost_estimate=cost(2 * rows * depth * (nq + 2) * PAIR, 2 * depth * rows),
        name="qkv",
    )(x, gain.reshape(1, depth), wq, wk, wv, cos_tab, sin_tab)


NQ = 512
PER_KV = 4


class Fetch:
    def __init__(self, sems):
        self.sems, self.used = sems, 0

    def start(self, pairs):
        copies = []
        for src, dst in pairs:
            copies.append(pltpu.make_async_copy(src, dst, self.sems.at[self.used]))
            self.used += 1
        for copy in copies:
            copy.start()
        return copies


def settle(copies):
    for copy in copies:
        copy.wait()


def q_block(q_ref, head, half):
    return q_ref[tile(half, NQ), tile(head, LANES)]


def attend_items(q_ref, kb_ref, vb_ref, acc_ref, m_ref, l_ref, pbufs, n_items, item, bk, c2, diag=False):
    depth = len(pbufs)

    def scores(i, pb):
        head, half, start = item(i)
        n = head * 2 + half
        ks = kb_ref[head // PER_KV, pl.ds(pl.multiple_of(start, bk), bk), :]
        s = lax.dot_general(ks, q_block(q_ref, head, half), NT, preferred_element_type=F32)
        e = jnp.exp2(s * c2 - m_ref[n])
        if diag:
            seen = lax.broadcasted_iota(jnp.int32, (bk, NQ), 0) <= lax.broadcasted_iota(jnp.int32, (bk, NQ), 1)
            e = jnp.where(seen, e, 0.0)
        pb[...] = e.astype(BF16)
        l_ref[n] += jnp.sum(e.reshape(-1, *l_ref.shape[1:]), axis=0)

    def values(i, pb):
        head, half, start = item(i)
        vt = vb_ref[head // PER_KV, :, pl.ds(pl.multiple_of(start, bk), bk)]
        acc_ref[head * 2 + half] += jnp.dot(vt, pb[...], preferred_element_type=F32)

    scores(0, pbufs[0])

    def body(g, carry):
        for u in range(depth):
            i = g * depth + u
            scores(i + 1, pbufs[(u + 1) % depth])
            values(i, pbufs[u])
        return carry

    trips = n_items // depth - 1
    lax.fori_loop(0, trips, body, 0)
    for u in range(depth):
        if u + 1 < depth:
            scores(trips * depth + u + 1, pbufs[u + 1])
        values(trips * depth + u, pbufs[u])


def prefix_kernel(q_ref, ka, va, kb, vb, acc_out, m_out, l_out, kbuf, vbuf, acc_ref, m_ref, l_ref, pa, pb, sems, *, heads, c2):
    fetch = Fetch(sems)
    n = ka.shape[1]
    settle(fetch.start([(ka, kbuf.at[:, tile(0, n), :]), (va, vbuf.at[:, :, tile(0, n)]), (kb, kbuf.at[:, tile(1, n), :]), (vb, vbuf.at[:, :, tile(1, n)])]))

    @each(heads * 2)
    def _(i):
        head, half = i // 2, i % 2
        s = lax.dot_general(kbuf[head // PER_KV, tile(0, LANES), :], q_block(q_ref, head, half), NT, preferred_element_type=F32)
        m_ref[i] = jnp.max(s, axis=0, keepdims=True) * c2
        for ref in (acc_ref, l_ref):
            ref[i] = jnp.zeros(ref.shape[1:], F32)

    bk = 2 * NQ
    per = kbuf.shape[1] // bk

    def item(i):
        pair = i // per
        return pair // 2, pair % 2, (i % per) * bk

    attend_items(q_ref, kbuf, vbuf, acc_ref, m_ref, l_ref, (pa, pb), heads * 2 * per, item, bk, c2)
    settle(fetch.start([(acc_ref, acc_out), (m_ref, m_out), (l_ref, l_out)]))


def state_shapes(heads):
    return [struct((heads * 2, n, NQ), F32) for n in (LANES, 1, 8)]


def vmem_like(shapes):
    return [pltpu.VMEM(s.shape, s.dtype) for s in shapes]


def attend_prefix(q, pieces, c2):
    heads = q.shape[1] // LANES
    flat = [a for p in pieces for a in p]
    n = 2 * pieces[0][0].shape[1]
    shapes = state_shapes(heads)
    return pl.pallas_call(
        functools.partial(prefix_kernel, heads=heads, c2=c2),
        in_specs=[VMEM] + [HBM] * len(flat),
        out_specs=[HBM] * len(shapes),
        out_shape=[pltpu.HBM(s.shape, s.dtype) for s in shapes],
        scratch_shapes=[
            pltpu.VMEM((2, n, LANES), BF16), pltpu.VMEM((2, LANES, n), BF16), *vmem_like(shapes),
            *[pltpu.VMEM((2 * NQ, NQ), BF16)] * 2, pltpu.SemaphoreType.DMA((8,)),
        ],
        compiler_params=params(20),
        cost_estimate=cost(4 * q.size * n, 4 * q.size),
        name="attend_prefix",
    )(q, *flat)


def rest_kernel(*refs, group, groups, c2, axis):
    q_hbm, *refs = refs
    flat, refs = refs[:4 * groups], refs[4 * groups:]
    pairs = list(zip(flat[::2], flat[1::2]))
    pre, suf = pairs[:groups], pairs[groups:]
    acc_in, m_in, l_in, here_out, there_out, q_ref, kbuf, vbuf, ksuf, vsuf, acc_ref, m_ref, l_ref, acc_old, l_old, o_ref, bad_ref, sems, wa, wb, pa, pb, pc, pd = refs
    heads = PER_KV
    me = lax.axis_index(axis)
    fetch = Fetch(sems)
    mine = pl.ds(group * heads * 2, heads * 2)
    n_pre, n_suf = pre[0][0].shape[1], suf[0][0].shape[1]
    first = fetch.start([(q_hbm.at[:, tile(group, heads * LANES)], q_ref), (m_in.at[mine], m_ref)])
    for i, (kr, vr) in enumerate(pre[2:]):
        first += fetch.start([(kr.at[group], kbuf.at[0, tile(i, n_pre), :]), (vr.at[group], vbuf.at[0, :, tile(i, n_pre)])])
    second = []
    for i, (kr, vr) in enumerate(suf):
        second += fetch.start([(kr.at[group], ksuf.at[0, tile(i, n_suf), :]), (vr.at[group], vsuf.at[0, :, tile(i, n_suf)])])
    third = fetch.start([(acc_in.at[mine], acc_old), (l_in.at[mine], l_old)])
    for ref in (acc_ref, l_ref):
        ref[...] = jnp.zeros_like(ref)
    settle(first)
    bk = 2 * NQ
    per = kbuf.shape[1] // bk

    def pre_item(i):
        pair = i // per
        return pair // 2, pair % 2, (i % per) * bk

    attend_items(q_ref, kbuf, vbuf, acc_ref, m_ref, l_ref, (wa, wb), heads * 2 * per, pre_item, bk, c2)
    settle(second)
    last = 2 * groups - 1

    def locate(blk):
        late = (blk >= groups).astype(jnp.int32)
        owner = jnp.where(blk < groups, blk, last - blk)
        diff = (owner % 2 != me % 2).astype(jnp.int32) + 2 * (owner // 2 != me // 2).astype(jnp.int32)
        return (diff * 2 + late) * NQ

    def full_item(i):
        head, r = i // last, i % last
        half = (r >= me).astype(jnp.int32)
        return head, half, locate(jnp.where(r < me, r, r - me))

    def diag_item(i):
        half = i % 2
        return i // 2, half, locate(jnp.where(half == 0, me, last - me))

    attend_items(q_ref, ksuf, vsuf, acc_ref, m_ref, l_ref, (pa, pb, pc, pd), heads * last, full_item, NQ, c2)
    attend_items(q_ref, ksuf, vsuf, acc_ref, m_ref, l_ref, (pa, pb), heads * 2, diag_item, NQ, c2, diag=True)
    settle(third)
    bad_ref[...] = jnp.zeros_like(bad_ref)
    chunk = ROWS_CH // 2

    def write(i, acc, total):
        head, half = i // 2, i % 2
        out = (acc * (1.0 / total)).T.astype(BF16)
        n_p = NQ // chunk
        for p in range(n_p):
            o_ref[p % 2, tile(half * (n_p // 2) + p // 2, chunk), tile(head, LANES)] = out[p * chunk:(p + 1) * chunk]

    @each(heads * 2)
    def _(i):
        acc = acc_ref[i] + acc_old[i]
        total = jnp.sum(l_ref[i] + l_old[i], axis=0, keepdims=True)
        bad = jnp.where((jnp.abs(acc) < jnp.inf) & (total < jnp.inf), 0.0, 1.0)
        for j in range(NQ // LANES):
            part = bad[:, j * LANES:(j + 1) * LANES]
            bad_ref[...] = jnp.maximum(bad_ref[...], jnp.max(part.reshape(-1, *bad_ref.shape), axis=0))
        write(i, acc, total)

    @pl.when(jnp.max(bad_ref[...]) > 0.0)
    def _():
        @each(heads * 2)
        def _(i):
            head, half = i // 2, i % 2
            q = q_block(q_ref, head, half)
            m_ref[i] = jnp.full((1, NQ), -jnp.inf, F32)
            for ref in (acc_ref, l_ref):
                ref[i] = jnp.zeros(ref.shape[1:], F32)

            def update(ks, vt, seen):
                s = lax.dot_general(ks, q, NT, preferred_element_type=F32) * c2
                if seen is not None:
                    s = jnp.where(seen, s, -jnp.inf)
                m_old = m_ref[i]
                m_new = jnp.maximum(m_old, jnp.max(s, axis=0, keepdims=True))
                alpha = jnp.exp2(m_old - m_new)
                e = jnp.exp2(s - m_new)
                m_ref[i] = m_new
                l_ref[i] = l_ref[i] * alpha + jnp.sum(e.reshape(-1, *l_ref.shape[1:]), axis=0)
                acc_ref[i] = acc_ref[i] * alpha + jnp.dot(vt, e.astype(BF16), preferred_element_type=F32)

            kpre, vpre = pa.at[:, tile(0, LANES)], pb.at[tile(0, LANES), :]
            for kr, vr in pre:
                @each(n_pre // NQ)
                def _(j):
                    pltpu.sync_copy(kr.at[group, tile(j, NQ), :], kpre)
                    pltpu.sync_copy(vr.at[group, :, tile(j, NQ)], vpre)
                    update(kpre[...], vpre[...], None)

            mine_blk = jnp.where(half == 0, me, last - me)

            @each(2 * groups)
            def _(blk):
                @pl.when(blk <= mine_blk)
                def _():
                    start = pl.ds(pl.multiple_of(locate(blk), NQ), NQ)
                    seen = (lax.broadcasted_iota(jnp.int32, (NQ, NQ), 0) <= lax.broadcasted_iota(jnp.int32, (NQ, NQ), 1)) | (blk < mine_blk)
                    update(ksuf[0, start, :], vsuf[0, :, start], seen)

            write(i, acc_ref[i], jnp.sum(l_ref[i], axis=0, keepdims=True))

    side = lax.axis_index('tp') // 2
    settle(fetch.start([(o_ref.at[side], here_out), (o_ref.at[1 - side], there_out)]))


def attend_rest(q, pre, suf, state, c2, axis, group):
    rows, groups, width = q.shape[0], len(suf), PER_KV * LANES
    n_pre, n_suf = 2 * pre[0][0].shape[1], groups * suf[0][0].shape[1]
    flat = [a for p in list(pre) + list(suf) for a in p]
    acc, m, total = state_shapes(PER_KV)
    out = pltpu.HBM((rows // 2, width), BF16)
    return pl.pallas_call(
        functools.partial(rest_kernel, group=group, groups=groups, c2=c2, axis=axis),
        in_specs=[IN_HBM] + [HBM] * len(flat) + [IN_HBM] * 3,
        out_specs=[HBM] * 2,
        out_shape=[out] * 2,
        scratch_shapes=[
            pltpu.VMEM((rows, width), BF16), pltpu.VMEM((1, n_pre, LANES), BF16), pltpu.VMEM((1, LANES, n_pre), BF16),
            pltpu.VMEM((1, n_suf, LANES), BF16), pltpu.VMEM((1, LANES, n_suf), BF16), *vmem_like([acc, m, total, acc, total, struct((2, rows // 2, width), BF16)]),
            pltpu.VMEM((8, LANES), F32), pltpu.SemaphoreType.DMA((22,)), *[pltpu.VMEM((2 * NQ, NQ), BF16)] * 2, *[pltpu.VMEM((NQ, NQ), BF16)] * 4,
        ],
        compiler_params=params(20),
        cost_estimate=cost(2 * rows * width * (2 * n_pre + n_suf), 4 * q.size),
        name="attend_rest",
    )(q, *flat, *state)


def swap(arrays, axis, groups, bit):
    return tuple(lax.ppermute(a, axis, [(i, i ^ bit) for i in range(groups)]) for a in arrays)


def attend(q, own_pre, near_pre, far_pre, own_suf, near_suf, far_suf, wo_z, c2, groups, tps, dps):
    state = attend_prefix(q, (own_pre, near_pre), c2)
    far_pre, far_suf, wo_z, state = lax.optimization_barrier((far_pre, far_suf, wo_z, state))
    cross_pre = swap(far_pre, 'cp', groups, 1)
    cross_suf = swap(far_suf, 'cp', groups, 1)
    wo = jnp.stack(wo_z)
    wo_x, = swap((wo,), 'dp', dps, 1)
    wo_y, = swap((wo,), 'cp', groups, 2)
    pre, suf = (own_pre, near_pre, far_pre, cross_pre), (own_suf, near_suf, far_suf, cross_suf)
    here, there = attend_rest(q, pre, suf, state, c2, 'cp', 0)
    o_got = tuple(lax.ppermute(a, 'tp', [(i, i ^ d) for i in range(tps)]) for d, a in ((1, here), (2, there), (3, there)))
    wo, wo_x, wo_y, there, q = lax.optimization_barrier((wo, wo_x, wo_y, there, q))
    wo_xy, = swap((wo_x,), 'cp', groups, 2)
    near = swap((wo, wo_x, wo_y), 'cp', groups, 1)
    o_last = attend_rest(q, pre, suf, state, c2, 'cp', 1)
    wo_xy, o_last = lax.optimization_barrier((wo_xy, o_last))
    return (here,) + o_got, o_last, (wo, wo_x, wo_y, wo_xy) + near + swap((wo_xy,), 'cp', groups, 1)


MESH = pl.DeviceIdType.MESH
DOT_N = 512
MID_PLAN = ((('r3', -1),), (('xc', -3), ('r2', -1), ('hb', 1), ('ha', 1),), (('xb', -2), ('xa', -2),), (('O', 3),), (('r4', -1),), (), (('hc', 1), ('r1', 0),))
END_PLAN = ((('hw', 0), ('f', -2),), (('O', 3),), (), (), (), (), ())
AHEAD, BEHIND = 3, 3


def side_of(z):
    return lax.div(z, 2)


def colhalf_of(z):
    return lax.rem(lax.div(z + 1, 2), 2)


def line_kernel(*refs, nc):
    o_first, o_last, x_ref, wo_ref, *refs = refs[:4], refs[4:6], *refs[6:]
    wo_pieces, refs = refs[:8], refs[8:]
    wg_ref, wu_ref, wd_ref, gain_ref, xout_ref, land_ref = refs[:6]
    (obuf, h2, ybuf, ring, psum, act, stage, xs, xo, sstat, rstat,
     ring_sem, loc_sem, o_send, o_recv, st_send, st_recv, a1_send, a1_recv, rs_send, rs_recv, a2_send, a2_recv) = refs[6:]
    R, H = ROWS_CH, ROWS_CH // 2
    depth = wg_ref.shape[0]
    ff = wg_ref.shape[1]
    half = depth // 2
    width = o_last[0].shape[-1]
    kz = 2 * width
    n_ct = half // DOT_N
    nd, ne = ff // PAIR, depth // DOT_N
    per = 4 + nd + ne
    total_loads = nc * per
    big = 1024

    z = lax.axis_index('tp')
    dp = lax.axis_index('dp')
    cp = lax.axis_index('cp')
    core, chip = lax.rem(cp, 2), lax.div(cp, 2)
    side, q = side_of(z), colhalf_of(z)
    is_mid = q == 1
    is_end = q != 1
    near = 1 + side
    outer = 3 * side
    inner = 2 - side
    far_end = 3 - 3 * side
    peers = {1: z + 1 - 2 * lax.rem(z, 2), 2: lax.rem(z + 2, 4), 3: 3 - z}
    mate = peers[1]

    def rdma(src, dst, ssem, rsem, dev):
        return pltpu.make_async_remote_copy(src_ref=src, dst_ref=dst, send_sem=ssem, recv_sem=rsem, device_id={'tp': dev}, device_id_type=MESH)

    def rows_at(zz):
        return tile(side_of(zz), H)

    def cols_at(zz):
        return tile(colhalf_of(zz), half)

    barrier = pltpu.get_barrier_semaphore()
    for d in (1, 2, 3):
        pl.semaphore_signal(barrier, inc=1, device_id={'tp': peers[d]}, device_id_type=MESH)
    pl.semaphore_wait(barrier, 3)

    def load_kind(ld):
        u = ld + (per - 4)
        i1 = lax.div(u, per)
        a = lax.div(i1 + big - 1, big)
        t = lax.rem(u, per) + 4 * lax.div(i1, nc)
        return a * t + (1 - a) * ld

    def issue(ld):
        slot = lax.rem(ld, 3)
        sem = ring_sem.at[slot]
        t = load_kind(ld)

        def start(src, dst):
            pltpu.make_async_copy(src, dst, sem).start()

        for d in range(4):
            @pl.when(t == d)
            def _():
                @each(n_ct)
                def _(ct):
                    c0 = pl.multiple_of(ct * DOT_N, DOT_N)
                    if d == 0:
                        cs = tile(q * n_ct + ct, DOT_N)
                        start(wo_ref.at[:, cs], ring.at[slot, tile(ct, kz), :])
                    else:
                        for k, piece in enumerate(wo_pieces):
                            bits = (dp, k % 2), (chip, k // 2 % 2), (core, k // 4)
                            n = piece.shape[1]
                            j = sum((own + x - 2 * own * x) * w for (own, x), w in zip(bits, (4, 2, 1)))
                            r0 = pl.multiple_of(ct * kz + j * n, n)
                            start(piece.at[d - 1, :, pl.ds(c0, DOT_N)], ring.at[slot, pl.ds(r0, n), :])

        @pl.when((t >= 4) & (t < 4 + nd))
        def _():
            cs = pl.ds(pl.multiple_of((t - 4) * 256, 256), 256)
            start(wg_ref.at[:, cs], ring.at[slot, :depth, :PAIR])
            start(wu_ref.at[:, cs], ring.at[slot, :depth, PAIR:])

        @pl.when(t >= 4 + nd)
        def _():
            cs = pl.ds(pl.multiple_of((t - 4 - nd) * DOT_N, DOT_N), DOT_N)
            start(wd_ref.at[:, cs], ring.at[slot, :ff, :])

    def take(ld, n_rows):
        slot = lax.rem(ld, 3)
        whole = ring.at[slot, :n_rows, :]
        pltpu.make_async_copy(whole, whole, ring_sem.at[slot]).wait()
        pl.when(ld + 2 < total_loads)(lambda: issue(ld + 2))
        return slot

    def late(c, d):
        return obuf.at[c, d, :, tile(1, width)]

    def o_copy(c, d):
        return rdma(o_last[int(d > 1)].at[tile(c, H), :], late(c, d), o_send.at[c, d - 1], o_recv.at[c, d - 1], peers[d])

    def o_start(c):
        for d in (1, 2, 3):
            o_copy(c, d).start()

    def project(c, ld0):
        own_o = pltpu.make_async_copy(o_last[0].at[tile(c, H), :], late(c, 0), loc_sem.at[0])
        own_x = pltpu.make_async_copy(x_ref.at[tile(c * 2 + side, H), cols_at(z)], xs, loc_sem.at[1])
        own_o.start()
        own_x.start()
        for d in (1, 2, 3):
            o_copy(c, d).wait_recv()
        own_o.wait()
        own_x.wait()

        @each(n_ct)
        def _(ct):
            cs = tile(ct, DOT_N)
            ybuf[c, :, cs] = xs[:, cs].astype(F32)

        @each(4)
        def _(d):
            slot = take(ld0 + d, n_ct * kz)

            @each(n_ct)
            def _(ct):
                cs = tile(ct, DOT_N)
                w = ring[slot, tile(ct, kz), :]
                ybuf[c, :, cs] += jnp.dot(obuf[c, d], w, preferred_element_type=F32)

        sstat[c] = jnp.zeros((H, LANES), F32)

        @each(n_ct)
        def _(ct):
            yv = ybuf[c, :, tile(ct, DOT_N)]
            sstat[c] += jnp.broadcast_to(jnp.sum(yv * yv, axis=-1, keepdims=True), (H, LANES))

        swap_stat = rdma(sstat.at[c], rstat.at[c], st_send.at[c, 0], st_recv.at[c, 0], mate)
        swap_stat.start()
        swap_stat.wait_recv()
        inv = lax.rsqrt((sstat[c] + rstat[c])[:, 0:1] * (1.0 / depth) + NORM_EPS)

        @each(n_ct)
        def _(ct):
            cs = tile(ct, DOT_N)
            gs = tile(q * n_ct + ct, DOT_N)
            h2[c, rows_at(z), gs] = (ybuf[c, :, cs] * inv * gain_ref[:, gs].astype(F32)).astype(BF16)

    class Spread:
        def __init__(self, block, send, recv, own=None):
            self.block, self.send, self.recv, self.own = block, send, recv, own

        def copy(self, c, zz, s, r, dev, own=False):
            src = self.own(c) if own and self.own is not None else self.block(c, zz)
            return rdma(src, self.block(c, zz), self.send.at[c, s], self.recv.at[c, r], dev)

        def to_near(self, c):
            return self.copy(c, z, 0, 0, near, own=True)

        def to_outer(self, c):
            return self.copy(c, z, 0, 0, outer, own=True)

        def to_inner(self, c):
            return self.copy(c, z, 1, 1, inner, own=True)

        def end_to_inner(self, c):
            return self.copy(c, outer, 2, 2, inner)

        def inner_to_outer(self, c):
            return self.copy(c, inner, 3, 1, outer)

        def far_to_outer(self, c):
            return self.copy(c, far_end, 4, 2, outer)

        def start(self, c):
            pl.when(is_end)(lambda: self.to_near(c).start())

            @pl.when(is_mid)
            def _():
                self.to_outer(c).start()
                self.to_inner(c).start()

        def wait(self, c, r):
            self.copy(c, z, 0, r, mate).wait_recv()

        def serve(self, r, c):
            self.wait(c, r)
            (self.end_to_inner, self.inner_to_outer, self.far_to_outer)[r](c).start()

        def drain(self, c):
            @pl.when(is_end)
            def _():
                self.to_near(c).wait_send()

            @pl.when(is_mid)
            def _():
                for copy in (self.to_outer(c), self.to_inner(c), self.end_to_inner(c), self.inner_to_outer(c), self.far_to_outer(c)):
                    copy.wait_send()

    hidden = Spread(lambda c, zz: h2.at[c, rows_at(zz), cols_at(zz)], a1_send, a1_recv)

    def out_block(c, zz):
        return xout_ref.at[tile(c * 2 + side_of(zz), H), cols_at(zz)]

    done = Spread(out_block, a2_send, a2_recv, own=lambda c: xo.at[c])

    def gate_up(c, ld0, active, after):
        @each(nd)
        def _(i):
            @pl.when(active)
            def _():
                slot = take(ld0 + i, depth)
                gu = jnp.dot(h2[c], ring[slot, :depth, :], preferred_element_type=F32)
                g, u = gu[:, :PAIR], gu[:, PAIR:]
                act[:, tile(i, PAIR)] = (g * (1.0 / (1.0 + jnp.exp(-g))) * u).astype(BF16)

            for k in range(4):
                pl.when(i == (k + 1) * nd // 4 - 1)(functools.partial(after, k + 1))

    def ps_copy(c, k_send, zz, k_recv, dev):
        return rdma(psum.at[lax.rem(c, 2), zz], land_ref.at[c, k_recv], rs_send.at[c, k_send], rs_recv.at[c, k_recv], dev)

    def sums_out(c):
        ends = (ps_copy(c, 0, far_end, 0, near), ps_copy(c, 1, inner, 2, near), ps_copy(c, 2, near, 3, near))
        mids = (ps_copy(c, 0, far_end, 1, inner), ps_copy(c, 1, outer, 0, outer), ps_copy(c, 2, inner, 4, inner))
        return ends, mids

    def wait_sums_out(c):
        ends, mids = sums_out(c)
        for flag, copies in ((is_end, ends), (is_mid, mids)):
            @pl.when(flag)
            def _():
                for copy in copies:
                    copy.wait_send()

    def down(c, ld0, part):
        ps = lax.rem(c, 2)
        ends, _ = sums_out(c)
        if part == 0:
            pl.when(c >= 2)(lambda: wait_sums_out(c - 2))

        @each(ne // 2)
        def _(i):
            slot = take(ld0 + part * (ne // 2) + i, ff)
            pv = jnp.dot(act[...], ring[slot, :ff, :], preferred_element_type=F32)
            cs = tile(i, DOT_N)
            psum[ps, part, :, cs] = pv[:H]
            psum[ps, 3 - part, :, cs] = pv[H:R]

        @pl.when(is_end)
        def _():
            for copy in (ends[:1], ends[1:])[part]:
                copy.start()

    def arrive(c, k, buf):
        ps_copy(c, 0, z, k, mate).wait_recv()
        copy = pltpu.make_async_copy(land_ref.at[c, k], stage.at[buf], loc_sem.at[2 + buf])
        copy.start()
        return copy

    def tiles(fn):
        @each(4)
        def _(i):
            fn(tile(i, H // 4))

    def pass_on(c, k, zz, send):
        arrive(c, k, 0).wait()

        def add(rs):
            psum[lax.rem(c, 2), zz, rs, :] += stage[0, rs, :]

        tiles(add)
        send.start()

    def finish(c, ks):
        for copy in [arrive(c, k, i) for i, k in enumerate(ks)]:
            copy.wait()

        def add(rs):
            v = psum[lax.rem(c, 2), z, rs, :] + stage[0, rs, :]
            if len(ks) == 2:
                v = v + stage[1, rs, :]
            xo[c, rs, :] = (ybuf[c, rs, :] + v).astype(BF16)

        tiles(add)
        done.start(c)
        pltpu.make_async_copy(xo.at[c], out_block(c, z), loc_sem.at[4]).start()
        pltpu.make_async_copy(xo.at[c], out_block(c, z), loc_sem.at[4]).wait()

    def relay(k, c):
        pass_on(c, k, (far_end, outer, inner)[k], sums_out(c)[1][k])

    def hidden_wait(c):
        for r in range(3):
            hidden.wait(c, r)

    steps = {'O': o_start, 'hw': hidden_wait, 'f': lambda c: finish(c, (0,)), 'r4': lambda c: finish(c, (3, 4))}
    for r in range(3):
        steps['h' + 'abc'[r]] = functools.partial(hidden.serve, r)
        steps['x' + 'abc'[r]] = functools.partial(done.serve, r)
        steps['r' + '123'[r]] = functools.partial(relay, r)

    early = [pltpu.make_async_copy(src, obuf.at[:, d, :, tile(0, width)], loc_sem.at[5 + d]) for d, src in enumerate(o_first)]
    for copy in early:
        copy.start()
    issue(jnp.int32(0))
    issue(jnp.int32(1))
    for copy in early:
        copy.wait()

    @each(AHEAD + nc + BEHIND)
    def _(t):
        j = t - AHEAD
        jj = j + 1
        active = (j >= 0) & (j < nc)

        def after(k):
            for flag, plan in ((is_mid, MID_PLAN[k]), (is_end, END_PLAN[k])):
                def run(plan=plan):
                    for name, ahead in plan:
                        c = j + ahead
                        pl.when((c >= 0) & (c < nc))(functools.partial(steps[name], c))

                if plan:
                    pl.when(flag)(run)

        @pl.when((jj >= 0) & (jj < nc))
        def _():
            project(jj, per * jj - (per - 4) * lax.div(jj + big - 1, big))
            hidden.start(jj)

        after(0)
        ld_d = per * jj - (per - 8) - 4 * lax.div(jj, nc)
        gate_up(j, ld_d, active, after)
        for part in range(2):
            pl.when(active)(lambda: down(j, ld_d + nd, part))
            after(5 + part)

    @each(nc)
    def _(c):
        @pl.when(is_end)
        def _():
            for r in range(3):
                done.wait(c, r)

        for d in (1, 2, 3):
            o_copy(c, d).wait_send()
        rdma(sstat.at[c], rstat.at[c], st_send.at[c, 0], st_recv.at[c, 0], mate).wait_send()
        hidden.drain(c)
        done.drain(c)
        pl.when(c >= nc - 2)(lambda: wait_sums_out(c))


def line_block(o_first, o_last, x, w_out, pieces, w_gate, w_up, w_down, gain):
    rows, depth = x.shape
    ff = w_gate.shape[1]
    width = o_last[0].shape[-1]
    kz = 2 * width
    nc = rows // ROWS_CH
    h, half = ROWS_CH // 2, depth // 2
    ring_rows = max(depth, ff, half // DOT_N * kz)
    sems = [pltpu.SemaphoreType.DMA((nc, n)) for n in (3, 3, 1, 1, 5, 3, 3, 5, 5, 3)]
    xout, _ = pl.pallas_call(
        functools.partial(line_kernel, nc=nc),
        in_specs=[HBM] * (11 + len(pieces)) + [VMEM],
        out_specs=[HBM] * 2,
        out_shape=[struct(x.shape, BF16), struct((nc, 5, h, half), F32)],
        scratch_shapes=[
            pltpu.VMEM((nc, 4, h, kz), BF16), pltpu.VMEM((nc, ROWS_CH, depth), BF16), pltpu.VMEM((nc, h, half), F32),
            pltpu.VMEM((3, ring_rows, DOT_N), BF16), pltpu.VMEM((2, 4, h, half), F32), pltpu.VMEM((ROWS_CH, ff), BF16),
            pltpu.VMEM((2, h, half), F32), pltpu.VMEM((h, half), BF16), pltpu.VMEM((nc, h, half), BF16),
            *[pltpu.VMEM((nc, h, LANES), F32)] * 2, pltpu.SemaphoreType.DMA((3,)), pltpu.SemaphoreType.DMA((9,)), *sems,
        ],
        compiler_params=params(60, collective_id=1, has_side_effects=True),
        cost_estimate=cost(6 * x.size * ff, 2 * x.size),
        name="line_block",
    )(*(a.reshape(nc, h, width) for a in o_first), *o_last, x, w_out, *pieces, w_gate, w_up, w_down, gain.reshape(1, depth))
    return xout


def copy_kernel(src_ref, dst_ref):
    dst_ref[...] = src_ref[...]


def copied(x):
    spec = pl.BlockSpec((LANES, x.shape[1]), lambda i: (i, 0))
    return pl.pallas_call(copy_kernel, grid=(x.shape[0] // LANES,), in_specs=[spec], out_specs=spec, out_shape=struct(x.shape, x.dtype), name="copied")(x)


def gather_w_out(w_out, tps):
    z, dp, cp = (lax.axis_index(a) for a in ('tp', 'dp', 'cp'))
    n, half = w_out.shape[0] // 8, w_out.shape[1] // 2
    q = (z + 1) // 2 % 2
    part = lax.dynamic_slice_in_dim(w_out, (dp * 4 + cp) * n, n, 0)
    same, other = (lax.dynamic_slice_in_dim(part, h * half, half, 1) for h in (q, 1 - q))
    return tuple(lax.ppermute(a, 'tp', [(i, i ^ d) for i in range(tps)]) for d, a in ((1, other), (2, other), (3, same)))


def solution(mesh):
    groups = mesh.shape['cp']
    tps = mesh.shape['tp']
    dps = mesh.shape['dp']

    def local_layer(x_loc, kp_loc, vp_loc, norm_attn, w_query, w_key, w_value, w_out, norm_mlp, w_gate, w_up, w_down):
        rows = x_loc.shape[0]
        pre_dev, kv_loc, head_dim = kp_loc.shape
        c2 = head_dim ** -0.5 * math.log2(math.e)
        me = lax.axis_index('cp')
        q_pos = block_positions(me, groups, rows // 2, pre_dev * groups)
        own_pre = (kp_loc.transpose(1, 0, 2), vp_loc.transpose(1, 2, 0))
        far_pre = swap(own_pre, 'cp', groups, 2)
        near_pre = swap(own_pre, 'cp', groups, 1)
        wo_z = gather_w_out(w_out, tps)
        cos_tab, sin_tab = rope_tables(q_pos, head_dim)
        q, k_new, vt_new, k_flat, v_flat = qkv(x_loc, norm_attn, w_query, w_key, w_value, cos_tab, sin_tab)
        own_suf = (k_new, vt_new)
        far_suf = swap(own_suf, 'cp', groups, 2)
        near_suf = swap(own_suf, 'cp', groups, 1)
        o_first, o_last, wo_pieces = attend(q, own_pre, near_pre, far_pre, own_suf, near_suf, far_suf, wo_z, c2, groups, tps, dps)
        x_out = line_block(o_first, o_last, x_loc, w_out, wo_pieces, w_gate, w_up, w_down, norm_mlp)
        x_out = copied(x_out)
        return x_out, k_flat.reshape(rows, kv_loc, head_dim), v_flat.reshape(rows, kv_loc, head_dim)

    row_spec = P(('dp', 'cp'), None)
    kv_spec = P(('dp', 'cp'), 'tp', None)
    col_spec = P(None, 'tp')
    row_split = P('tp', None)
    vec_spec = P(None)
    return jax.shard_map(local_layer, mesh=mesh, in_specs=(row_spec, kv_spec, kv_spec, vec_spec, col_spec, col_spec, col_spec, row_split, vec_spec, col_spec, col_spec, row_split), out_specs=(row_spec, kv_spec, kv_spec), check_vma=False)
```

```python
import functools
import math

import jax
import jax.numpy as jnp
from jax import lax
from jax.experimental import pallas as pl
from jax.experimental.pallas import tpu as pltpu
from jax.sharding import PartitionSpec as P


ROPE_THETA = 500000.0
NORM_EPS = 1e-5
ROWS_CH = 128
F32 = jnp.float32
BF16 = jnp.bfloat16
HBM = pl.BlockSpec(memory_space=pl.ANY)
VMEM = pl.BlockSpec(memory_space=pltpu.VMEM)
IN_HBM = pl.BlockSpec(memory_space=pltpu.HBM)
LANES = 128
PAIR = 2 * LANES
NT = (((1,), (1,)), ((), ()))
each = functools.partial(pl.loop, 0)


def tile(i, n):
    return pl.ds(pl.multiple_of(i * n, n), n)


def params(mib, **more):
    return pltpu.CompilerParams(vmem_limit_bytes=mib * 2**20, **more)


def cost(flops, moved):
    return pl.CostEstimate(flops=flops, bytes_accessed=moved, transcendentals=0)


def struct(shape, dtype):
    return jax.ShapeDtypeStruct(shape, dtype)


def block_positions(owner, groups, blk_len, prefix_len):
    local_row = jnp.arange(2 * blk_len, dtype=jnp.int32)
    blk_idx = jnp.where(local_row < blk_len, owner, 2 * groups - 1 - owner)
    return prefix_len + blk_idx * blk_len + local_row % blk_len


def rope_tables(positions, head_dim):
    inv_freq = ROPE_THETA ** (-jnp.arange(0, head_dim, 2, dtype=F32) / head_dim)
    angles = positions.astype(F32)[:, None] * inv_freq[None, :]
    cos_tab, sin_tab = jnp.cos(angles), jnp.sin(angles)
    return jnp.concatenate([cos_tab, cos_tab], axis=1), jnp.concatenate([-sin_tab, sin_tab], axis=1)


def qkv_kernel(x_hbm, g_ref, wq_ref, wk_ref, wv_ref, cos_ref, sin_ref, q_ref, kv_ref, kf_ref, vf_ref, x_ref, h_ref, sems, *, nq):
    step = pl.program_id(0)
    rows = x_ref.shape[0]
    parts, rt = sems.shape[0], 32

    @pl.when(step == 0)
    def _():
        n = rows // parts
        copies = [pltpu.make_async_copy(x_hbm.at[tile(i, n), :], x_ref.at[tile(i, n), :], sems.at[i]) for i in range(parts)]
        for copy in copies:
            copy.start()
        for i, copy in enumerate(copies):
            copy.wait()

            @pl.loop(i * n // rt, (i + 1) * n // rt, unroll=2)
            def _(j):
                sl = tile(j, rt)
                xv = x_ref[sl, :].astype(F32)
                inv = lax.rsqrt(jnp.mean(xv * xv, axis=-1, keepdims=True) + NORM_EPS)
                h_ref[sl, :] = (xv * inv * g_ref[...].astype(F32)).astype(BF16)

    def rope(block, sl):
        return (block * cos_ref[sl, :] + pltpu.roll(block, 64, axis=1) * sin_ref[sl, :]).astype(BF16)

    mt = 512

    def project(w_ref, store):
        @each(rows // mt)
        def _(i):
            sl = tile(i, mt)
            acc = jnp.dot(h_ref[sl, :], w_ref[...], preferred_element_type=F32)
            store(acc, sl)

    def heads_of(acc):
        return [(t, slice(t * LANES, (t + 1) * LANES), acc[:, t * LANES:(t + 1) * LANES]) for t in range(2)]

    def store_q(acc, sl):
        for _, cs, part in heads_of(acc):
            q_ref[sl, cs] = rope(part, sl)

    def store_k(acc, sl):
        for t, cs, part in heads_of(acc):
            kf_ref[sl, cs] = rope(part, sl)
            kv_ref[0, t, sl, :] = kf_ref[sl, cs]

    def store_v(acc, sl):
        vf_ref[sl, :] = acc.astype(BF16)
        for t, _, part in heads_of(acc):
            for b in range(mt // LANES):
                kv_ref[1, t, pl.ds(sl.start + b * LANES, LANES), :] = part[b * LANES:(b + 1) * LANES].T.astype(BF16)

    pl.when(step < nq)(lambda: project(wq_ref, store_q))
    pl.when(step == nq)(lambda: project(wk_ref, store_k))
    pl.when(step == nq + 1)(lambda: project(wv_ref, store_v))


def qkv(x, gain, wq, wk, wv, cos_tab, sin_tab):
    rows, depth = x.shape
    nq = wq.shape[1] // PAIR

    def fixed(shape):
        return pl.BlockSpec(shape, lambda j: tuple(0 for _ in shape))

    def whole(shape):
        return pl.BlockSpec(shape, lambda j: tuple(0 for _ in shape), pipeline_mode=pl.Buffered(1))

    def columns(n):
        return pl.BlockSpec((n, PAIR), lambda j: (0, jnp.minimum(j, nq - 1)))

    flat, by_head = (rows, PAIR), (2, 2, rows, LANES)
    return pl.pallas_call(
        functools.partial(qkv_kernel, nq=nq),
        grid=(nq + 2,),
        in_specs=[HBM, whole((1, depth)), columns(depth), fixed(wk.shape), fixed(wv.shape), whole(cos_tab.shape), whole(sin_tab.shape)],
        out_specs=[columns(rows), fixed(by_head), fixed(flat), fixed(flat)],
        out_shape=[struct(s, BF16) for s in ((rows, nq * PAIR), by_head, flat, flat)],
        scratch_shapes=[pltpu.VMEM((rows, depth), BF16), pltpu.VMEM((rows, depth), BF16), pltpu.SemaphoreType.DMA((4,))],
        compiler_params=params(56, dimension_semantics=("arbitrary",)),
        cost_estimate=cost(2 * rows * depth * (nq + 2) * PAIR, 2 * depth * rows),
        name="qkv",
    )(x, gain.reshape(1, depth), wq, wk, wv, cos_tab, sin_tab)


NQ = 512
PER_KV = 4


class Fetch:
    def __init__(self, sems):
        self.sems, self.used = sems, 0

    def start(self, pairs):
        copies = []
        for src, dst in pairs:
            copies.append(pltpu.make_async_copy(src, dst, self.sems.at[self.used]))
            self.used += 1
        for copy in copies:
            copy.start()
        return copies


def settle(copies):
    for copy in copies:
        copy.wait()


def q_block(q_ref, head, half):
    return q_ref[tile(half, NQ), tile(head, LANES)]


def across(blocks):
    return jnp.concatenate([blocks[i:i + LANES] for i in range(0, blocks.shape[0], LANES)], axis=1)


def attend_items(q_ref, kb_ref, vb_ref, acc_ref, m_ref, l_ref, pbufs, n_items, item, bk, c2, diag=False):
    depth = len(pbufs)

    def scores(i, pb):
        head, half, start = item(i)
        n = head * 2 + half
        ks = kb_ref[head // PER_KV, pl.ds(pl.multiple_of(start, bk), bk), :]
        s = lax.dot_general(ks, q_block(q_ref, head, half), NT, preferred_element_type=F32)
        e = jnp.exp2(s * c2 - m_ref[n])
        if diag:
            seen = lax.broadcasted_iota(jnp.int32, (bk, NQ), 0) <= lax.broadcasted_iota(jnp.int32, (bk, NQ), 1)
            e = jnp.where(seen, e, 0.0)
        pb[...] = e.astype(BF16)
        l_ref[n] += jnp.sum(e.reshape(-1, *l_ref.shape[1:]), axis=0)

    def values(i, pb):
        head, half, start = item(i)
        vt = across(vb_ref[head // PER_KV, pl.ds(pl.multiple_of(start, bk), bk), :])
        acc_ref[head * 2 + half] += jnp.dot(vt, pb[...], preferred_element_type=F32)

    scores(0, pbufs[0])

    def body(g, carry):
        for u in range(depth):
            i = g * depth + u
            scores(i + 1, pbufs[(u + 1) % depth])
            values(i, pbufs[u])
        return carry

    trips = n_items // depth - 1
    lax.fori_loop(0, trips, body, 0)
    for u in range(depth):
        if u + 1 < depth:
            scores(trips * depth + u + 1, pbufs[u + 1])
        values(trips * depth + u, pbufs[u])


def prefix_kernel(q_ref, ka, va, kb, vb, acc_out, m_out, l_out, kbuf, vbuf, acc_ref, m_ref, l_ref, pa, pb, sems, *, heads, c2):
    fetch = Fetch(sems)
    n = ka.shape[1]
    settle(fetch.start([(ka, kbuf.at[:, tile(0, n), :]), (va, vbuf.at[:, tile(0, n), :]), (kb, kbuf.at[:, tile(1, n), :]), (vb, vbuf.at[:, tile(1, n), :])]))

    @each(heads // PER_KV)
    def _(group):
        for j in range(2 * PER_KV):
            i = group * 2 * PER_KV + j
            s = lax.dot_general(kbuf[group, tile(0, LANES), :], q_block(q_ref, i // 2, j % 2), NT, preferred_element_type=F32)
            m_ref[i] = jnp.max(s, axis=0, keepdims=True) * c2

    for ref in (acc_ref, l_ref):
        ref[...] = jnp.zeros_like(ref)
    bk = 2 * NQ
    per = kbuf.shape[1] // bk

    def item(i):
        pair = i // per
        return pair // 2, pair % 2, (i % per) * bk

    attend_items(q_ref, kbuf, vbuf, acc_ref, m_ref, l_ref, (pa, pb), heads * 2 * per, item, bk, c2)
    settle(fetch.start([(acc_ref, acc_out), (m_ref, m_out), (l_ref, l_out)]))


def state_shapes(heads):
    return [struct((heads * 2, n, NQ), F32) for n in (LANES, 1, 8)]


def vmem_like(shapes):
    return [pltpu.VMEM(s.shape, s.dtype) for s in shapes]


def attend_prefix(q, pieces, c2):
    heads = q.shape[1] // LANES
    flat = [a for p in pieces for a in p]
    n = 2 * pieces[0][0].shape[1]
    shapes = state_shapes(heads)
    return pl.pallas_call(
        functools.partial(prefix_kernel, heads=heads, c2=c2),
        in_specs=[VMEM] + [HBM] * len(flat),
        out_specs=[HBM] * len(shapes),
        out_shape=[pltpu.HBM(s.shape, s.dtype) for s in shapes],
        scratch_shapes=[
            *[pltpu.VMEM((2, n, LANES), BF16)] * 2, *vmem_like(shapes),
            *[pltpu.VMEM((2 * NQ, NQ), BF16)] * 2, pltpu.SemaphoreType.DMA((8,)),
        ],
        compiler_params=params(20),
        cost_estimate=cost(4 * q.size * n, 4 * q.size),
        name="attend_prefix",
    )(q, *flat)


def rest_kernel(*refs, group, groups, c2, axis):
    q_hbm, *refs = refs
    flat, suf, refs = refs[:2 * groups], refs[2 * groups:3 * groups], refs[3 * groups:]
    pre = list(zip(flat[::2], flat[1::2]))
    acc_in, m_in, l_in, here_out, there_out, q_ref, kbuf, vbuf, ksuf, vsuf, acc_ref, m_ref, l_ref, acc_old, l_old, o_ref, bad_ref, sems, wa, wb, pa, pb, pc, pd = refs
    heads = PER_KV
    me = lax.axis_index(axis)
    fetch = Fetch(sems)
    mine = pl.ds(group * heads * 2, heads * 2)
    n_pre, n_suf = pre[0][0].shape[1], suf[0].shape[2]
    first = fetch.start([(q_hbm.at[:, tile(group, heads * LANES)], q_ref), (m_in.at[mine], m_ref)])
    for i, (kr, vr) in enumerate(pre[2:]):
        first += fetch.start([(kr.at[group], kbuf.at[0, tile(i, n_pre), :]), (vr.at[group], vbuf.at[0, tile(i, n_pre), :])])
    second = []
    for i, kv in enumerate(suf):
        second += fetch.start([(kv.at[j, group], buf.at[0, tile(i, n_suf), :]) for j, buf in enumerate((ksuf, vsuf))])
    third = fetch.start([(acc_in.at[mine], acc_old), (l_in.at[mine], l_old)])
    for ref in (acc_ref, l_ref):
        ref[...] = jnp.zeros_like(ref)
    settle(first)
    bk = 2 * NQ
    per = kbuf.shape[1] // bk

    def pre_item(i):
        pair = i // per
        return pair // 2, pair % 2, (i % per) * bk

    attend_items(q_ref, kbuf, vbuf, acc_ref, m_ref, l_ref, (wa, wb), heads * 2 * per, pre_item, bk, c2)
    settle(second)
    last = 2 * groups - 1

    def locate(blk):
        late = (blk >= groups).astype(jnp.int32)
        owner = jnp.where(blk < groups, blk, last - blk)
        diff = (owner % 2 != me % 2).astype(jnp.int32) + 2 * (owner // 2 != me // 2).astype(jnp.int32)
        return (diff * 2 + late) * NQ

    def full_item(i):
        head, r = i // last, i % last
        half = (r >= me).astype(jnp.int32)
        return head, half, locate(jnp.where(r < me, r, r - me))

    def diag_item(i):
        half = i % 2
        return i // 2, half, locate(jnp.where(half == 0, me, last - me))

    attend_items(q_ref, ksuf, vsuf, acc_ref, m_ref, l_ref, (pa, pb, pc, pd), heads * last, full_item, NQ, c2)
    attend_items(q_ref, ksuf, vsuf, acc_ref, m_ref, l_ref, (pa, pb), heads * 2, diag_item, NQ, c2, diag=True)
    settle(third)
    bad_ref[...] = jnp.zeros_like(bad_ref)
    chunk = ROWS_CH // 2

    def write(i, acc, total):
        head, half = i // 2, i % 2
        out = (acc * (1.0 / total)).T.astype(BF16)
        n_p = NQ // chunk
        for p in range(n_p):
            o_ref[p % 2, tile(half * (n_p // 2) + p // 2, chunk), tile(head, LANES)] = out[p * chunk:(p + 1) * chunk]

    @each(heads * 2)
    def _(i):
        acc = acc_ref[i] + acc_old[i]
        total = jnp.sum(l_ref[i] + l_old[i], axis=0, keepdims=True)
        bad = jnp.where((jnp.abs(acc) < jnp.inf) & (total < jnp.inf), 0.0, 1.0)
        for j in range(NQ // LANES):
            part = bad[:, j * LANES:(j + 1) * LANES]
            bad_ref[...] = jnp.maximum(bad_ref[...], jnp.max(part.reshape(-1, *bad_ref.shape), axis=0))
        write(i, acc, total)

    @pl.when(jnp.max(bad_ref[...]) > 0.0)
    def _():
        @each(heads * 2)
        def _(i):
            head, half = i // 2, i % 2
            q = q_block(q_ref, head, half)
            m_ref[i] = jnp.full((1, NQ), -jnp.inf, F32)
            for ref in (acc_ref, l_ref):
                ref[i] = jnp.zeros(ref.shape[1:], F32)

            def update(ks, vt, seen):
                s = lax.dot_general(ks, q, NT, preferred_element_type=F32) * c2
                if seen is not None:
                    s = jnp.where(seen, s, -jnp.inf)
                m_old = m_ref[i]
                m_new = jnp.maximum(m_old, jnp.max(s, axis=0, keepdims=True))
                alpha = jnp.exp2(m_old - m_new)
                e = jnp.exp2(s - m_new)
                m_ref[i] = m_new
                l_ref[i] = l_ref[i] * alpha + jnp.sum(e.reshape(-1, *l_ref.shape[1:]), axis=0)
                acc_ref[i] = acc_ref[i] * alpha + jnp.dot(vt, e.astype(BF16), preferred_element_type=F32)

            kpre, vpre = (p.at[:, tile(0, LANES)] for p in (pa, pb))
            for kr, vr in pre:
                @each(n_pre // NQ)
                def _(j):
                    pltpu.sync_copy(kr.at[group, tile(j, NQ), :], kpre)
                    pltpu.sync_copy(vr.at[group, tile(j, NQ), :], vpre)
                    update(kpre[...], across(vpre[...]), None)

            mine_blk = jnp.where(half == 0, me, last - me)

            @each(2 * groups)
            def _(blk):
                @pl.when(blk <= mine_blk)
                def _():
                    start = pl.ds(pl.multiple_of(locate(blk), NQ), NQ)
                    seen = (lax.broadcasted_iota(jnp.int32, (NQ, NQ), 0) <= lax.broadcasted_iota(jnp.int32, (NQ, NQ), 1)) | (blk < mine_blk)
                    update(ksuf[0, start, :], across(vsuf[0, start, :]), seen)

            write(i, acc_ref[i], jnp.sum(l_ref[i], axis=0, keepdims=True))

    side = lax.axis_index('tp') // 2
    settle(fetch.start([(o_ref.at[side], here_out), (o_ref.at[1 - side], there_out)]))


def attend_rest(q, pre, suf, state, c2, axis, group):
    rows, groups, width = q.shape[0], len(suf), PER_KV * LANES
    n_pre, n_suf = 2 * pre[0][0].shape[1], groups * suf[0].shape[2]
    flat = [a for p in pre for a in p] + list(suf)
    acc, m, total = state_shapes(PER_KV)
    out = pltpu.HBM((rows // 2, width), BF16)
    return pl.pallas_call(
        functools.partial(rest_kernel, group=group, groups=groups, c2=c2, axis=axis),
        in_specs=[IN_HBM] + [HBM] * len(flat) + [IN_HBM] * 3,
        out_specs=[HBM] * 2,
        out_shape=[out] * 2,
        scratch_shapes=[
            pltpu.VMEM((rows, width), BF16), *[pltpu.VMEM((1, n, LANES), BF16) for n in (n_pre, n_pre, n_suf, n_suf)], *vmem_like([acc, m, total, acc, total, struct((2, rows // 2, width), BF16)]),
            pltpu.VMEM((8, LANES), F32), pltpu.SemaphoreType.DMA((22,)), *[pltpu.VMEM((2 * NQ, NQ), BF16)] * 2, *[pltpu.VMEM((NQ, NQ), BF16)] * 4,
        ],
        compiler_params=params(20),
        cost_estimate=cost(2 * rows * width * (2 * n_pre + n_suf), 4 * q.size),
        name="attend_rest",
    )(q, *flat, *state)


def swap(arrays, axis, groups, bit):
    return tuple(lax.ppermute(a, axis, [(i, i ^ bit) for i in range(groups)]) for a in arrays)


def attend(q, own_pre, near_pre, far_pre, own_suf, near_suf, far_suf, wo_z, c2, groups, tps, dps):
    state = attend_prefix(q, (own_pre, near_pre), c2)
    far_pre, far_suf, wo_z, state = lax.optimization_barrier((far_pre, far_suf, wo_z, state))
    cross_pre = swap(far_pre, 'cp', groups, 1)
    cross_suf, = swap((far_suf,), 'cp', groups, 1)
    wo = jnp.stack(wo_z)
    wo_x, = swap((wo,), 'dp', dps, 1)
    wo_y, = swap((wo,), 'cp', groups, 2)
    pre, suf = (own_pre, near_pre, far_pre, cross_pre), (own_suf, near_suf, far_suf, cross_suf)
    here, there = attend_rest(q, pre, suf, state, c2, 'cp', 0)
    o_got = tuple(lax.ppermute(a, 'tp', [(i, i ^ d) for i in range(tps)]) for d, a in ((1, here), (2, there), (3, there)))
    wo, wo_x, wo_y, there, q = lax.optimization_barrier((wo, wo_x, wo_y, there, q))
    wo_xy, = swap((wo_x,), 'cp', groups, 2)
    near = swap((wo, wo_x, wo_y), 'cp', groups, 1)
    o_last = attend_rest(q, pre, suf, state, c2, 'cp', 1)
    wo_xy, o_last = lax.optimization_barrier((wo_xy, o_last))
    return (here,) + o_got, o_last, (wo, wo_x, wo_y, wo_xy) + near + swap((wo_xy,), 'cp', groups, 1)


MESH = pl.DeviceIdType.MESH
DOT_N = 512
SLOTS = 6
MID_PLAN = ((('r3', -1),), (('xc', -3), ('r2', -1), ('hb', 1), ('ha', 1),), (('xb', -2), ('xa', -2),), (('O', 3),), (('r4', -1),), (), (('hc', 1), ('r1', 0),))
END_PLAN = ((('hw', 0), ('f', -2),), (('O', 3),), (), (), (), (), ())
AHEAD, BEHIND = 3, 3


def side_of(z):
    return lax.div(z, 2)


def colhalf_of(z):
    return lax.rem(lax.div(z + 1, 2), 2)


def line_kernel(*refs, nc):
    o_first, o_last, x_ref, wo_ref, *refs = refs[:4], refs[4:6], *refs[6:]
    wo_pieces, refs = refs[:8], refs[8:]
    wg_ref, wu_ref, wd_ref, gain_ref, xout_ref, land_ref = refs[:6]
    (obuf, h2, ybuf, ring, psum, act, stage, xs, xo, sstat, rstat,
     ring_sem, loc_sem, o_send, o_recv, st_send, st_recv, a1_send, a1_recv, rs_send, rs_recv, a2_send, a2_recv) = refs[6:]
    R, H = ROWS_CH, ROWS_CH // 2
    depth = wg_ref.shape[0]
    ff = wg_ref.shape[1]
    half = depth // 2
    width = o_last[0].shape[-1]
    kz = 2 * width
    n_ct = half // DOT_N
    nd, ne = ff // PAIR, depth // DOT_N
    per = 4 + nd + ne
    total_loads = nc * per
    big = 1024

    z = lax.axis_index('tp')
    dp = lax.axis_index('dp')
    cp = lax.axis_index('cp')
    core, chip = lax.rem(cp, 2), lax.div(cp, 2)
    side, q = side_of(z), colhalf_of(z)
    is_mid = q == 1
    is_end = q != 1
    near = 1 + side
    outer = 3 * side
    inner = 2 - side
    far_end = 3 - 3 * side
    peers = {1: z + 1 - 2 * lax.rem(z, 2), 2: lax.rem(z + 2, 4), 3: 3 - z}
    mate = peers[1]

    def rdma(src, dst, ssem, rsem, dev):
        return pltpu.make_async_remote_copy(src_ref=src, dst_ref=dst, send_sem=ssem, recv_sem=rsem, device_id={'tp': dev}, device_id_type=MESH)

    def rows_at(zz):
        return tile(side_of(zz), H)

    def cols_at(zz):
        return tile(colhalf_of(zz), half)

    barrier = pltpu.get_barrier_semaphore()
    for d in (1, 2, 3):
        pl.semaphore_signal(barrier, inc=1, device_id={'tp': peers[d]}, device_id_type=MESH)
    pl.semaphore_wait(barrier, 3)

    def load_kind(ld):
        u = ld + (per - 4)
        i1 = lax.div(u, per)
        a = lax.div(i1 + big - 1, big)
        t = lax.rem(u, per) + 4 * lax.div(i1, nc)
        return a * t + (1 - a) * ld

    def issue(ld):
        slot = lax.rem(ld, SLOTS)
        sem = ring_sem.at[slot]
        t = load_kind(ld)

        def start(src, dst):
            pltpu.make_async_copy(src, dst, sem).start()

        for d in range(4):
            @pl.when(t == d)
            def _():
                @each(n_ct)
                def _(ct):
                    c0 = pl.multiple_of(ct * DOT_N, DOT_N)
                    if d == 0:
                        cs = tile(q * n_ct + ct, DOT_N)
                        start(wo_ref.at[:, cs], ring.at[slot, tile(ct, kz), :])
                    else:
                        for k, piece in enumerate(wo_pieces):
                            bits = (dp, k % 2), (chip, k // 2 % 2), (core, k // 4)
                            n = piece.shape[1]
                            j = sum((own + x - 2 * own * x) * w for (own, x), w in zip(bits, (4, 2, 1)))
                            r0 = pl.multiple_of(ct * kz + j * n, n)
                            start(piece.at[d - 1, :, pl.ds(c0, DOT_N)], ring.at[slot, pl.ds(r0, n), :])

        @pl.when((t >= 4) & (t < 4 + nd))
        def _():
            cs = pl.ds(pl.multiple_of((t - 4) * 256, 256), 256)
            start(wg_ref.at[:, cs], ring.at[slot, :depth, :PAIR])
            start(wu_ref.at[:, cs], ring.at[slot, :depth, PAIR:])

        @pl.when(t >= 4 + nd)
        def _():
            cs = pl.ds(pl.multiple_of((t - 4 - nd) * DOT_N, DOT_N), DOT_N)
            start(wd_ref.at[:, cs], ring.at[slot, :ff, :])

    def take(ld, n_rows):
        slot = lax.rem(ld, SLOTS)
        whole = ring.at[slot, :n_rows, :]
        pltpu.make_async_copy(whole, whole, ring_sem.at[slot]).wait()
        pl.when(ld + SLOTS - 1 < total_loads)(lambda: issue(ld + SLOTS - 1))
        return slot

    def late(c, d):
        return obuf.at[c, d, :, tile(1, width)]

    def o_copy(c, d):
        return rdma(o_last[int(d > 1)].at[tile(c, H), :], late(c, d), o_send.at[c, d - 1], o_recv.at[c, d - 1], peers[d])

    def o_start(c):
        for d in (1, 2, 3):
            o_copy(c, d).start()

    def project(c, ld0):
        own_o = pltpu.make_async_copy(o_last[0].at[tile(c, H), :], late(c, 0), loc_sem.at[0])
        own_x = pltpu.make_async_copy(x_ref.at[tile(c * 2 + side, H), cols_at(z)], xs, loc_sem.at[1])
        own_o.start()
        own_x.start()
        for d in (1, 2, 3):
            o_copy(c, d).wait_recv()
        own_o.wait()
        own_x.wait()

        @each(n_ct)
        def _(ct):
            cs = tile(ct, DOT_N)
            ybuf[c, :, cs] = xs[:, cs].astype(F32)

        @each(4)
        def _(d):
            slot = take(ld0 + d, n_ct * kz)

            @each(n_ct)
            def _(ct):
                cs = tile(ct, DOT_N)
                w = ring[slot, tile(ct, kz), :]
                ybuf[c, :, cs] += jnp.dot(obuf[c, d], w, preferred_element_type=F32)

        sstat[c] = jnp.zeros((H, LANES), F32)

        @each(n_ct)
        def _(ct):
            yv = ybuf[c, :, tile(ct, DOT_N)]
            sstat[c] += jnp.broadcast_to(jnp.sum(yv * yv, axis=-1, keepdims=True), (H, LANES))

        swap_stat = rdma(sstat.at[c], rstat.at[c], st_send.at[c, 0], st_recv.at[c, 0], mate)
        swap_stat.start()
        swap_stat.wait_recv()
        inv = lax.rsqrt((sstat[c] + rstat[c])[:, 0:1] * (1.0 / depth) + NORM_EPS)

        @each(n_ct)
        def _(ct):
            cs = tile(ct, DOT_N)
            gs = tile(q * n_ct + ct, DOT_N)
            h2[c, rows_at(z), gs] = (ybuf[c, :, cs] * inv * gain_ref[:, gs].astype(F32)).astype(BF16)

    class Spread:
        def __init__(self, block, send, recv, own=None):
            self.block, self.send, self.recv, self.own = block, send, recv, own

        def copy(self, c, zz, s, r, dev, own=False):
            src = self.own(c) if own and self.own is not None else self.block(c, zz)
            return rdma(src, self.block(c, zz), self.send.at[c, s], self.recv.at[c, r], dev)

        def to_near(self, c):
            return self.copy(c, z, 0, 0, near, own=True)

        def to_outer(self, c):
            return self.copy(c, z, 0, 0, outer, own=True)

        def to_inner(self, c):
            return self.copy(c, z, 1, 1, inner, own=True)

        def end_to_inner(self, c):
            return self.copy(c, outer, 2, 2, inner)

        def inner_to_outer(self, c):
            return self.copy(c, inner, 3, 1, outer)

        def far_to_outer(self, c):
            return self.copy(c, far_end, 4, 2, outer)

        def start(self, c):
            pl.when(is_end)(lambda: self.to_near(c).start())

            @pl.when(is_mid)
            def _():
                self.to_outer(c).start()
                self.to_inner(c).start()

        def wait(self, c, r):
            self.copy(c, z, 0, r, mate).wait_recv()

        def serve(self, r, c):
            self.wait(c, r)
            (self.end_to_inner, self.inner_to_outer, self.far_to_outer)[r](c).start()

        def drain(self, c):
            @pl.when(is_end)
            def _():
                self.to_near(c).wait_send()

            @pl.when(is_mid)
            def _():
                for copy in (self.to_outer(c), self.to_inner(c), self.end_to_inner(c), self.inner_to_outer(c), self.far_to_outer(c)):
                    copy.wait_send()

    hidden = Spread(lambda c, zz: h2.at[c, rows_at(zz), cols_at(zz)], a1_send, a1_recv)

    def out_block(c, zz):
        return xout_ref.at[tile(c * 2 + side_of(zz), H), cols_at(zz)]

    done = Spread(out_block, a2_send, a2_recv, own=lambda c: xo.at[c])

    def gate_up(c, ld0, active, after):
        @each(nd)
        def _(i):
            @pl.when(active)
            def _():
                slot = take(ld0 + i, depth)
                gu = jnp.dot(h2[c], ring[slot, :depth, :], preferred_element_type=F32)
                g, u = gu[:, :PAIR], gu[:, PAIR:]
                act[:, tile(i, PAIR)] = (g * (1.0 / (1.0 + jnp.exp(-g))) * u).astype(BF16)

            for k in range(4):
                pl.when(i == (k + 1) * nd // 4 - 1)(functools.partial(after, k + 1))

    def ps_copy(c, k_send, zz, k_recv, dev):
        return rdma(psum.at[lax.rem(c, 2), zz], land_ref.at[c, k_recv], rs_send.at[c, k_send], rs_recv.at[c, k_recv], dev)

    def sums_out(c):
        ends = (ps_copy(c, 0, far_end, 0, near), ps_copy(c, 1, inner, 2, near), ps_copy(c, 2, near, 3, near))
        mids = (ps_copy(c, 0, far_end, 1, inner), ps_copy(c, 1, outer, 0, outer), ps_copy(c, 2, inner, 4, inner))
        return ends, mids

    def wait_sums_out(c):
        ends, mids = sums_out(c)
        for flag, copies in ((is_end, ends), (is_mid, mids)):
            @pl.when(flag)
            def _():
                for copy in copies:
                    copy.wait_send()

    def down(c, ld0, part):
        ps = lax.rem(c, 2)
        ends, _ = sums_out(c)
        if part == 0:
            pl.when(c >= 2)(lambda: wait_sums_out(c - 2))

        @each(ne // 2)
        def _(i):
            slot = take(ld0 + part * (ne // 2) + i, ff)
            pv = jnp.dot(act[...], ring[slot, :ff, :], preferred_element_type=F32)
            cs = tile(i, DOT_N)
            psum[ps, part, :, cs] = pv[:H]
            psum[ps, 3 - part, :, cs] = pv[H:R]

        @pl.when(is_end)
        def _():
            for copy in (ends[:1], ends[1:])[part]:
                copy.start()

    def arrive(c, k, buf):
        ps_copy(c, 0, z, k, mate).wait_recv()
        copy = pltpu.make_async_copy(land_ref.at[c, k], stage.at[buf], loc_sem.at[2 + buf])
        copy.start()
        return copy

    def tiles(fn):
        @each(4)
        def _(i):
            fn(tile(i, H // 4))

    def pass_on(c, k, zz, send):
        arrive(c, k, 0).wait()

        def add(rs):
            psum[lax.rem(c, 2), zz, rs, :] += stage[0, rs, :]

        tiles(add)
        send.start()

    def finish(c, ks):
        for copy in [arrive(c, k, i) for i, k in enumerate(ks)]:
            copy.wait()

        def add(rs):
            v = psum[lax.rem(c, 2), z, rs, :] + stage[0, rs, :]
            if len(ks) == 2:
                v = v + stage[1, rs, :]
            xo[c, rs, :] = (ybuf[c, rs, :] + v).astype(BF16)

        tiles(add)
        done.start(c)
        pltpu.make_async_copy(xo.at[c], out_block(c, z), loc_sem.at[4]).start()
        pltpu.make_async_copy(xo.at[c], out_block(c, z), loc_sem.at[4]).wait()

    def relay(k, c):
        pass_on(c, k, (far_end, outer, inner)[k], sums_out(c)[1][k])

    def hidden_wait(c):
        for r in range(3):
            hidden.wait(c, r)

    steps = {'O': o_start, 'hw': hidden_wait, 'f': lambda c: finish(c, (0,)), 'r4': lambda c: finish(c, (3, 4))}
    for r in range(3):
        steps['h' + 'abc'[r]] = functools.partial(hidden.serve, r)
        steps['x' + 'abc'[r]] = functools.partial(done.serve, r)
        steps['r' + '123'[r]] = functools.partial(relay, r)

    early = [pltpu.make_async_copy(src, obuf.at[:, d, :, tile(0, width)], loc_sem.at[5 + d]) for d, src in enumerate(o_first)]
    for copy in early:
        copy.start()
    each(SLOTS - 1)(issue)
    for copy in early:
        copy.wait()

    @each(AHEAD + nc + BEHIND)
    def _(t):
        j = t - AHEAD
        jj = j + 1
        active = (j >= 0) & (j < nc)

        def after(k):
            for flag, plan in ((is_mid, MID_PLAN[k]), (is_end, END_PLAN[k])):
                def run(plan=plan):
                    for name, ahead in plan:
                        c = j + ahead
                        pl.when((c >= 0) & (c < nc))(functools.partial(steps[name], c))

                if plan:
                    pl.when(flag)(run)

        @pl.when((jj >= 0) & (jj < nc))
        def _():
            project(jj, per * jj - (per - 4) * lax.div(jj + big - 1, big))
            hidden.start(jj)

        after(0)
        ld_d = per * jj - (per - 8) - 4 * lax.div(jj, nc)
        gate_up(j, ld_d, active, after)
        for part in range(2):
            pl.when(active)(lambda: down(j, ld_d + nd, part))
            after(5 + part)

    @each(nc)
    def _(c):
        @pl.when(is_end)
        def _():
            for r in range(3):
                done.wait(c, r)

        for d in (1, 2, 3):
            o_copy(c, d).wait_send()
        rdma(sstat.at[c], rstat.at[c], st_send.at[c, 0], st_recv.at[c, 0], mate).wait_send()
        hidden.drain(c)
        done.drain(c)
        pl.when(c >= nc - 2)(lambda: wait_sums_out(c))


def line_block(o_first, o_last, x, w_out, pieces, w_gate, w_up, w_down, gain):
    rows, depth = x.shape
    ff = w_gate.shape[1]
    width = o_last[0].shape[-1]
    kz = 2 * width
    nc = rows // ROWS_CH
    h, half = ROWS_CH // 2, depth // 2
    ring_rows = max(depth, ff, half // DOT_N * kz)
    sems = [pltpu.SemaphoreType.DMA((nc, n)) for n in (3, 3, 1, 1, 5, 3, 3, 5, 5, 3)]
    xout, _ = pl.pallas_call(
        functools.partial(line_kernel, nc=nc),
        in_specs=[HBM] * (11 + len(pieces)) + [VMEM],
        out_specs=[HBM] * 2,
        out_shape=[struct(x.shape, BF16), struct((nc, 5, h, half), F32)],
        scratch_shapes=[
            pltpu.VMEM((nc, 4, h, kz), BF16), pltpu.VMEM((nc, ROWS_CH, depth), BF16), pltpu.VMEM((nc, h, half), F32),
            pltpu.VMEM((SLOTS, ring_rows, DOT_N), BF16), pltpu.VMEM((2, 4, h, half), F32), pltpu.VMEM((ROWS_CH, ff), BF16),
            pltpu.VMEM((2, h, half), F32), pltpu.VMEM((h, half), BF16), pltpu.VMEM((nc, h, half), BF16),
            *[pltpu.VMEM((nc, h, LANES), F32)] * 2, pltpu.SemaphoreType.DMA((SLOTS,)), pltpu.SemaphoreType.DMA((9,)), *sems,
        ],
        compiler_params=params(60, collective_id=1, has_side_effects=True),
        cost_estimate=cost(6 * x.size * ff, 2 * x.size),
        name="line_block",
    )(*(a.reshape(nc, h, width) for a in o_first), *o_last, x, w_out, *pieces, w_gate, w_up, w_down, gain.reshape(1, depth))
    return xout


def gather_w_out(w_out, tps):
    z, dp, cp = (lax.axis_index(a) for a in ('tp', 'dp', 'cp'))
    n, half = w_out.shape[0] // 8, w_out.shape[1] // 2
    q = (z + 1) // 2 % 2
    part = lax.dynamic_slice_in_dim(w_out, (dp * 4 + cp) * n, n, 0)
    same, other = (lax.dynamic_slice_in_dim(part, h * half, half, 1) for h in (q, 1 - q))
    return tuple(lax.ppermute(a, 'tp', [(i, i ^ d) for i in range(tps)]) for d, a in ((1, other), (2, other), (3, same)))


def solution(mesh):
    groups = mesh.shape['cp']
    tps = mesh.shape['tp']
    dps = mesh.shape['dp']

    def local_layer(x_loc, kp_loc, vp_loc, norm_attn, w_query, w_key, w_value, w_out, norm_mlp, w_gate, w_up, w_down):
        rows = x_loc.shape[0]
        pre_dev, kv_loc, head_dim = kp_loc.shape
        c2 = head_dim ** -0.5 * math.log2(math.e)
        me = lax.axis_index('cp')
        q_pos = block_positions(me, groups, rows // 2, pre_dev * groups)
        vals = vp_loc.reshape(pre_dev // LANES, LANES, kv_loc, head_dim).transpose(2, 0, 3, 1)
        own_pre = (kp_loc.transpose(1, 0, 2), vals.reshape(kv_loc, pre_dev, LANES))
        far_pre = swap(own_pre, 'cp', groups, 2)
        near_pre = swap(own_pre, 'cp', groups, 1)
        wo_z = gather_w_out(w_out, tps)
        cos_tab, sin_tab = rope_tables(q_pos, head_dim)
        q, own_suf, k_flat, v_flat = qkv(x_loc, norm_attn, w_query, w_key, w_value, cos_tab, sin_tab)
        far_suf, = swap((own_suf,), 'cp', groups, 2)
        near_suf, = swap((own_suf,), 'cp', groups, 1)
        o_first, o_last, wo_pieces = attend(q, own_pre, near_pre, far_pre, own_suf, near_suf, far_suf, wo_z, c2, groups, tps, dps)
        x_out = line_block(o_first, o_last, x_loc, w_out, wo_pieces, w_gate, w_up, w_down, norm_mlp)
        return x_out, k_flat.reshape(rows, kv_loc, head_dim), v_flat.reshape(rows, kv_loc, head_dim)

    row_spec = P(('dp', 'cp'), None)
    kv_spec = P(('dp', 'cp'), 'tp', None)
    col_spec = P(None, 'tp')
    row_split = P('tp', None)
    vec_spec = P(None)
    return jax.shard_map(local_layer, mesh=mesh, in_specs=(row_spec, kv_spec, kv_spec, vec_spec, col_spec, col_spec, col_spec, row_split, vec_spec, col_spec, col_spec, row_split), out_specs=(row_spec, kv_spec, kv_spec), check_vma=False)
```

```python
import functools
import math

import jax
import jax.numpy as jnp
from jax import lax
from jax.experimental import pallas as pl
from jax.experimental.pallas import tpu as pltpu
from jax.sharding import PartitionSpec as P


ROPE_THETA = 500000.0
NORM_EPS = 1e-5
ROWS_CH = 128
F32 = jnp.float32
BF16 = jnp.bfloat16
HBM = pl.BlockSpec(memory_space=pl.ANY)
VMEM = pl.BlockSpec(memory_space=pltpu.VMEM)
IN_HBM = pl.BlockSpec(memory_space=pltpu.HBM)
LANES = 128
PAIR = 2 * LANES
NT = (((1,), (1,)), ((), ()))
each = functools.partial(pl.loop, 0)


def tile(i, n):
    return pl.ds(pl.multiple_of(i * n, n), n)


def params(mib, **more):
    return pltpu.CompilerParams(vmem_limit_bytes=mib * 2**20, **more)


def cost(flops, moved):
    return pl.CostEstimate(flops=flops, bytes_accessed=moved, transcendentals=0)


def struct(shape, dtype):
    return jax.ShapeDtypeStruct(shape, dtype)


def block_positions(owner, groups, blk_len, prefix_len):
    local_row = jnp.arange(2 * blk_len, dtype=jnp.int32)
    blk_idx = jnp.where(local_row < blk_len, owner, 2 * groups - 1 - owner)
    return prefix_len + blk_idx * blk_len + local_row % blk_len


def rope_tables(positions, head_dim):
    inv_freq = ROPE_THETA ** (-jnp.arange(0, head_dim, 2, dtype=F32) / head_dim)
    angles = positions.astype(F32)[:, None] * inv_freq[None, :]
    cos_tab, sin_tab = jnp.cos(angles), jnp.sin(angles)
    return jnp.concatenate([cos_tab, cos_tab], axis=1), jnp.concatenate([-sin_tab, sin_tab], axis=1)


def qkv_kernel(x_hbm, g_ref, wq_ref, wk_ref, wv_ref, cos_ref, sin_ref, q_ref, kv_ref, kf_ref, vf_ref, x_ref, h_ref, sems, *, nq):
    step = pl.program_id(0)
    rows = x_ref.shape[0]
    parts, rt = sems.shape[0], 32

    @pl.when(step == 0)
    def _():
        n = rows // parts
        copies = [pltpu.make_async_copy(x_hbm.at[tile(i, n), :], x_ref.at[tile(i, n), :], sems.at[i]) for i in range(parts)]
        for copy in copies:
            copy.start()
        for i, copy in enumerate(copies):
            copy.wait()

            @pl.loop(i * n // rt, (i + 1) * n // rt, unroll=2)
            def _(j):
                sl = tile(j, rt)
                xv = x_ref[sl, :].astype(F32)
                inv = lax.rsqrt(jnp.mean(xv * xv, axis=-1, keepdims=True) + NORM_EPS)
                h_ref[sl, :] = (xv * inv * g_ref[...].astype(F32)).astype(BF16)

    def rope(block, sl):
        return (block * cos_ref[sl, :] + pltpu.roll(block, 64, axis=1) * sin_ref[sl, :]).astype(BF16)

    mt = 512

    def project(w_ref, store):
        @each(rows // mt)
        def _(i):
            sl = tile(i, mt)
            acc = jnp.dot(h_ref[sl, :], w_ref[...], preferred_element_type=F32)
            store(acc, sl)

    def heads_of(acc):
        return [(t, slice(t * LANES, (t + 1) * LANES), acc[:, t * LANES:(t + 1) * LANES]) for t in range(2)]

    def store_q(acc, sl):
        for _, cs, part in heads_of(acc):
            q_ref[sl, cs] = rope(part, sl)

    def store_k(acc, sl):
        for t, cs, part in heads_of(acc):
            kf_ref[sl, cs] = rope(part, sl)
            kv_ref[0, t, sl, :] = kf_ref[sl, cs]

    def store_v(acc, sl):
        vf_ref[sl, :] = acc.astype(BF16)
        for t, _, part in heads_of(acc):
            for b in range(mt // LANES):
                kv_ref[1, t, pl.ds(sl.start + b * LANES, LANES), :] = part[b * LANES:(b + 1) * LANES].T.astype(BF16)

    pl.when(step < nq)(lambda: project(wq_ref, store_q))
    pl.when(step == nq)(lambda: project(wk_ref, store_k))
    pl.when(step == nq + 1)(lambda: project(wv_ref, store_v))


def qkv(x, gain, wq, wk, wv, cos_tab, sin_tab):
    rows, depth = x.shape
    nq = wq.shape[1] // PAIR

    def fixed(shape):
        return pl.BlockSpec(shape, lambda j: tuple(0 for _ in shape))

    def whole(shape):
        return pl.BlockSpec(shape, lambda j: tuple(0 for _ in shape), pipeline_mode=pl.Buffered(1))

    def columns(n):
        return pl.BlockSpec((n, PAIR), lambda j: (0, jnp.minimum(j, nq - 1)))

    flat, by_head = (rows, PAIR), (2, 2, rows, LANES)
    return pl.pallas_call(
        functools.partial(qkv_kernel, nq=nq),
        grid=(nq + 2,),
        in_specs=[HBM, whole((1, depth)), columns(depth), fixed(wk.shape), fixed(wv.shape), whole(cos_tab.shape), whole(sin_tab.shape)],
        out_specs=[columns(rows), fixed(by_head), fixed(flat), fixed(flat)],
        out_shape=[struct(s, BF16) for s in ((rows, nq * PAIR), by_head, flat, flat)],
        scratch_shapes=[pltpu.VMEM((rows, depth), BF16), pltpu.VMEM((rows, depth), BF16), pltpu.SemaphoreType.DMA((4,))],
        compiler_params=params(58, dimension_semantics=("arbitrary",)),
        cost_estimate=cost(2 * rows * depth * (nq + 2) * PAIR, 2 * depth * rows),
        name="qkv",
    )(x, gain.reshape(1, depth), wq, wk, wv, cos_tab, sin_tab)


NQ = 512
PER_KV = 4


class Fetch:
    def __init__(self, sems):
        self.sems, self.used = sems, 0

    def start(self, pairs):
        copies = []
        for src, dst in pairs:
            copies.append(pltpu.make_async_copy(src, dst, self.sems.at[self.used]))
            self.used += 1
        for copy in copies:
            copy.start()
        return copies


def settle(copies):
    for copy in copies:
        copy.wait()


def q_block(q_ref, head, half):
    return q_ref[tile(half, NQ), tile(head, LANES)]


def across(blocks):
    return jnp.concatenate([blocks[i:i + LANES] for i in range(0, blocks.shape[0], LANES)], axis=1)


def attend_items(q_ref, kb_ref, vb_ref, acc_ref, m_ref, l_ref, pbufs, n_items, item, bk, c2, diag=False):
    depth = len(pbufs)

    def scores(i, pb):
        head, half, start = item(i)
        n = head * 2 + half
        ks = kb_ref[head // PER_KV, pl.ds(pl.multiple_of(start, bk), bk), :]
        s = lax.dot_general(ks, q_block(q_ref, head, half), NT, preferred_element_type=F32)
        e = jnp.exp2(s * c2 - m_ref[n])
        if diag:
            seen = lax.broadcasted_iota(jnp.int32, (bk, NQ), 0) <= lax.broadcasted_iota(jnp.int32, (bk, NQ), 1)
            e = jnp.where(seen, e, 0.0)
        pb[...] = e.astype(BF16)
        l_ref[n] += jnp.sum(e.reshape(-1, *l_ref.shape[1:]), axis=0)

    def values(i, pb):
        head, half, start = item(i)
        vt = across(vb_ref[head // PER_KV, pl.ds(pl.multiple_of(start, bk), bk), :])
        acc_ref[head * 2 + half] += jnp.dot(vt, pb[...], preferred_element_type=F32)

    scores(0, pbufs[0])

    def body(g, carry):
        for u in range(depth):
            i = g * depth + u
            scores(i + 1, pbufs[(u + 1) % depth])
            values(i, pbufs[u])
        return carry

    trips = n_items // depth - 1
    lax.fori_loop(0, trips, body, 0)
    for u in range(depth):
        if u + 1 < depth:
            scores(trips * depth + u + 1, pbufs[u + 1])
        values(trips * depth + u, pbufs[u])


def prefix_kernel(q_hbm, ka, va, kb, vb, acc_out, m_out, l_out, q_ref, kbuf, vbuf, acc_ref, m_ref, l_ref, pa, pb, sems, *, heads, c2):
    fetch = Fetch(sems)
    n = ka.shape[1]
    settle(fetch.start([(q_hbm, q_ref), (ka, kbuf.at[:, tile(0, n), :]), (va, vbuf.at[:, tile(0, n), :]), (kb, kbuf.at[:, tile(1, n), :]), (vb, vbuf.at[:, tile(1, n), :])]))

    @each(heads // PER_KV)
    def _(group):
        for j in range(2 * PER_KV):
            i = group * 2 * PER_KV + j
            s = lax.dot_general(kbuf[group, tile(0, LANES), :], q_block(q_ref, i // 2, j % 2), NT, preferred_element_type=F32)
            m_ref[i] = jnp.max(s, axis=0, keepdims=True) * c2

    for ref in (acc_ref, l_ref):
        ref[...] = jnp.zeros_like(ref)
    bk = 2 * NQ
    per = kbuf.shape[1] // bk

    def item(i):
        pair = i // per
        return pair // 2, pair % 2, (i % per) * bk

    attend_items(q_ref, kbuf, vbuf, acc_ref, m_ref, l_ref, (pa, pb), heads * 2 * per, item, bk, c2)
    settle(fetch.start([(acc_ref, acc_out), (m_ref, m_out), (l_ref, l_out)]))


def state_shapes(heads):
    return [struct((heads * 2, n, NQ), F32) for n in (LANES, 1, 8)]


def vmem_like(shapes):
    return [pltpu.VMEM(s.shape, s.dtype) for s in shapes]


def attend_prefix(q, pieces, c2):
    heads = q.shape[1] // LANES
    flat = [a for p in pieces for a in p]
    n = 2 * pieces[0][0].shape[1]
    shapes = state_shapes(heads)
    return pl.pallas_call(
        functools.partial(prefix_kernel, heads=heads, c2=c2),
        in_specs=[HBM] * (1 + len(flat)),
        out_specs=[HBM] * len(shapes),
        out_shape=[pltpu.HBM(s.shape, s.dtype) for s in shapes],
        scratch_shapes=[
            *vmem_like([q]), *[pltpu.VMEM((2, n, LANES), BF16)] * 2, *vmem_like(shapes),
            *[pltpu.VMEM((2 * NQ, NQ), BF16)] * 2, pltpu.SemaphoreType.DMA((8,)),
        ],
        compiler_params=params(58),
        cost_estimate=cost(4 * q.size * n, 4 * q.size),
        name="attend_prefix",
    )(q, *flat)


def rest_kernel(*refs, group, groups, c2, axis):
    q_hbm, *refs = refs
    flat, suf, refs = refs[:2 * groups], refs[2 * groups:3 * groups], refs[3 * groups:]
    pre = list(zip(flat[::2], flat[1::2]))
    acc_in, m_in, l_in, here_out, there_out, q_ref, kbuf, vbuf, ksuf, vsuf, acc_ref, m_ref, l_ref, acc_old, l_old, o_ref, bad_ref, sems, wa, wb, pa, pb, pc, pd = refs
    heads = PER_KV
    me = lax.axis_index(axis)
    fetch = Fetch(sems)
    mine = pl.ds(group * heads * 2, heads * 2)
    n_pre, n_suf = pre[0][0].shape[1], suf[0].shape[2]
    first = fetch.start([(q_hbm.at[:, tile(group, heads * LANES)], q_ref), (m_in.at[mine], m_ref)])
    for i, (kr, vr) in enumerate(pre[2:]):
        first += fetch.start([(kr.at[group], kbuf.at[0, tile(i, n_pre), :]), (vr.at[group], vbuf.at[0, tile(i, n_pre), :])])
    second = []
    for i, kv in enumerate(suf):
        second += fetch.start([(kv.at[j, group], buf.at[0, tile(i, n_suf), :]) for j, buf in enumerate((ksuf, vsuf))])
    third = fetch.start([(acc_in.at[mine], acc_old), (l_in.at[mine], l_old)])
    for ref in (acc_ref, l_ref):
        ref[...] = jnp.zeros_like(ref)
    settle(first)
    bk = 2 * NQ
    per = kbuf.shape[1] // bk

    def pre_item(i):
        pair = i // per
        return pair // 2, pair % 2, (i % per) * bk

    attend_items(q_ref, kbuf, vbuf, acc_ref, m_ref, l_ref, (wa, wb), heads * 2 * per, pre_item, bk, c2)
    settle(second)
    last = 2 * groups - 1

    def locate(blk):
        late = (blk >= groups).astype(jnp.int32)
        owner = jnp.where(blk < groups, blk, last - blk)
        diff = (owner % 2 != me % 2).astype(jnp.int32) + 2 * (owner // 2 != me // 2).astype(jnp.int32)
        return (diff * 2 + late) * NQ

    def full_item(i):
        head, r = i // last, i % last
        half = (r >= me).astype(jnp.int32)
        return head, half, locate(jnp.where(r < me, r, r - me))

    def diag_item(i):
        half = i % 2
        return i // 2, half, locate(jnp.where(half == 0, me, last - me))

    attend_items(q_ref, ksuf, vsuf, acc_ref, m_ref, l_ref, (pa, pb, pc, pd), heads * last, full_item, NQ, c2)
    attend_items(q_ref, ksuf, vsuf, acc_ref, m_ref, l_ref, (pa, pb), heads * 2, diag_item, NQ, c2, diag=True)
    settle(third)
    bad_ref[...] = jnp.zeros_like(bad_ref)
    chunk = ROWS_CH // 2

    def write(i, acc, total):
        head, half = i // 2, i % 2
        out = (acc * (1.0 / total)).T.astype(BF16)
        n_p = NQ // chunk
        for p in range(n_p):
            o_ref[p % 2, tile(half * (n_p // 2) + p // 2, chunk), tile(head, LANES)] = out[p * chunk:(p + 1) * chunk]

    @each(heads * 2)
    def _(i):
        acc = acc_ref[i] + acc_old[i]
        total = jnp.sum(l_ref[i] + l_old[i], axis=0, keepdims=True)
        bad = jnp.where((jnp.abs(acc) < jnp.inf) & (total < jnp.inf), 0.0, 1.0)
        for j in range(NQ // LANES):
            part = bad[:, j * LANES:(j + 1) * LANES]
            bad_ref[...] = jnp.maximum(bad_ref[...], jnp.max(part.reshape(-1, *bad_ref.shape), axis=0))
        write(i, acc, total)

    @pl.when(jnp.max(bad_ref[...]) > 0.0)
    def _():
        @each(heads * 2)
        def _(i):
            head, half = i // 2, i % 2
            q = q_block(q_ref, head, half)
            m_ref[i] = jnp.full((1, NQ), -jnp.inf, F32)
            for ref in (acc_ref, l_ref):
                ref[i] = jnp.zeros(ref.shape[1:], F32)

            def update(ks, vt, seen):
                s = lax.dot_general(ks, q, NT, preferred_element_type=F32) * c2
                if seen is not None:
                    s = jnp.where(seen, s, -jnp.inf)
                m_old = m_ref[i]
                m_new = jnp.maximum(m_old, jnp.max(s, axis=0, keepdims=True))
                alpha = jnp.exp2(m_old - m_new)
                e = jnp.exp2(s - m_new)
                m_ref[i] = m_new
                l_ref[i] = l_ref[i] * alpha + jnp.sum(e.reshape(-1, *l_ref.shape[1:]), axis=0)
                acc_ref[i] = acc_ref[i] * alpha + jnp.dot(vt, e.astype(BF16), preferred_element_type=F32)

            kpre, vpre = (p.at[:, tile(0, LANES)] for p in (pa, pb))
            for kr, vr in pre:
                @each(n_pre // NQ)
                def _(j):
                    pltpu.sync_copy(kr.at[group, tile(j, NQ), :], kpre)
                    pltpu.sync_copy(vr.at[group, tile(j, NQ), :], vpre)
                    update(kpre[...], across(vpre[...]), None)

            mine_blk = jnp.where(half == 0, me, last - me)

            @each(2 * groups)
            def _(blk):
                @pl.when(blk <= mine_blk)
                def _():
                    start = pl.ds(pl.multiple_of(locate(blk), NQ), NQ)
                    seen = (lax.broadcasted_iota(jnp.int32, (NQ, NQ), 0) <= lax.broadcasted_iota(jnp.int32, (NQ, NQ), 1)) | (blk < mine_blk)
                    update(ksuf[0, start, :], across(vsuf[0, start, :]), seen)

            write(i, acc_ref[i], jnp.sum(l_ref[i], axis=0, keepdims=True))

    side = lax.axis_index('tp') // 2
    settle(fetch.start([(o_ref.at[side], here_out), (o_ref.at[1 - side], there_out)]))


def attend_rest(q, pre, suf, state, c2, axis, group):
    rows, groups, width = q.shape[0], len(suf), PER_KV * LANES
    n_pre, n_suf = 2 * pre[0][0].shape[1], groups * suf[0].shape[2]
    flat = [a for p in pre for a in p] + list(suf)
    acc, m, total = state_shapes(PER_KV)
    out = pltpu.HBM((rows // 2, width), BF16)
    return pl.pallas_call(
        functools.partial(rest_kernel, group=group, groups=groups, c2=c2, axis=axis),
        in_specs=[IN_HBM] + [HBM] * len(flat) + [IN_HBM] * 3,
        out_specs=[HBM] * 2,
        out_shape=[out] * 2,
        scratch_shapes=[
            pltpu.VMEM((rows, width), BF16), *[pltpu.VMEM((1, n, LANES), BF16) for n in (n_pre, n_pre, n_suf, n_suf)], *vmem_like([acc, m, total, acc, total, struct((2, rows // 2, width), BF16)]),
            pltpu.VMEM((8, LANES), F32), pltpu.SemaphoreType.DMA((22,)), *[pltpu.VMEM((2 * NQ, NQ), BF16)] * 2, *[pltpu.VMEM((NQ, NQ), BF16)] * 4,
        ],
        compiler_params=params(42),
        cost_estimate=cost(2 * rows * width * (2 * n_pre + n_suf), 4 * q.size),
        name="attend_rest",
    )(q, *flat, *state)


def swap(arrays, axis, groups, bit):
    return tuple(lax.ppermute(a, axis, [(i, i ^ bit) for i in range(groups)]) for a in arrays)


def attend(q, own_pre, near_pre, far_pre, own_suf, near_suf, far_suf, wo_z, c2, groups, tps, dps):
    state = attend_prefix(q, (own_pre, near_pre), c2)
    far_pre, far_suf, wo_z, state = lax.optimization_barrier((far_pre, far_suf, wo_z, state))
    cross_pre = swap(far_pre, 'cp', groups, 1)
    cross_suf, = swap((far_suf,), 'cp', groups, 1)
    wo = jnp.stack(wo_z)
    wo_x, = swap((wo,), 'dp', dps, 1)
    wo_y, = swap((wo,), 'cp', groups, 2)
    pre, suf = (own_pre, near_pre, far_pre, cross_pre), (own_suf, near_suf, far_suf, cross_suf)
    here, there = attend_rest(q, pre, suf, state, c2, 'cp', 0)
    o_got = tuple(lax.ppermute(a, 'tp', [(i, i ^ d) for i in range(tps)]) for d, a in ((1, here), (2, there), (3, there)))
    wo, wo_x, wo_y, there, q = lax.optimization_barrier((wo, wo_x, wo_y, there, q))
    wo_xy, = swap((wo_x,), 'cp', groups, 2)
    near = swap((wo, wo_x, wo_y), 'cp', groups, 1)
    o_last = attend_rest(q, pre, suf, state, c2, 'cp', 1)
    wo_xy, o_last = lax.optimization_barrier((wo_xy, o_last))
    return (here,) + o_got, o_last, (wo, wo_x, wo_y, wo_xy) + near + swap((wo_xy,), 'cp', groups, 1)


MESH = pl.DeviceIdType.MESH
DOT_N = 512
SLOTS = 3
MID_PLAN = ((('r3', -1),), (('xc', -3), ('r2', -1), ('hb', 1), ('ha', 1),), (('xb', -2), ('xa', -2),), (('O', 3),), (('r4', -1),), (), (('hc', 1), ('r1', 0),))
END_PLAN = ((('hw', 0), ('f', -2),), (('O', 3),), (), (), (), (), ())
AHEAD, BEHIND = 3, 3


def side_of(z):
    return lax.div(z, 2)


def colhalf_of(z):
    return lax.rem(lax.div(z + 1, 2), 2)


def line_kernel(*refs, nc):
    o_first, o_last, x_ref, wo_ref, *refs = refs[:4], refs[4:6], *refs[6:]
    wo_pieces, refs = refs[:8], refs[8:]
    wg_ref, wu_ref, wd_ref, gain_ref, xout_ref, land_ref = refs[:6]
    (obuf, h2, ybuf, ring, psum, act, stage, xs, sstat, rstat,
     ring_sem, loc_sem, o_send, o_recv, st_send, st_recv, a1_send, a1_recv, rs_send, rs_recv, a2_send, a2_recv) = refs[6:]
    R, H = ROWS_CH, ROWS_CH // 2
    depth = wg_ref.shape[0]
    ff = wg_ref.shape[1]
    half = depth // 2
    width = o_last[0].shape[-1]
    kz = 2 * width
    n_ct = half // DOT_N
    nd, ne = ff // PAIR, depth // DOT_N
    per = 4 + nd + ne
    total_loads = nc * per
    big = 1024

    z = lax.axis_index('tp')
    dp = lax.axis_index('dp')
    cp = lax.axis_index('cp')
    core, chip = lax.rem(cp, 2), lax.div(cp, 2)
    side, q = side_of(z), colhalf_of(z)
    is_mid = q == 1
    is_end = q != 1
    near = 1 + side
    outer = 3 * side
    inner = 2 - side
    far_end = 3 - 3 * side
    peers = {1: z + 1 - 2 * lax.rem(z, 2), 2: lax.rem(z + 2, 4), 3: 3 - z}
    mate = peers[1]

    def rdma(src, dst, ssem, rsem, dev):
        return pltpu.make_async_remote_copy(src_ref=src, dst_ref=dst, send_sem=ssem, recv_sem=rsem, device_id={'tp': dev}, device_id_type=MESH)

    def rows_at(zz):
        return tile(side_of(zz), H)

    def cols_at(zz):
        return tile(colhalf_of(zz), half)

    barrier = pltpu.get_barrier_semaphore()
    for d in (1, 2, 3):
        pl.semaphore_signal(barrier, inc=1, device_id={'tp': peers[d]}, device_id_type=MESH)
    pl.semaphore_wait(barrier, 3)

    def load_kind(ld):
        u = ld + (per - 4)
        i1 = lax.div(u, per)
        a = lax.div(i1 + big - 1, big)
        t = lax.rem(u, per) + 4 * lax.div(i1, nc)
        return a * t + (1 - a) * ld

    def issue(ld):
        slot = lax.rem(ld, SLOTS)
        sem = ring_sem.at[slot]
        t = load_kind(ld)

        def start(src, dst):
            pltpu.make_async_copy(src, dst, sem).start()

        for d in range(4):
            @pl.when(t == d)
            def _():
                @each(n_ct)
                def _(ct):
                    c0 = pl.multiple_of(ct * DOT_N, DOT_N)
                    if d == 0:
                        cs = tile(q * n_ct + ct, DOT_N)
                        start(wo_ref.at[:, cs], ring.at[slot, tile(ct, kz), :])
                    else:
                        for k, piece in enumerate(wo_pieces):
                            bits = (dp, k % 2), (chip, k // 2 % 2), (core, k // 4)
                            n = piece.shape[1]
                            j = sum((own + x - 2 * own * x) * w for (own, x), w in zip(bits, (4, 2, 1)))
                            r0 = pl.multiple_of(ct * kz + j * n, n)
                            start(piece.at[d - 1, :, pl.ds(c0, DOT_N)], ring.at[slot, pl.ds(r0, n), :])

        @pl.when((t >= 4) & (t < 4 + nd))
        def _():
            cs = pl.ds(pl.multiple_of((t - 4) * 256, 256), 256)
            start(wg_ref.at[:, cs], ring.at[slot, :depth, :PAIR])
            start(wu_ref.at[:, cs], ring.at[slot, :depth, PAIR:])

        @pl.when(t >= 4 + nd)
        def _():
            cs = pl.ds(pl.multiple_of((t - 4 - nd) * DOT_N, DOT_N), DOT_N)
            start(wd_ref.at[:, cs], ring.at[slot, :ff, :])

    def take(ld, n_rows):
        slot = lax.rem(ld, SLOTS)
        whole = ring.at[slot, :n_rows, :]
        pltpu.make_async_copy(whole, whole, ring_sem.at[slot]).wait()
        pl.when(ld + SLOTS - 1 < total_loads)(lambda: issue(ld + SLOTS - 1))
        return slot

    def late(c, d):
        return obuf.at[c, d, :, tile(1, width)]

    def o_copy(c, d):
        return rdma(o_last[int(d > 1)].at[tile(c, H), :], late(c, d), o_send.at[c, d - 1], o_recv.at[c, d - 1], peers[d])

    def o_start(c):
        for d in (1, 2, 3):
            o_copy(c, d).start()

    def project(c, ld0):
        own_o = pltpu.make_async_copy(o_last[0].at[tile(c, H), :], late(c, 0), loc_sem.at[0])
        own_x = pltpu.make_async_copy(x_ref.at[tile(c * 2 + side, H), cols_at(z)], xs, loc_sem.at[1])
        own_o.start()
        own_x.start()
        for d in (1, 2, 3):
            o_copy(c, d).wait_recv()
        own_o.wait()
        own_x.wait()

        @each(n_ct)
        def _(ct):
            cs = tile(ct, DOT_N)
            ybuf[c, :, cs] = xs[:, cs].astype(F32)

        @each(4)
        def _(d):
            slot = take(ld0 + d, n_ct * kz)

            @each(n_ct)
            def _(ct):
                cs = tile(ct, DOT_N)
                w = ring[slot, tile(ct, kz), :]
                ybuf[c, :, cs] += jnp.dot(obuf[c, d], w, preferred_element_type=F32)

        sstat[c] = jnp.zeros((H, LANES), F32)

        @each(n_ct)
        def _(ct):
            yv = ybuf[c, :, tile(ct, DOT_N)]
            sstat[c] += jnp.broadcast_to(jnp.sum(yv * yv, axis=-1, keepdims=True), (H, LANES))

        swap_stat = rdma(sstat.at[c], rstat.at[c], st_send.at[c, 0], st_recv.at[c, 0], mate)
        swap_stat.start()
        swap_stat.wait_recv()
        inv = lax.rsqrt((sstat[c] + rstat[c])[:, 0:1] * (1.0 / depth) + NORM_EPS)

        @each(n_ct)
        def _(ct):
            cs = tile(ct, DOT_N)
            gs = tile(q * n_ct + ct, DOT_N)
            h2[c, rows_at(z), gs] = (ybuf[c, :, cs] * inv * gain_ref[:, gs].astype(F32)).astype(BF16)

    class Spread:
        def __init__(self, block, send, recv):
            self.block, self.send, self.recv = block, send, recv

        def copy(self, c, zz, s, r, dev):
            return rdma(self.block(c, zz), self.block(c, zz), self.send.at[c, s], self.recv.at[c, r], dev)

        def to_near(self, c):
            return self.copy(c, z, 0, 0, near)

        def to_outer(self, c):
            return self.copy(c, z, 0, 0, outer)

        def to_inner(self, c):
            return self.copy(c, z, 1, 1, inner)

        def end_to_inner(self, c):
            return self.copy(c, outer, 2, 2, inner)

        def inner_to_outer(self, c):
            return self.copy(c, inner, 3, 1, outer)

        def far_to_outer(self, c):
            return self.copy(c, far_end, 4, 2, outer)

        def start(self, c):
            pl.when(is_end)(lambda: self.to_near(c).start())

            @pl.when(is_mid)
            def _():
                self.to_outer(c).start()
                self.to_inner(c).start()

        def wait(self, c, r):
            self.copy(c, z, 0, r, mate).wait_recv()

        def serve(self, r, c):
            self.wait(c, r)
            (self.end_to_inner, self.inner_to_outer, self.far_to_outer)[r](c).start()

        def drain(self, c):
            @pl.when(is_end)
            def _():
                self.to_near(c).wait_send()

            @pl.when(is_mid)
            def _():
                for copy in (self.to_outer(c), self.to_inner(c), self.end_to_inner(c), self.inner_to_outer(c), self.far_to_outer(c)):
                    copy.wait_send()

    hidden = Spread(lambda c, zz: h2.at[c, rows_at(zz), cols_at(zz)], a1_send, a1_recv)

    done = Spread(lambda c, zz: xout_ref.at[tile(c * 2 + side_of(zz), H), cols_at(zz)], a2_send, a2_recv)

    def gate_up(c, ld0, active, after):
        @each(nd)
        def _(i):
            @pl.when(active)
            def _():
                slot = take(ld0 + i, depth)
                gu = jnp.dot(h2[c], ring[slot, :depth, :], preferred_element_type=F32)
                g, u = gu[:, :PAIR], gu[:, PAIR:]
                act[:, tile(i, PAIR)] = (g * (1.0 / (1.0 + jnp.exp(-g))) * u).astype(BF16)

            for k in range(4):
                pl.when(i == (k + 1) * nd // 4 - 1)(functools.partial(after, k + 1))

    def ps_copy(c, k_send, zz, k_recv, dev):
        return rdma(psum.at[lax.rem(c, 2), zz], land_ref.at[c, k_recv], rs_send.at[c, k_send], rs_recv.at[c, k_recv], dev)

    def sums_out(c):
        ends = (ps_copy(c, 0, far_end, 0, near), ps_copy(c, 1, inner, 2, near), ps_copy(c, 2, near, 3, near))
        mids = (ps_copy(c, 0, far_end, 1, inner), ps_copy(c, 1, outer, 0, outer), ps_copy(c, 2, inner, 4, inner))
        return ends, mids

    def wait_sums_out(c):
        ends, mids = sums_out(c)
        for flag, copies in ((is_end, ends), (is_mid, mids)):
            @pl.when(flag)
            def _():
                for copy in copies:
                    copy.wait_send()

    def down(c, ld0, part):
        ps = lax.rem(c, 2)
        ends, _ = sums_out(c)
        if part == 0:
            pl.when(c >= 2)(lambda: wait_sums_out(c - 2))

        @each(ne // 2)
        def _(i):
            slot = take(ld0 + part * (ne // 2) + i, ff)
            pv = jnp.dot(act[...], ring[slot, :ff, :], preferred_element_type=F32)
            cs = tile(i, DOT_N)
            psum[ps, part, :, cs] = pv[:H]
            psum[ps, 3 - part, :, cs] = pv[H:R]

        @pl.when(is_end)
        def _():
            for copy in (ends[:1], ends[1:])[part]:
                copy.start()

    def arrive(c, k, buf):
        ps_copy(c, 0, z, k, mate).wait_recv()
        copy = pltpu.make_async_copy(land_ref.at[c, k], stage.at[buf], loc_sem.at[2 + buf])
        copy.start()
        return copy

    def tiles(fn):
        @each(4)
        def _(i):
            fn(tile(i, H // 4))

    def pass_on(c, k, zz, send):
        arrive(c, k, 0).wait()

        def add(rs):
            psum[lax.rem(c, 2), zz, rs, :] += stage[0, rs, :]

        tiles(add)
        send.start()

    def finish(c, ks):
        for copy in [arrive(c, k, i) for i, k in enumerate(ks)]:
            copy.wait()

        def add(rs):
            v = psum[lax.rem(c, 2), z, rs, :] + stage[0, rs, :]
            if len(ks) == 2:
                v = v + stage[1, rs, :]
            r0 = pl.multiple_of((c * 2 + side) * H + rs.start, rs.size)
            xout_ref[pl.ds(r0, rs.size), cols_at(z)] = (ybuf[c, rs, :] + v).astype(BF16)

        tiles(add)
        done.start(c)

    def relay(k, c):
        pass_on(c, k, (far_end, outer, inner)[k], sums_out(c)[1][k])

    def hidden_wait(c):
        for r in range(3):
            hidden.wait(c, r)

    steps = {'O': o_start, 'hw': hidden_wait, 'f': lambda c: finish(c, (0,)), 'r4': lambda c: finish(c, (3, 4))}
    for r in range(3):
        steps['h' + 'abc'[r]] = functools.partial(hidden.serve, r)
        steps['x' + 'abc'[r]] = functools.partial(done.serve, r)
        steps['r' + '123'[r]] = functools.partial(relay, r)

    early = [pltpu.make_async_copy(src, obuf.at[:, d, :, tile(0, width)], loc_sem.at[5 + d]) for d, src in enumerate(o_first)]
    for copy in early:
        copy.start()
    each(SLOTS - 1)(issue)
    for copy in early:
        copy.wait()

    @each(AHEAD + nc + BEHIND)
    def _(t):
        j = t - AHEAD
        jj = j + 1
        active = (j >= 0) & (j < nc)

        def after(k):
            for flag, plan in ((is_mid, MID_PLAN[k]), (is_end, END_PLAN[k])):
                def run(plan=plan):
                    for name, ahead in plan:
                        c = j + ahead
                        pl.when((c >= 0) & (c < nc))(functools.partial(steps[name], c))

                if plan:
                    pl.when(flag)(run)

        @pl.when((jj >= 0) & (jj < nc))
        def _():
            project(jj, per * jj - (per - 4) * lax.div(jj + big - 1, big))
            hidden.start(jj)

        after(0)
        ld_d = per * jj - (per - 8) - 4 * lax.div(jj, nc)
        gate_up(j, ld_d, active, after)
        for part in range(2):
            pl.when(active)(lambda: down(j, ld_d + nd, part))
            after(5 + part)

    @each(nc)
    def _(c):
        @pl.when(is_end)
        def _():
            for r in range(3):
                done.wait(c, r)

        for d in (1, 2, 3):
            o_copy(c, d).wait_send()
        rdma(sstat.at[c], rstat.at[c], st_send.at[c, 0], st_recv.at[c, 0], mate).wait_send()
        hidden.drain(c)
        done.drain(c)
        pl.when(c >= nc - 2)(lambda: wait_sums_out(c))


def line_block(o_first, o_last, x, w_out, pieces, w_gate, w_up, w_down, gain):
    rows, depth = x.shape
    ff = w_gate.shape[1]
    width = o_last[0].shape[-1]
    kz = 2 * width
    nc = rows // ROWS_CH
    h, half = ROWS_CH // 2, depth // 2
    ring_rows = max(depth, ff, half // DOT_N * kz)
    sems = [pltpu.SemaphoreType.DMA((nc, n)) for n in (3, 3, 1, 1, 5, 3, 3, 5, 5, 3)]
    xout, _ = pl.pallas_call(
        functools.partial(line_kernel, nc=nc),
        in_specs=[HBM] * (11 + len(pieces)) + [VMEM],
        out_specs=[VMEM, HBM],
        out_shape=[pltpu.VMEM(x.shape, BF16), struct((nc, 5, h, half), F32)],
        scratch_shapes=[
            pltpu.VMEM((nc, 4, h, kz), BF16), pltpu.VMEM((nc, ROWS_CH, depth), BF16), pltpu.VMEM((nc, h, half), F32),
            pltpu.VMEM((SLOTS, ring_rows, DOT_N), BF16), pltpu.VMEM((2, 4, h, half), F32), pltpu.VMEM((ROWS_CH, ff), BF16),
            pltpu.VMEM((2, h, half), F32), pltpu.VMEM((h, half), BF16),
            *[pltpu.VMEM((nc, h, LANES), F32)] * 2, pltpu.SemaphoreType.DMA((SLOTS,)), pltpu.SemaphoreType.DMA((9,)), *sems,
        ],
        compiler_params=params(50, collective_id=1, has_side_effects=True),
        cost_estimate=cost(6 * x.size * ff, 2 * x.size),
        name="line_block",
    )(*(a.reshape(nc, h, width) for a in o_first), *o_last, x, w_out, *pieces, w_gate, w_up, w_down, gain.reshape(1, depth))
    return xout


def gather_w_out(w_out, tps):
    z, dp, cp = (lax.axis_index(a) for a in ('tp', 'dp', 'cp'))
    n, half = w_out.shape[0] // 8, w_out.shape[1] // 2
    q = (z + 1) // 2 % 2
    part = lax.dynamic_slice_in_dim(w_out, (dp * 4 + cp) * n, n, 0)
    same, other = (lax.dynamic_slice_in_dim(part, h * half, half, 1) for h in (q, 1 - q))
    return tuple(lax.ppermute(a, 'tp', [(i, i ^ d) for i in range(tps)]) for d, a in ((1, other), (2, other), (3, same)))


def solution(mesh):
    groups = mesh.shape['cp']
    tps = mesh.shape['tp']
    dps = mesh.shape['dp']

    def local_layer(x_loc, kp_loc, vp_loc, norm_attn, w_query, w_key, w_value, w_out, norm_mlp, w_gate, w_up, w_down):
        rows = x_loc.shape[0]
        pre_dev, kv_loc, head_dim = kp_loc.shape
        c2 = head_dim ** -0.5 * math.log2(math.e)
        me = lax.axis_index('cp')
        q_pos = block_positions(me, groups, rows // 2, pre_dev * groups)
        vals = vp_loc.reshape(pre_dev // LANES, LANES, kv_loc, head_dim).transpose(2, 0, 3, 1)
        own_pre = (kp_loc.transpose(1, 0, 2), vals.reshape(kv_loc, pre_dev, LANES))
        far_pre = swap(own_pre, 'cp', groups, 2)
        near_pre = swap(own_pre, 'cp', groups, 1)
        wo_z = gather_w_out(w_out, tps)
        cos_tab, sin_tab = rope_tables(q_pos, head_dim)
        q, own_suf, k_flat, v_flat = qkv(x_loc, norm_attn, w_query, w_key, w_value, cos_tab, sin_tab)
        far_suf, = swap((own_suf,), 'cp', groups, 2)
        near_suf, = swap((own_suf,), 'cp', groups, 1)
        o_first, o_last, wo_pieces = attend(q, own_pre, near_pre, far_pre, own_suf, near_suf, far_suf, wo_z, c2, groups, tps, dps)
        x_out = line_block(o_first, o_last, x_loc, w_out, wo_pieces, w_gate, w_up, w_down, norm_mlp)
        return x_out, k_flat.reshape(rows, kv_loc, head_dim), v_flat.reshape(rows, kv_loc, head_dim)

    row_spec = P(('dp', 'cp'), None)
    kv_spec = P(('dp', 'cp'), 'tp', None)
    col_spec = P(None, 'tp')
    row_split = P('tp', None)
    vec_spec = P(None)
    return jax.shard_map(local_layer, mesh=mesh, in_specs=(row_spec, kv_spec, kv_spec, vec_spec, col_spec, col_spec, col_spec, row_split, vec_spec, col_spec, col_spec, row_split), out_specs=(row_spec, kv_spec, kv_spec), check_vma=False)
```

```python
import functools
import math

import jax
import jax.numpy as jnp
from jax import lax
from jax.experimental import pallas as pl
from jax.experimental.pallas import tpu as pltpu
from jax.sharding import PartitionSpec as P


ROPE_THETA = 500000.0
NORM_EPS = 1e-5
ROWS_CH = 128
F32 = jnp.float32
BF16 = jnp.bfloat16
HBM = pl.BlockSpec(memory_space=pl.ANY)
VMEM = pl.BlockSpec(memory_space=pltpu.VMEM)
IN_HBM = pl.BlockSpec(memory_space=pltpu.HBM)
LANES = 128
PAIR = 2 * LANES
NT = (((1,), (1,)), ((), ()))
each = functools.partial(pl.loop, 0)


def tile(i, n):
    return pl.ds(pl.multiple_of(i * n, n), n)


def params(mib, **more):
    return pltpu.CompilerParams(vmem_limit_bytes=mib * 2**20, **more)


def cost(flops, moved):
    return pl.CostEstimate(flops=flops, bytes_accessed=moved, transcendentals=0)


def struct(shape, dtype):
    return jax.ShapeDtypeStruct(shape, dtype)


def block_positions(owner, groups, blk_len, prefix_len):
    local_row = jnp.arange(2 * blk_len, dtype=jnp.int32)
    blk_idx = jnp.where(local_row < blk_len, owner, 2 * groups - 1 - owner)
    return prefix_len + blk_idx * blk_len + local_row % blk_len


def rope_tables(positions, head_dim):
    inv_freq = ROPE_THETA ** (-jnp.arange(0, head_dim, 2, dtype=F32) / head_dim)
    angles = positions.astype(F32)[:, None] * inv_freq[None, :]
    cos_tab, sin_tab = jnp.cos(angles), jnp.sin(angles)
    return jnp.concatenate([cos_tab, cos_tab], axis=1), jnp.concatenate([-sin_tab, sin_tab], axis=1)


def qkv_kernel(x_hbm, g_ref, wq_ref, wk_ref, wv_ref, cos_ref, sin_ref, q_ref, kv_ref, kf_ref, vf_ref, x_ref, h_ref, sems, *, nq):
    step = pl.program_id(0)
    rows = x_ref.shape[0]
    parts, rt = sems.shape[0], 32

    @pl.when(step == 0)
    def _():
        n = rows // parts
        copies = [pltpu.make_async_copy(x_hbm.at[tile(i, n), :], x_ref.at[tile(i, n), :], sems.at[i]) for i in range(parts)]
        for copy in copies:
            copy.start()
        for i, copy in enumerate(copies):
            copy.wait()

            @pl.loop(i * n // rt, (i + 1) * n // rt, unroll=2)
            def _(j):
                sl = tile(j, rt)
                xv = x_ref[sl, :].astype(F32)
                inv = lax.rsqrt(jnp.mean(xv * xv, axis=-1, keepdims=True) + NORM_EPS)
                h_ref[sl, :] = (xv * inv * g_ref[...].astype(F32)).astype(BF16)

    def rope(block, sl):
        return (block * cos_ref[sl, :] + pltpu.roll(block, 64, axis=1) * sin_ref[sl, :]).astype(BF16)

    mt = rows

    def project(w_ref, store):
        @each(rows // mt)
        def _(i):
            sl = tile(i, mt)
            acc = jnp.dot(h_ref[sl, :], w_ref[...], preferred_element_type=F32)
            store(acc, sl)

    def heads_of(acc):
        return [(t, slice(t * LANES, (t + 1) * LANES), acc[:, t * LANES:(t + 1) * LANES]) for t in range(2)]

    def store_q(acc, sl):
        for _, cs, part in heads_of(acc):
            q_ref[sl, cs] = rope(part, sl)

    def store_k(acc, sl):
        for t, cs, part in heads_of(acc):
            kf_ref[sl, cs] = rope(part, sl)
            kv_ref[0, t, sl, :] = kf_ref[sl, cs]

    def store_v(acc, sl):
        vf_ref[sl, :] = acc.astype(BF16)
        for t, _, part in heads_of(acc):
            for b in range(mt // LANES):
                kv_ref[1, t, pl.ds(sl.start + b * LANES, LANES), :] = part[b * LANES:(b + 1) * LANES].T.astype(BF16)

    pl.when(step < nq)(lambda: project(wq_ref, store_q))
    pl.when(step == nq)(lambda: project(wk_ref, store_k))
    pl.when(step == nq + 1)(lambda: project(wv_ref, store_v))


def qkv(x, gain, wq, wk, wv, cos_tab, sin_tab):
    rows, depth = x.shape
    nq = wq.shape[1] // PAIR

    def fixed(shape):
        return pl.BlockSpec(shape, lambda j: tuple(0 for _ in shape))

    def whole(shape):
        return pl.BlockSpec(shape, lambda j: tuple(0 for _ in shape), pipeline_mode=pl.Buffered(1))

    def columns(n):
        return pl.BlockSpec((n, PAIR), lambda j: (0, jnp.minimum(j, nq - 1)))

    flat, by_head = (rows, PAIR), (2, 2, rows, LANES)
    return pl.pallas_call(
        functools.partial(qkv_kernel, nq=nq),
        grid=(nq + 2,),
        in_specs=[HBM, whole((1, depth)), columns(depth), fixed(wk.shape), fixed(wv.shape), whole(cos_tab.shape), whole(sin_tab.shape)],
        out_specs=[columns(rows), fixed(by_head), fixed(flat), fixed(flat)],
        out_shape=[struct(s, BF16) for s in ((rows, nq * PAIR), by_head, flat, flat)],
        scratch_shapes=[pltpu.VMEM((rows, depth), BF16), pltpu.VMEM((rows, depth), BF16), pltpu.SemaphoreType.DMA((4,))],
        compiler_params=params(58, dimension_semantics=("arbitrary",)),
        cost_estimate=cost(2 * rows * depth * (nq + 2) * PAIR, 2 * depth * rows),
        name="qkv",
    )(x, gain.reshape(1, depth), wq, wk, wv, cos_tab, sin_tab)


NQ = 512
PER_KV = 4


class Fetch:
    def __init__(self, sems):
        self.sems, self.used = sems, 0

    def start(self, pairs):
        copies = []
        for src, dst in pairs:
            copies.append(pltpu.make_async_copy(src, dst, self.sems.at[self.used]))
            self.used += 1
        for copy in copies:
            copy.start()
        return copies


def settle(copies):
    for copy in copies:
        copy.wait()


def q_block(q_ref, head, half):
    return q_ref[tile(half, NQ), tile(head, LANES)]


def across(blocks):
    return jnp.concatenate([blocks[i:i + LANES] for i in range(0, blocks.shape[0], LANES)], axis=1)


def attend_items(q_ref, kb_ref, vb_ref, acc_ref, m_ref, l_ref, pbufs, n_items, item, bk, c2, diag=False):
    depth = len(pbufs)

    def scores(i, pb):
        head, half, start = item(i)
        n = head * 2 + half
        ks = kb_ref[head // PER_KV, pl.ds(pl.multiple_of(start, bk), bk), :]
        s = lax.dot_general(ks, q_block(q_ref, head, half), NT, preferred_element_type=F32)
        e = jnp.exp2(s * c2 - m_ref[n])
        if diag:
            seen = lax.broadcasted_iota(jnp.int32, (bk, NQ), 0) <= lax.broadcasted_iota(jnp.int32, (bk, NQ), 1)
            e = jnp.where(seen, e, 0.0)
        pb[...] = e.astype(BF16)
        l_ref[n] += jnp.sum(e.reshape(-1, *l_ref.shape[1:]), axis=0)

    def values(i, pb):
        head, half, start = item(i)
        vt = across(vb_ref[head // PER_KV, pl.ds(pl.multiple_of(start, bk), bk), :])
        acc_ref[head * 2 + half] += jnp.dot(vt, pb[...], preferred_element_type=F32)

    scores(0, pbufs[0])

    def body(g, carry):
        for u in range(depth):
            i = g * depth + u
            scores(i + 1, pbufs[(u + 1) % depth])
            values(i, pbufs[u])
        return carry

    trips = n_items // depth - 1
    lax.fori_loop(0, trips, body, 0)
    for u in range(depth):
        if u + 1 < depth:
            scores(trips * depth + u + 1, pbufs[u + 1])
        values(trips * depth + u, pbufs[u])


def prefix_kernel(q_hbm, ka, va, kb, vb, acc_out, m_out, l_out, q_ref, kbuf, vbuf, acc_ref, m_ref, l_ref, pa, pb, sems, *, heads, c2):
    fetch = Fetch(sems)
    n = ka.shape[1]
    settle(fetch.start([(q_hbm, q_ref), (ka, kbuf.at[:, tile(0, n), :]), (va, vbuf.at[:, tile(0, n), :]), (kb, kbuf.at[:, tile(1, n), :]), (vb, vbuf.at[:, tile(1, n), :])]))

    @each(heads // PER_KV)
    def _(group):
        for j in range(2 * PER_KV):
            i = group * 2 * PER_KV + j
            s = lax.dot_general(kbuf[group, tile(0, LANES), :], q_block(q_ref, i // 2, j % 2), NT, preferred_element_type=F32)
            m_ref[i] = jnp.max(s, axis=0, keepdims=True) * c2

    for ref in (acc_ref, l_ref):
        ref[...] = jnp.zeros_like(ref)
    bk = 2 * NQ
    per = kbuf.shape[1] // bk

    def item(i):
        pair = i // per
        return pair // 2, pair % 2, (i % per) * bk

    attend_items(q_ref, kbuf, vbuf, acc_ref, m_ref, l_ref, (pa, pb), heads * 2 * per, item, bk, c2)
    settle(fetch.start([(acc_ref, acc_out), (m_ref, m_out), (l_ref, l_out)]))


def state_shapes(heads):
    return [struct((heads * 2, n, NQ), F32) for n in (LANES, 1, 8)]


def vmem_like(shapes):
    return [pltpu.VMEM(s.shape, s.dtype) for s in shapes]


def attend_prefix(q, pieces, c2):
    heads = q.shape[1] // LANES
    flat = [a for p in pieces for a in p]
    n = 2 * pieces[0][0].shape[1]
    shapes = state_shapes(heads)
    return pl.pallas_call(
        functools.partial(prefix_kernel, heads=heads, c2=c2),
        in_specs=[HBM] * (1 + len(flat)),
        out_specs=[HBM] * len(shapes),
        out_shape=[pltpu.HBM(s.shape, s.dtype) for s in shapes],
        scratch_shapes=[
            *vmem_like([q]), *[pltpu.VMEM((2, n, LANES), BF16)] * 2, *vmem_like(shapes),
            *[pltpu.VMEM((2 * NQ, NQ), BF16)] * 2, pltpu.SemaphoreType.DMA((8,)),
        ],
        compiler_params=params(58),
        cost_estimate=cost(4 * q.size * n, 4 * q.size),
        name="attend_prefix",
    )(q, *flat)


def rest_kernel(*refs, group, groups, c2, axis):
    q_hbm, *refs = refs
    flat, suf, refs = refs[:2 * groups], refs[2 * groups:3 * groups], refs[3 * groups:]
    pre = list(zip(flat[::2], flat[1::2]))
    acc_in, m_in, l_in, here_out, there_out, q_ref, kbuf, vbuf, ksuf, vsuf, acc_ref, m_ref, l_ref, acc_old, l_old, o_ref, bad_ref, sems, wa, wb, pa, pb, pc, pd = refs
    heads = PER_KV
    me = lax.axis_index(axis)
    fetch = Fetch(sems)
    mine = pl.ds(group * heads * 2, heads * 2)
    n_pre, n_suf = pre[0][0].shape[1], suf[0].shape[2]
    first = fetch.start([(q_hbm.at[:, tile(group, heads * LANES)], q_ref), (m_in.at[mine], m_ref)])
    for i, (kr, vr) in enumerate(pre[2:]):
        first += fetch.start([(kr.at[group], kbuf.at[0, tile(i, n_pre), :]), (vr.at[group], vbuf.at[0, tile(i, n_pre), :])])
    second = []
    for i, kv in enumerate(suf):
        second += fetch.start([(kv.at[j, group], buf.at[0, tile(i, n_suf), :]) for j, buf in enumerate((ksuf, vsuf))])
    third = fetch.start([(acc_in.at[mine], acc_old), (l_in.at[mine], l_old)])
    for ref in (acc_ref, l_ref):
        ref[...] = jnp.zeros_like(ref)
    settle(first)
    bk = 2 * NQ
    per = kbuf.shape[1] // bk

    def pre_item(i):
        pair = i // per
        return pair // 2, pair % 2, (i % per) * bk

    attend_items(q_ref, kbuf, vbuf, acc_ref, m_ref, l_ref, (wa, wb), heads * 2 * per, pre_item, bk, c2)
    settle(second)
    last = 2 * groups - 1

    def locate(blk):
        late = (blk >= groups).astype(jnp.int32)
        owner = jnp.where(blk < groups, blk, last - blk)
        diff = (owner % 2 != me % 2).astype(jnp.int32) + 2 * (owner // 2 != me // 2).astype(jnp.int32)
        return (diff * 2 + late) * NQ

    def full_item(i):
        head, r = i // last, i % last
        half = (r >= me).astype(jnp.int32)
        return head, half, locate(jnp.where(r < me, r, r - me))

    def diag_item(i):
        half = i % 2
        return i // 2, half, locate(jnp.where(half == 0, me, last - me))

    attend_items(q_ref, ksuf, vsuf, acc_ref, m_ref, l_ref, (pa, pb, pc, pd), heads * last, full_item, NQ, c2)
    attend_items(q_ref, ksuf, vsuf, acc_ref, m_ref, l_ref, (pa, pb), heads * 2, diag_item, NQ, c2, diag=True)
    settle(third)
    bad_ref[...] = jnp.zeros_like(bad_ref)
    chunk = ROWS_CH // 2

    def write(head, half, acc, total):
        out = (acc * (1.0 / total)).T.astype(BF16)
        n_p = NQ // chunk
        for p in range(n_p):
            o_ref[p % 2, tile(half * (n_p // 2) + p // 2, chunk), tile(head, LANES)] = out[p * chunk:(p + 1) * chunk]

    @each(heads)
    def _(head):
        for half in range(2):
            i = head * 2 + half
            acc = acc_ref[i] + acc_old[i]
            total = jnp.sum(l_ref[i] + l_old[i], axis=0, keepdims=True)
            bad = jnp.where((jnp.abs(acc) < jnp.inf) & (total < jnp.inf), 0.0, 1.0)
            for j in range(NQ // LANES):
                part = bad[:, j * LANES:(j + 1) * LANES]
                bad_ref[...] = jnp.maximum(bad_ref[...], jnp.max(part.reshape(-1, *bad_ref.shape), axis=0))
            write(head, half, acc, total)

    @pl.when(jnp.max(bad_ref[...]) > 0.0)
    def _():
        @each(heads * 2)
        def _(i):
            head, half = i // 2, i % 2
            q = q_block(q_ref, head, half)
            m_ref[i] = jnp.full((1, NQ), -jnp.inf, F32)
            for ref in (acc_ref, l_ref):
                ref[i] = jnp.zeros(ref.shape[1:], F32)

            def update(ks, vt, seen):
                s = lax.dot_general(ks, q, NT, preferred_element_type=F32) * c2
                if seen is not None:
                    s = jnp.where(seen, s, -jnp.inf)
                m_old = m_ref[i]
                m_new = jnp.maximum(m_old, jnp.max(s, axis=0, keepdims=True))
                alpha = jnp.exp2(m_old - m_new)
                e = jnp.exp2(s - m_new)
                m_ref[i] = m_new
                l_ref[i] = l_ref[i] * alpha + jnp.sum(e.reshape(-1, *l_ref.shape[1:]), axis=0)
                acc_ref[i] = acc_ref[i] * alpha + jnp.dot(vt, e.astype(BF16), preferred_element_type=F32)

            kpre, vpre = (p.at[:, tile(0, LANES)] for p in (pa, pb))
            for kr, vr in pre:
                @each(n_pre // NQ)
                def _(j):
                    pltpu.sync_copy(kr.at[group, tile(j, NQ), :], kpre)
                    pltpu.sync_copy(vr.at[group, tile(j, NQ), :], vpre)
                    update(kpre[...], across(vpre[...]), None)

            mine_blk = jnp.where(half == 0, me, last - me)

            @each(2 * groups)
            def _(blk):
                @pl.when(blk <= mine_blk)
                def _():
                    start = pl.ds(pl.multiple_of(locate(blk), NQ), NQ)
                    seen = (lax.broadcasted_iota(jnp.int32, (NQ, NQ), 0) <= lax.broadcasted_iota(jnp.int32, (NQ, NQ), 1)) | (blk < mine_blk)
                    update(ksuf[0, start, :], across(vsuf[0, start, :]), seen)

            write(head, half, acc_ref[i], jnp.sum(l_ref[i], axis=0, keepdims=True))

    side = lax.axis_index('tp') // 2
    settle(fetch.start([(o_ref.at[side], here_out), (o_ref.at[1 - side], there_out)]))


def attend_rest(q, pre, suf, state, c2, axis, group):
    rows, groups, width = q.shape[0], len(suf), PER_KV * LANES
    n_pre, n_suf = 2 * pre[0][0].shape[1], groups * suf[0].shape[2]
    flat = [a for p in pre for a in p] + list(suf)
    acc, m, total = state_shapes(PER_KV)
    out = pltpu.HBM((rows // 2, width), BF16)
    return pl.pallas_call(
        functools.partial(rest_kernel, group=group, groups=groups, c2=c2, axis=axis),
        in_specs=[IN_HBM] + [HBM] * len(flat) + [IN_HBM] * 3,
        out_specs=[HBM] * 2,
        out_shape=[out] * 2,
        scratch_shapes=[
            pltpu.VMEM((rows, width), BF16), *[pltpu.VMEM((1, n, LANES), BF16) for n in (n_pre, n_pre, n_suf, n_suf)], *vmem_like([acc, m, total, acc, total, struct((2, rows // 2, width), BF16)]),
            pltpu.VMEM((8, LANES), F32), pltpu.SemaphoreType.DMA((22,)), *[pltpu.VMEM((2 * NQ, NQ), BF16)] * 2, *[pltpu.VMEM((NQ, NQ), BF16)] * 4,
        ],
        compiler_params=params(42),
        cost_estimate=cost(2 * rows * width * (2 * n_pre + n_suf), 4 * q.size),
        name="attend_rest",
    )(q, *flat, *state)


def swap(arrays, axis, groups, bit):
    return tuple(lax.ppermute(a, axis, [(i, i ^ bit) for i in range(groups)]) for a in arrays)


def attend(q, own_pre, near_pre, far_pre, own_suf, near_suf, far_suf, wo_z, c2, groups, tps, dps):
    state = attend_prefix(q, (own_pre, near_pre), c2)
    far_pre, far_suf, wo_z, state = lax.optimization_barrier((far_pre, far_suf, wo_z, state))
    cross_pre = swap(far_pre, 'cp', groups, 1)
    cross_suf, = swap((far_suf,), 'cp', groups, 1)
    wo = jnp.stack(wo_z)
    wo_x, = swap((wo,), 'dp', dps, 1)
    wo_y, = swap((wo,), 'cp', groups, 2)
    pre, suf = (own_pre, near_pre, far_pre, cross_pre), (own_suf, near_suf, far_suf, cross_suf)
    here, there = attend_rest(q, pre, suf, state, c2, 'cp', 0)
    o_far = tuple(lax.ppermute(there, 'tp', [(i, i ^ d) for i in range(tps)]) for d in (2, 3))
    o_mate = swap((here,), 'tp', tps, 1)
    wo, wo_x, wo_y, there, q = lax.optimization_barrier((wo, wo_x, wo_y, there, q))
    wo_xy, = swap((wo_x,), 'cp', groups, 2)
    near = swap((wo, wo_x, wo_y), 'cp', groups, 1)
    o_last = attend_rest(q, pre, suf, state, c2, 'cp', 1)
    wo_xy, o_last = lax.optimization_barrier((wo_xy, o_last))
    return (here,) + o_mate + o_far, o_last, (wo, wo_x, wo_y, wo_xy) + near + swap((wo_xy,), 'cp', groups, 1)


MESH = pl.DeviceIdType.MESH
DOT_N = 512
SLOTS = 3
MID_PLAN = ((('r3', -1),), (('xc', -3), ('r2', -1), ('hb', 1), ('ha', 1),), (('xb', -2), ('xa', -2),), (('O', 3),), (('r4', -1),), (), (('hc', 1), ('r1', 0),))
END_PLAN = ((('hw', 0), ('f', -2),), (('O', 3),), (), (), (), (), ())
AHEAD, BEHIND = 3, 3


def side_of(z):
    return lax.div(z, 2)


def colhalf_of(z):
    return lax.rem(lax.div(z + 1, 2), 2)


def line_kernel(*refs, nc):
    o_first, o_last, x_ref, wo_ref, *refs = refs[:4], refs[4:6], *refs[6:]
    wo_pieces, refs = refs[:8], refs[8:]
    wg_ref, wu_ref, wd_ref, gain_ref, xout_ref, land_ref = refs[:6]
    (obuf, h2, ybuf, ring, psum, act, stage, xs, sstat, rstat,
     ring_sem, loc_sem, o_send, o_recv, st_send, st_recv, a1_send, a1_recv, rs_send, rs_recv, a2_send, a2_recv) = refs[6:]
    R, H = ROWS_CH, ROWS_CH // 2
    depth = wg_ref.shape[0]
    ff = wg_ref.shape[1]
    half = depth // 2
    width = o_last[0].shape[-1]
    kz = 2 * width
    n_ct = half // DOT_N
    nd, ne = ff // PAIR, depth // DOT_N
    per = 4 + nd + ne
    total_loads = nc * per
    big = 1024

    z = lax.axis_index('tp')
    dp = lax.axis_index('dp')
    cp = lax.axis_index('cp')
    core, chip = lax.rem(cp, 2), lax.div(cp, 2)
    side, q = side_of(z), colhalf_of(z)
    is_mid = q == 1
    is_end = q != 1
    near = 1 + side
    outer = 3 * side
    inner = 2 - side
    far_end = 3 - 3 * side
    peers = {1: z + 1 - 2 * lax.rem(z, 2), 2: lax.rem(z + 2, 4), 3: 3 - z}
    mate = peers[1]

    def rdma(src, dst, ssem, rsem, dev):
        return pltpu.make_async_remote_copy(src_ref=src, dst_ref=dst, send_sem=ssem, recv_sem=rsem, device_id={'tp': dev}, device_id_type=MESH)

    def rows_at(zz):
        return tile(side_of(zz), H)

    def cols_at(zz):
        return tile(colhalf_of(zz), half)

    barrier = pltpu.get_barrier_semaphore()
    for d in (1, 2, 3):
        pl.semaphore_signal(barrier, inc=1, device_id={'tp': peers[d]}, device_id_type=MESH)
    pl.semaphore_wait(barrier, 3)

    def load_kind(ld):
        u = ld + (per - 4)
        i1 = lax.div(u, per)
        a = lax.div(i1 + big - 1, big)
        t = lax.rem(u, per) + 4 * lax.div(i1, nc)
        return a * t + (1 - a) * ld

    def issue(ld):
        slot = lax.rem(ld, SLOTS)
        sem = ring_sem.at[slot]
        t = load_kind(ld)

        def start(src, dst):
            pltpu.make_async_copy(src, dst, sem).start()

        for d in range(4):
            @pl.when(t == d)
            def _():
                @each(n_ct)
                def _(ct):
                    c0 = pl.multiple_of(ct * DOT_N, DOT_N)
                    if d == 0:
                        cs = tile(q * n_ct + ct, DOT_N)
                        start(wo_ref.at[:, cs], ring.at[slot, tile(ct, kz), :])
                    else:
                        for k, piece in enumerate(wo_pieces):
                            bits = (dp, k % 2), (chip, k // 2 % 2), (core, k // 4)
                            n = piece.shape[1]
                            j = sum((own + x - 2 * own * x) * w for (own, x), w in zip(bits, (4, 2, 1)))
                            r0 = pl.multiple_of(ct * kz + j * n, n)
                            start(piece.at[d - 1, :, pl.ds(c0, DOT_N)], ring.at[slot, pl.ds(r0, n), :])

        @pl.when((t >= 4) & (t < 4 + nd))
        def _():
            cs = pl.ds(pl.multiple_of((t - 4) * 256, 256), 256)
            start(wg_ref.at[:, cs], ring.at[slot, :depth, :PAIR])
            start(wu_ref.at[:, cs], ring.at[slot, :depth, PAIR:])

        @pl.when(t >= 4 + nd)
        def _():
            cs = pl.ds(pl.multiple_of((t - 4 - nd) * DOT_N, DOT_N), DOT_N)
            start(wd_ref.at[:, cs], ring.at[slot, :ff, :])

    def take(ld, n_rows):
        slot = lax.rem(ld, SLOTS)
        whole = ring.at[slot, :n_rows, :]
        pltpu.make_async_copy(whole, whole, ring_sem.at[slot]).wait()
        pl.when(ld + SLOTS - 1 < total_loads)(lambda: issue(ld + SLOTS - 1))
        return slot

    def late(c, d):
        return obuf.at[c, d, :, tile(1, width)]

    def o_copy(c, d):
        return rdma(o_last[int(d > 1)].at[tile(c, H), :], late(c, d), o_send.at[c, d - 1], o_recv.at[c, d - 1], peers[d])

    def o_start(c):
        for d in (1, 2, 3):
            o_copy(c, d).start()

    def project(c, ld0):
        own_o = pltpu.make_async_copy(o_last[0].at[tile(c, H), :], late(c, 0), loc_sem.at[0])
        own_x = pltpu.make_async_copy(x_ref.at[tile(c * 2 + side, H), cols_at(z)], xs, loc_sem.at[1])
        own_o.start()
        own_x.start()
        for d in (1, 2, 3):
            o_copy(c, d).wait_recv()
        own_o.wait()
        own_x.wait()

        @each(n_ct)
        def _(ct):
            cs = tile(ct, DOT_N)
            ybuf[c, :, cs] = xs[:, cs].astype(F32)

        @each(4)
        def _(d):
            slot = take(ld0 + d, n_ct * kz)

            @each(n_ct)
            def _(ct):
                cs = tile(ct, DOT_N)
                w = ring[slot, tile(ct, kz), :]
                ybuf[c, :, cs] += jnp.dot(obuf[c, d], w, preferred_element_type=F32)

        sstat[c] = jnp.zeros((H, LANES), F32)

        @each(n_ct)
        def _(ct):
            yv = ybuf[c, :, tile(ct, DOT_N)]
            sstat[c] += jnp.broadcast_to(jnp.sum(yv * yv, axis=-1, keepdims=True), (H, LANES))

        swap_stat = rdma(sstat.at[c], rstat.at[c], st_send.at[c, 0], st_recv.at[c, 0], mate)
        swap_stat.start()
        swap_stat.wait_recv()
        inv = lax.rsqrt((sstat[c] + rstat[c])[:, 0:1] * (1.0 / depth) + NORM_EPS)

        @each(n_ct)
        def _(ct):
            cs = tile(ct, DOT_N)
            gs = tile(q * n_ct + ct, DOT_N)
            h2[c, rows_at(z), gs] = (ybuf[c, :, cs] * inv * gain_ref[:, gs].astype(F32)).astype(BF16)

    class Spread:
        def __init__(self, block, send, recv):
            self.block, self.send, self.recv = block, send, recv

        def copy(self, c, zz, s, r, dev):
            return rdma(self.block(c, zz), self.block(c, zz), self.send.at[c, s], self.recv.at[c, r], dev)

        def to_near(self, c):
            return self.copy(c, z, 0, 0, near)

        def to_outer(self, c):
            return self.copy(c, z, 0, 0, outer)

        def to_inner(self, c):
            return self.copy(c, z, 1, 1, inner)

        def end_to_inner(self, c):
            return self.copy(c, outer, 2, 2, inner)

        def inner_to_outer(self, c):
            return self.copy(c, inner, 3, 1, outer)

        def far_to_outer(self, c):
            return self.copy(c, far_end, 4, 2, outer)

        def start(self, c):
            pl.when(is_end)(lambda: self.to_near(c).start())

            @pl.when(is_mid)
            def _():
                self.to_outer(c).start()
                self.to_inner(c).start()

        def wait(self, c, r):
            self.copy(c, z, 0, r, mate).wait_recv()

        def serve(self, r, c):
            self.wait(c, r)
            (self.end_to_inner, self.inner_to_outer, self.far_to_outer)[r](c).start()

        def drain(self, c):
            @pl.when(is_end)
            def _():
                self.to_near(c).wait_send()

            @pl.when(is_mid)
            def _():
                for copy in (self.to_outer(c), self.to_inner(c), self.end_to_inner(c), self.inner_to_outer(c), self.far_to_outer(c)):
                    copy.wait_send()

    hidden = Spread(lambda c, zz: h2.at[c, rows_at(zz), cols_at(zz)], a1_send, a1_recv)

    done = Spread(lambda c, zz: xout_ref.at[tile(c * 2 + side_of(zz), H), cols_at(zz)], a2_send, a2_recv)

    def gate_up(c, ld0, active, after):
        @each(nd)
        def _(i):
            @pl.when(active)
            def _():
                slot = take(ld0 + i, depth)
                gu = jnp.dot(h2[c], ring[slot, :depth, :], preferred_element_type=F32)
                g, u = gu[:, :PAIR], gu[:, PAIR:]
                act[:, tile(i, PAIR)] = (g * (1.0 / (1.0 + jnp.exp(-g))) * u).astype(BF16)

            for k in range(4):
                pl.when(i == (k + 1) * nd // 4 - 1)(functools.partial(after, k + 1))

    def ps_copy(c, k_send, zz, k_recv, dev):
        return rdma(psum.at[lax.rem(c, 2), zz], land_ref.at[c, k_recv], rs_send.at[c, k_send], rs_recv.at[c, k_recv], dev)

    def sums_out(c):
        ends = (ps_copy(c, 0, far_end, 0, near), ps_copy(c, 1, inner, 2, near), ps_copy(c, 2, near, 3, near))
        mids = (ps_copy(c, 0, far_end, 1, inner), ps_copy(c, 1, outer, 0, outer), ps_copy(c, 2, inner, 4, inner))
        return ends, mids

    def wait_sums_out(c):
        ends, mids = sums_out(c)
        for flag, copies in ((is_end, ends), (is_mid, mids)):
            @pl.when(flag)
            def _():
                for copy in copies:
                    copy.wait_send()

    def down(c, ld0, part):
        ps = lax.rem(c, 2)
        ends, _ = sums_out(c)
        if part == 0:
            pl.when(c >= 2)(lambda: wait_sums_out(c - 2))

        @each(ne // 2)
        def _(i):
            slot = take(ld0 + part * (ne // 2) + i, ff)
            pv = jnp.dot(act[...], ring[slot, :ff, :], preferred_element_type=F32)
            cs = tile(i, DOT_N)
            psum[ps, part, :, cs] = pv[:H]
            psum[ps, 3 - part, :, cs] = pv[H:R]

        @pl.when(is_end)
        def _():
            for copy in (ends[:1], ends[1:])[part]:
                copy.start()

    def arrive(c, k, buf):
        ps_copy(c, 0, z, k, mate).wait_recv()
        copy = pltpu.make_async_copy(land_ref.at[c, k], stage.at[buf], loc_sem.at[2 + buf])
        copy.start()
        return copy

    def tiles(fn):
        @each(4)
        def _(i):
            fn(tile(i, H // 4))

    def pass_on(c, k, zz, send):
        arrive(c, k, 0).wait()

        def add(rs):
            psum[lax.rem(c, 2), zz, rs, :] += stage[0, rs, :]

        tiles(add)
        send.start()

    def finish(c, ks):
        for copy in [arrive(c, k, i) for i, k in enumerate(ks)]:
            copy.wait()

        def add(rs):
            v = psum[lax.rem(c, 2), z, rs, :] + stage[0, rs, :]
            if len(ks) == 2:
                v = v + stage[1, rs, :]
            r0 = pl.multiple_of((c * 2 + side) * H + rs.start, rs.size)
            xout_ref[pl.ds(r0, rs.size), cols_at(z)] = (ybuf[c, rs, :] + v).astype(BF16)

        tiles(add)
        done.start(c)

    def relay(k, c):
        pass_on(c, k, (far_end, outer, inner)[k], sums_out(c)[1][k])

    def hidden_wait(c):
        for r in range(3):
            hidden.wait(c, r)

    steps = {'O': o_start, 'hw': hidden_wait, 'f': lambda c: finish(c, (0,)), 'r4': lambda c: finish(c, (3, 4))}
    for r in range(3):
        steps['h' + 'abc'[r]] = functools.partial(hidden.serve, r)
        steps['x' + 'abc'[r]] = functools.partial(done.serve, r)
        steps['r' + '123'[r]] = functools.partial(relay, r)

    early = [pltpu.make_async_copy(src, obuf.at[:, d, :, tile(0, width)], loc_sem.at[5 + d]) for d, src in enumerate(o_first)]
    for copy in early:
        copy.start()
    each(SLOTS - 1)(issue)
    for copy in early:
        copy.wait()

    @each(AHEAD + nc + BEHIND)
    def _(t):
        j = t - AHEAD
        jj = j + 1
        active = (j >= 0) & (j < nc)

        def after(k):
            for flag, plan in ((is_mid, MID_PLAN[k]), (is_end, END_PLAN[k])):
                def run(plan=plan):
                    for name, ahead in plan:
                        c = j + ahead
                        pl.when((c >= 0) & (c < nc))(functools.partial(steps[name], c))

                if plan:
                    pl.when(flag)(run)

        @pl.when((jj >= 0) & (jj < nc))
        def _():
            project(jj, per * jj - (per - 4) * lax.div(jj + big - 1, big))
            hidden.start(jj)

        after(0)
        ld_d = per * jj - (per - 8) - 4 * lax.div(jj, nc)
        gate_up(j, ld_d, active, after)
        for part in range(2):
            pl.when(active)(lambda: down(j, ld_d + nd, part))
            after(5 + part)

    @each(nc)
    def _(c):
        @pl.when(is_end)
        def _():
            for r in range(3):
                done.wait(c, r)

        for d in (1, 2, 3):
            o_copy(c, d).wait_send()
        rdma(sstat.at[c], rstat.at[c], st_send.at[c, 0], st_recv.at[c, 0], mate).wait_send()
        hidden.drain(c)
        done.drain(c)
        pl.when(c >= nc - 2)(lambda: wait_sums_out(c))


def line_block(o_first, o_last, x, w_out, pieces, w_gate, w_up, w_down, gain):
    rows, depth = x.shape
    ff = w_gate.shape[1]
    width = o_last[0].shape[-1]
    kz = 2 * width
    nc = rows // ROWS_CH
    h, half = ROWS_CH // 2, depth // 2
    ring_rows = max(depth, ff, half // DOT_N * kz)
    sems = [pltpu.SemaphoreType.DMA((nc, n)) for n in (3, 3, 1, 1, 5, 3, 3, 5, 5, 3)]
    xout, _ = pl.pallas_call(
        functools.partial(line_kernel, nc=nc),
        in_specs=[HBM] * (11 + len(pieces)) + [VMEM],
        out_specs=[VMEM, HBM],
        out_shape=[pltpu.VMEM(x.shape, BF16), struct((nc, 5, h, half), F32)],
        scratch_shapes=[
            pltpu.VMEM((nc, 4, h, kz), BF16), pltpu.VMEM((nc, ROWS_CH, depth), BF16), pltpu.VMEM((nc, h, half), F32),
            pltpu.VMEM((SLOTS, ring_rows, DOT_N), BF16), pltpu.VMEM((2, 4, h, half), F32), pltpu.VMEM((ROWS_CH, ff), BF16),
            pltpu.VMEM((2, h, half), F32), pltpu.VMEM((h, half), BF16),
            *[pltpu.VMEM((nc, h, LANES), F32)] * 2, pltpu.SemaphoreType.DMA((SLOTS,)), pltpu.SemaphoreType.DMA((9,)), *sems,
        ],
        compiler_params=params(50, collective_id=1, has_side_effects=True),
        cost_estimate=cost(6 * x.size * ff, 2 * x.size),
        name="line_block",
    )(*(a.reshape(nc, h, width) for a in o_first), *o_last, x, w_out, *pieces, w_gate, w_up, w_down, gain.reshape(1, depth))
    return xout


def gather_w_out(w_out, tps):
    z, dp, cp = (lax.axis_index(a) for a in ('tp', 'dp', 'cp'))
    n, half = w_out.shape[0] // 8, w_out.shape[1] // 2
    q = (z + 1) // 2 % 2
    part = lax.dynamic_slice_in_dim(w_out, (dp * 4 + cp) * n, n, 0)
    same, other = (lax.dynamic_slice_in_dim(part, h * half, half, 1) for h in (q, 1 - q))
    return tuple(lax.ppermute(a, 'tp', [(i, i ^ d) for i in range(tps)]) for d, a in ((1, other), (2, other), (3, same)))


def solution(mesh):
    groups = mesh.shape['cp']
    tps = mesh.shape['tp']
    dps = mesh.shape['dp']

    def local_layer(x_loc, kp_loc, vp_loc, norm_attn, w_query, w_key, w_value, w_out, norm_mlp, w_gate, w_up, w_down):
        rows = x_loc.shape[0]
        pre_dev, kv_loc, head_dim = kp_loc.shape
        c2 = head_dim ** -0.5 * math.log2(math.e)
        me = lax.axis_index('cp')
        q_pos = block_positions(me, groups, rows // 2, pre_dev * groups)
        vals = vp_loc.reshape(pre_dev // LANES, LANES, kv_loc, head_dim).transpose(2, 0, 3, 1)
        own_pre = (kp_loc.transpose(1, 0, 2), vals.reshape(kv_loc, pre_dev, LANES))
        far_pre = swap(own_pre, 'cp', groups, 2)
        near_pre = swap(own_pre, 'cp', groups, 1)
        wo_z = gather_w_out(w_out, tps)
        cos_tab, sin_tab = rope_tables(q_pos, head_dim)
        q, own_suf, k_flat, v_flat = qkv(x_loc, norm_attn, w_query, w_key, w_value, cos_tab, sin_tab)
        far_suf, = swap((own_suf,), 'cp', groups, 2)
        near_suf, = swap((own_suf,), 'cp', groups, 1)
        o_first, o_last, wo_pieces = attend(q, own_pre, near_pre, far_pre, own_suf, near_suf, far_suf, wo_z, c2, groups, tps, dps)
        x_out = line_block(o_first, o_last, x_loc, w_out, wo_pieces, w_gate, w_up, w_down, norm_mlp)
        return x_out, k_flat.reshape(rows, kv_loc, head_dim), v_flat.reshape(rows, kv_loc, head_dim)

    row_spec = P(('dp', 'cp'), None)
    kv_spec = P(('dp', 'cp'), 'tp', None)
    col_spec = P(None, 'tp')
    row_split = P('tp', None)
    vec_spec = P(None)
    return jax.shard_map(local_layer, mesh=mesh, in_specs=(row_spec, kv_spec, kv_spec, vec_spec, col_spec, col_spec, col_spec, row_split, vec_spec, col_spec, col_spec, row_split), out_specs=(row_spec, kv_spec, kv_spec), check_vma=False)
```

```python
import functools
import math

import jax
import jax.numpy as jnp
from jax import lax
from jax.experimental import pallas as pl
from jax.experimental.pallas import tpu as pltpu
from jax.sharding import PartitionSpec as P


ROPE_THETA = 500000.0
NORM_EPS = 1e-5
ROWS_CH = 128
F32 = jnp.float32
BF16 = jnp.bfloat16
HBM = pl.BlockSpec(memory_space=pl.ANY)
VMEM = pl.BlockSpec(memory_space=pltpu.VMEM)
IN_HBM = pl.BlockSpec(memory_space=pltpu.HBM)
LANES = 128
PAIR = 2 * LANES
NT = (((1,), (1,)), ((), ()))
each = functools.partial(pl.loop, 0)


def tile(i, n):
    return pl.ds(pl.multiple_of(i * n, n), n)


def params(mib, **more):
    return pltpu.CompilerParams(vmem_limit_bytes=mib * 2**20, **more)


def cost(flops, moved):
    return pl.CostEstimate(flops=flops, bytes_accessed=moved, transcendentals=0)


def struct(shape, dtype):
    return jax.ShapeDtypeStruct(shape, dtype)


def block_positions(owner, groups, blk_len, prefix_len):
    local_row = jnp.arange(2 * blk_len, dtype=jnp.int32)
    blk_idx = jnp.where(local_row < blk_len, owner, 2 * groups - 1 - owner)
    return prefix_len + blk_idx * blk_len + local_row % blk_len


def rope_tables(positions, head_dim):
    inv_freq = ROPE_THETA ** (-jnp.arange(0, head_dim, 2, dtype=F32) / head_dim)
    angles = positions.astype(F32)[:, None] * inv_freq[None, :]
    cos_tab, sin_tab = jnp.cos(angles), jnp.sin(angles)
    return jnp.concatenate([cos_tab, cos_tab], axis=1), jnp.concatenate([-sin_tab, sin_tab], axis=1)


def qkv_kernel(x_hbm, g_ref, wq_ref, wk_ref, wv_ref, cos_ref, sin_ref, q_ref, kv_ref, kf_ref, vf_ref, x_ref, h_ref, sems, *, nq):
    step = pl.program_id(0)
    rows = x_ref.shape[0]
    parts, rt = sems.shape[0], 32

    @pl.when(step == 0)
    def _():
        n = rows // parts
        copies = [pltpu.make_async_copy(x_hbm.at[tile(i, n), :], x_ref.at[tile(i, n), :], sems.at[i]) for i in range(parts)]
        for copy in copies:
            copy.start()
        for i, copy in enumerate(copies):
            copy.wait()

            @pl.loop(i * n // rt, (i + 1) * n // rt, unroll=2)
            def _(j):
                sl = tile(j, rt)
                xv = x_ref[sl, :].astype(F32)
                inv = lax.rsqrt(jnp.mean(xv * xv, axis=-1, keepdims=True) + NORM_EPS)
                h_ref[sl, :] = (xv * inv * g_ref[...].astype(F32)).astype(BF16)

    def rope(block, sl):
        return (block * cos_ref[sl, :] + pltpu.roll(block, 64, axis=1) * sin_ref[sl, :]).astype(BF16)

    mt = rows

    def project(w_ref, store):
        @each(rows // mt)
        def _(i):
            sl = tile(i, mt)
            acc = jnp.dot(h_ref[sl, :], w_ref[...], preferred_element_type=F32)
            store(acc, sl)

    def heads_of(acc):
        return [(t, slice(t * LANES, (t + 1) * LANES), acc[:, t * LANES:(t + 1) * LANES]) for t in range(2)]

    def store_q(acc, sl):
        for _, cs, part in heads_of(acc):
            q_ref[sl, cs] = rope(part, sl)

    def store_k(acc, sl):
        for t, cs, part in heads_of(acc):
            kf_ref[sl, cs] = rope(part, sl)
            kv_ref[0, t, sl, :] = kf_ref[sl, cs]

    def store_v(acc, sl):
        vf_ref[sl, :] = acc.astype(BF16)
        for t, _, part in heads_of(acc):
            for b in range(mt // LANES):
                kv_ref[1, t, pl.ds(sl.start + b * LANES, LANES), :] = part[b * LANES:(b + 1) * LANES].T.astype(BF16)

    pl.when(step < nq)(lambda: project(wq_ref, store_q))
    pl.when(step == nq)(lambda: project(wk_ref, store_k))
    pl.when(step == nq + 1)(lambda: project(wv_ref, store_v))


def qkv(x, gain, wq, wk, wv, cos_tab, sin_tab):
    rows, depth = x.shape
    nq = wq.shape[1] // PAIR

    def fixed(shape):
        return pl.BlockSpec(shape, lambda j: tuple(0 for _ in shape))

    def whole(shape):
        return pl.BlockSpec(shape, lambda j: tuple(0 for _ in shape), pipeline_mode=pl.Buffered(1))

    def columns(n):
        return pl.BlockSpec((n, PAIR), lambda j: (0, jnp.minimum(j, nq - 1)))

    flat, by_head = (rows, PAIR), (2, 2, rows, LANES)
    return pl.pallas_call(
        functools.partial(qkv_kernel, nq=nq),
        grid=(nq + 2,),
        in_specs=[HBM, whole((1, depth)), columns(depth), fixed(wk.shape), fixed(wv.shape), whole(cos_tab.shape), whole(sin_tab.shape)],
        out_specs=[columns(rows), fixed(by_head), fixed(flat), fixed(flat)],
        out_shape=[struct(s, BF16) for s in ((rows, nq * PAIR), by_head, flat, flat)],
        scratch_shapes=[pltpu.VMEM((rows, depth), BF16), pltpu.VMEM((rows, depth), BF16), pltpu.SemaphoreType.DMA((4,))],
        compiler_params=params(58, dimension_semantics=("arbitrary",)),
        cost_estimate=cost(2 * rows * depth * (nq + 2) * PAIR, 2 * depth * rows),
        name="qkv",
    )(x, gain.reshape(1, depth), wq, wk, wv, cos_tab, sin_tab)


NQ = 512
PER_KV = 4


class Fetch:
    def __init__(self, sems):
        self.sems, self.used = sems, 0

    def start(self, pairs):
        copies = []
        for src, dst in pairs:
            copies.append(pltpu.make_async_copy(src, dst, self.sems.at[self.used]))
            self.used += 1
        for copy in copies:
            copy.start()
        return copies


def settle(copies):
    for copy in copies:
        copy.wait()


def q_block(q_ref, head, half):
    return q_ref[tile(half, NQ), tile(head, LANES)]


def across(blocks):
    return jnp.concatenate([blocks[i:i + LANES] for i in range(0, blocks.shape[0], LANES)], axis=1)


def attend_items(q_ref, kb_ref, vb_ref, acc_ref, m_ref, l_ref, pbufs, n_items, item, bk, c2, diag=False):
    depth = len(pbufs)

    def scores(i, pb):
        head, half, start = item(i)
        n = head * 2 + half
        ks = kb_ref[head // PER_KV, pl.ds(pl.multiple_of(start, bk), bk), :]
        s = lax.dot_general(ks, q_block(q_ref, head, half), NT, preferred_element_type=F32)
        e = jnp.exp2(s * c2 - m_ref[n])
        if diag:
            seen = lax.broadcasted_iota(jnp.int32, (bk, NQ), 0) <= lax.broadcasted_iota(jnp.int32, (bk, NQ), 1)
            e = jnp.where(seen, e, 0.0)
        pb[...] = e.astype(BF16)
        l_ref[n] += jnp.sum(e.reshape(-1, *l_ref.shape[1:]), axis=0)

    def values(i, pb):
        head, half, start = item(i)
        vt = across(vb_ref[head // PER_KV, pl.ds(pl.multiple_of(start, bk), bk), :])
        acc_ref[head * 2 + half] += jnp.dot(vt, pb[...], preferred_element_type=F32)

    scores(0, pbufs[0])

    def body(g, carry):
        for u in range(depth):
            i = g * depth + u
            scores(i + 1, pbufs[(u + 1) % depth])
            values(i, pbufs[u])
        return carry

    trips = n_items // depth - 1
    lax.fori_loop(0, trips, body, 0)
    for u in range(depth):
        if u + 1 < depth:
            scores(trips * depth + u + 1, pbufs[u + 1])
        values(trips * depth + u, pbufs[u])


def prefix_kernel(q_hbm, ka, va, kb, vb, acc_out, m_out, l_out, q_ref, kbuf, vbuf, acc_ref, m_ref, l_ref, pa, pb, sems, *, heads, c2):
    fetch = Fetch(sems)
    n = ka.shape[1]
    settle(fetch.start([(q_hbm, q_ref), (ka, kbuf.at[:, tile(0, n), :]), (va, vbuf.at[:, tile(0, n), :]), (kb.at[0], kbuf.at[0, tile(1, n), :]), (vb.at[0], vbuf.at[0, tile(1, n), :])]))

    @each(heads // PER_KV)
    def _(group):
        for j in range(2 * PER_KV):
            i = group * 2 * PER_KV + j
            s = lax.dot_general(kbuf[group, tile(0, LANES), :], q_block(q_ref, i // 2, j % 2), NT, preferred_element_type=F32)
            m_ref[i] = jnp.max(s, axis=0, keepdims=True) * c2

    for ref in (acc_ref, l_ref):
        ref[...] = jnp.zeros_like(ref)
    bk = 2 * NQ
    per = n // bk
    pairs = 2 * PER_KV
    whole = pairs * 2 * per

    def item(i):
        j = jnp.maximum(i - whole, 0)
        pair = jnp.where(i < whole, i // (2 * per), pairs + j // per)
        return pair // 2, pair % 2, jnp.where(i < whole, i % (2 * per), j % per) * bk

    attend_items(q_ref, kbuf, vbuf, acc_ref, m_ref, l_ref, (pa, pb), whole + pairs * per, item, bk, c2)
    settle(fetch.start([(acc_ref, acc_out), (m_ref, m_out), (l_ref, l_out)]))


def state_shapes(heads):
    return [struct((heads * 2, n, NQ), F32) for n in (LANES, 1, 8)]


def vmem_like(shapes):
    return [pltpu.VMEM(s.shape, s.dtype) for s in shapes]


def attend_prefix(q, pieces, c2):
    heads = q.shape[1] // LANES
    flat = [a for p in pieces for a in p]
    n = 2 * pieces[0][0].shape[1]
    shapes = state_shapes(heads)
    return pl.pallas_call(
        functools.partial(prefix_kernel, heads=heads, c2=c2),
        in_specs=[HBM] * (1 + len(flat)),
        out_specs=[HBM] * len(shapes),
        out_shape=[pltpu.HBM(s.shape, s.dtype) for s in shapes],
        scratch_shapes=[
            *vmem_like([q]), *[pltpu.VMEM((2, n, LANES), BF16)] * 2, *vmem_like(shapes),
            *[pltpu.VMEM((2 * NQ, NQ), BF16)] * 2, pltpu.SemaphoreType.DMA((8,)),
        ],
        compiler_params=params(58),
        cost_estimate=cost(4 * q.size * n, 4 * q.size),
        name="attend_prefix",
    )(q, *flat)


def rest_kernel(*refs, group, groups, c2, axis):
    q_hbm, *refs = refs
    flat, suf, refs = refs[:2 * groups], refs[2 * groups:3 * groups], refs[3 * groups:]
    pre = list(zip(flat[::2], flat[1::2]))
    acc_in, m_in, l_in, here_out, there_out, q_ref, kbuf, vbuf, ksuf, vsuf, acc_ref, m_ref, l_ref, acc_old, l_old, o_ref, bad_ref, sems, wa, wb, pa, pb, pc, pd = refs
    heads = PER_KV
    me = lax.axis_index(axis)
    fetch = Fetch(sems)
    mine = pl.ds(group * heads * 2, heads * 2)
    n_pre, n_suf = pre[0][0].shape[1], suf[0].shape[2]
    first = fetch.start([(q_hbm.at[:, tile(group, heads * LANES)], q_ref), (m_in.at[mine], m_ref)])
    for i, (kr, vr) in enumerate(pre[2 - group:]):
        first += fetch.start([(kr.at[group], kbuf.at[0, tile(i, n_pre), :]), (vr.at[group], vbuf.at[0, tile(i, n_pre), :])])
    second = []
    for i, kv in enumerate(suf):
        second += fetch.start([(kv.at[j, group], buf.at[0, tile(i, n_suf), :]) for j, buf in enumerate((ksuf, vsuf))])
    third = fetch.start([(acc_in.at[mine], acc_old), (l_in.at[mine], l_old)])
    for ref in (acc_ref, l_ref):
        ref[...] = jnp.zeros_like(ref)
    settle(first)
    bk = 2 * NQ
    per = kbuf.shape[1] // bk

    def pre_item(i):
        pair = i // per
        return pair // 2, pair % 2, (i % per) * bk

    attend_items(q_ref, kbuf, vbuf, acc_ref, m_ref, l_ref, (wa, wb), heads * 2 * per, pre_item, bk, c2)
    settle(second)
    last = 2 * groups - 1

    def locate(blk):
        late = (blk >= groups).astype(jnp.int32)
        owner = jnp.where(blk < groups, blk, last - blk)
        diff = (owner % 2 != me % 2).astype(jnp.int32) + 2 * (owner // 2 != me // 2).astype(jnp.int32)
        return (diff * 2 + late) * NQ

    def full_item(i):
        head, r = i // last, i % last
        half = (r >= me).astype(jnp.int32)
        return head, half, locate(jnp.where(r < me, r, r - me))

    def diag_item(i):
        half = i % 2
        return i // 2, half, locate(jnp.where(half == 0, me, last - me))

    attend_items(q_ref, ksuf, vsuf, acc_ref, m_ref, l_ref, (pa, pb, pc, pd), heads * last, full_item, NQ, c2)
    attend_items(q_ref, ksuf, vsuf, acc_ref, m_ref, l_ref, (pa, pb), heads * 2, diag_item, NQ, c2, diag=True)
    settle(third)
    bad_ref[...] = jnp.zeros_like(bad_ref)
    chunk = ROWS_CH // 2

    def write(head, half, acc, total):
        out = (acc * (1.0 / total)).T.astype(BF16)
        n_p = NQ // chunk
        for p in range(n_p):
            o_ref[p % 2, tile(half * (n_p // 2) + p // 2, chunk), tile(head, LANES)] = out[p * chunk:(p + 1) * chunk]

    @each(heads)
    def _(head):
        for half in range(2):
            i = head * 2 + half
            acc = acc_ref[i] + acc_old[i]
            total = jnp.sum(l_ref[i] + l_old[i], axis=0, keepdims=True)
            bad = jnp.where((jnp.abs(acc) < jnp.inf) & (total < jnp.inf), 0.0, 1.0)
            for j in range(NQ // LANES):
                part = bad[:, j * LANES:(j + 1) * LANES]
                bad_ref[...] = jnp.maximum(bad_ref[...], jnp.max(part.reshape(-1, *bad_ref.shape), axis=0))
            write(head, half, acc, total)

    @pl.when(jnp.max(bad_ref[...]) > 0.0)
    def _():
        @each(heads * 2)
        def _(i):
            head, half = i // 2, i % 2
            q = q_block(q_ref, head, half)
            m_ref[i] = jnp.full((1, NQ), -jnp.inf, F32)
            for ref in (acc_ref, l_ref):
                ref[i] = jnp.zeros(ref.shape[1:], F32)

            def update(ks, vt, seen):
                s = lax.dot_general(ks, q, NT, preferred_element_type=F32) * c2
                if seen is not None:
                    s = jnp.where(seen, s, -jnp.inf)
                m_old = m_ref[i]
                m_new = jnp.maximum(m_old, jnp.max(s, axis=0, keepdims=True))
                alpha = jnp.exp2(m_old - m_new)
                e = jnp.exp2(s - m_new)
                m_ref[i] = m_new
                l_ref[i] = l_ref[i] * alpha + jnp.sum(e.reshape(-1, *l_ref.shape[1:]), axis=0)
                acc_ref[i] = acc_ref[i] * alpha + jnp.dot(vt, e.astype(BF16), preferred_element_type=F32)

            kpre, vpre = (p.at[:, tile(0, LANES)] for p in (pa, pb))
            for kr, vr in pre:
                @each(n_pre // NQ)
                def _(j):
                    pltpu.sync_copy(kr.at[group, tile(j, NQ), :], kpre)
                    pltpu.sync_copy(vr.at[group, tile(j, NQ), :], vpre)
                    update(kpre[...], across(vpre[...]), None)

            mine_blk = jnp.where(half == 0, me, last - me)

            @each(2 * groups)
            def _(blk):
                @pl.when(blk <= mine_blk)
                def _():
                    start = pl.ds(pl.multiple_of(locate(blk), NQ), NQ)
                    seen = (lax.broadcasted_iota(jnp.int32, (NQ, NQ), 0) <= lax.broadcasted_iota(jnp.int32, (NQ, NQ), 1)) | (blk < mine_blk)
                    update(ksuf[0, start, :], across(vsuf[0, start, :]), seen)

            write(head, half, acc_ref[i], jnp.sum(l_ref[i], axis=0, keepdims=True))

    side = lax.axis_index('tp') // 2
    settle(fetch.start([(o_ref.at[side], here_out), (o_ref.at[1 - side], there_out)]))


def attend_rest(q, pre, suf, state, c2, axis, group):
    rows, groups, width = q.shape[0], len(suf), PER_KV * LANES
    n_pre, n_suf = (2 + group) * pre[0][0].shape[1], groups * suf[0].shape[2]
    flat = [a for p in pre for a in p] + list(suf)
    acc, m, total = state_shapes(PER_KV)
    out = pltpu.HBM((rows // 2, width), BF16)
    return pl.pallas_call(
        functools.partial(rest_kernel, group=group, groups=groups, c2=c2, axis=axis),
        in_specs=[IN_HBM] + [HBM] * len(flat) + [IN_HBM] * 3,
        out_specs=[HBM] * 2,
        out_shape=[out] * 2,
        scratch_shapes=[
            pltpu.VMEM((rows, width), BF16), *[pltpu.VMEM((1, n, LANES), BF16) for n in (n_pre, n_pre, n_suf, n_suf)], *vmem_like([acc, m, total, acc, total, struct((2, rows // 2, width), BF16)]),
            pltpu.VMEM((8, LANES), F32), pltpu.SemaphoreType.DMA((22,)), *[pltpu.VMEM((2 * NQ, NQ), BF16)] * 2, *[pltpu.VMEM((NQ, NQ), BF16)] * 4,
        ],
        compiler_params=params(42),
        cost_estimate=cost(2 * rows * width * (2 * n_pre + n_suf), 4 * q.size),
        name="attend_rest",
    )(q, *flat, *state)


def swap(arrays, axis, groups, bit):
    return tuple(lax.ppermute(a, axis, [(i, i ^ bit) for i in range(groups)]) for a in arrays)


def attend(q, own_pre, near_pre, far_pre, own_suf, near_suf, far_suf, wo_z, c2, groups, tps, dps):
    state = attend_prefix(q, (own_pre, near_pre), c2)
    far_pre, far_suf, wo_z, state = lax.optimization_barrier((far_pre, far_suf, wo_z, state))
    cross_pre = swap(far_pre, 'cp', groups, 1)
    cross_suf, = swap((far_suf,), 'cp', groups, 1)
    wo = jnp.stack(wo_z)
    wo_x, = swap((wo,), 'dp', dps, 1)
    wo_y, = swap((wo,), 'cp', groups, 2)
    pre, suf = (own_pre, near_pre, far_pre, cross_pre), (own_suf, near_suf, far_suf, cross_suf)
    here, there = attend_rest(q, pre, suf, state, c2, 'cp', 0)
    o_far = tuple(lax.ppermute(there, 'tp', [(i, i ^ d) for i in range(tps)]) for d in (2, 3))
    o_mate = swap((here,), 'tp', tps, 1)
    wo, wo_x, wo_y, there, q = lax.optimization_barrier((wo, wo_x, wo_y, there, q))
    wo_xy, = swap((wo_x,), 'cp', groups, 2)
    near = swap((wo, wo_x, wo_y), 'cp', groups, 1)
    o_last = attend_rest(q, pre, suf, state, c2, 'cp', 1)
    wo_xy, o_last = lax.optimization_barrier((wo_xy, o_last))
    return (here,) + o_mate + o_far, o_last, (wo, wo_x, wo_y, wo_xy) + near + swap((wo_xy,), 'cp', groups, 1)


MESH = pl.DeviceIdType.MESH
DOT_N = 512
SLOTS = 3
MID_PLAN = ((('r3', -1),), (('xc', -3), ('r2', -1), ('hb', 1), ('ha', 1),), (('xb', -2), ('xa', -2),), (('O', 3),), (('r4', -1),), (), (('hc', 1), ('r1', 0),))
END_PLAN = ((('hw', 0), ('f', -2),), (('O', 3),), (), (), (), (), ())
AHEAD, BEHIND = 3, 3


def side_of(z):
    return lax.div(z, 2)


def colhalf_of(z):
    return lax.rem(lax.div(z + 1, 2), 2)


def line_kernel(*refs, nc):
    o_first, o_last, x_ref, wo_ref, *refs = refs[:4], refs[4:6], *refs[6:]
    wo_pieces, refs = refs[:8], refs[8:]
    wg_ref, wu_ref, wd_ref, gain_ref, xout_ref, land_ref = refs[:6]
    (obuf, h2, ybuf, ring, psum, act, stage, xs, sstat, rstat,
     ring_sem, loc_sem, o_send, o_recv, st_send, st_recv, a1_send, a1_recv, rs_send, rs_recv, a2_send, a2_recv) = refs[6:]
    R, H = ROWS_CH, ROWS_CH // 2
    depth = wg_ref.shape[0]
    ff = wg_ref.shape[1]
    half = depth // 2
    width = o_last[0].shape[-1]
    kz = 2 * width
    n_ct = half // DOT_N
    nd, ne = ff // PAIR, depth // DOT_N
    per = 4 + nd + ne
    total_loads = nc * per
    big = 1024

    z = lax.axis_index('tp')
    dp = lax.axis_index('dp')
    cp = lax.axis_index('cp')
    core, chip = lax.rem(cp, 2), lax.div(cp, 2)
    side, q = side_of(z), colhalf_of(z)
    is_mid = q == 1
    is_end = q != 1
    near = 1 + side
    outer = 3 * side
    inner = 2 - side
    far_end = 3 - 3 * side
    peers = {1: z + 1 - 2 * lax.rem(z, 2), 2: lax.rem(z + 2, 4), 3: 3 - z}
    mate = peers[1]

    def rdma(src, dst, ssem, rsem, dev):
        return pltpu.make_async_remote_copy(src_ref=src, dst_ref=dst, send_sem=ssem, recv_sem=rsem, device_id={'tp': dev}, device_id_type=MESH)

    def rows_at(zz):
        return tile(side_of(zz), H)

    def cols_at(zz):
        return tile(colhalf_of(zz), half)

    barrier = pltpu.get_barrier_semaphore()
    for d in (1, 2, 3):
        pl.semaphore_signal(barrier, inc=1, device_id={'tp': peers[d]}, device_id_type=MESH)
    pl.semaphore_wait(barrier, 3)

    def load_kind(ld):
        u = ld + (per - 4)
        i1 = lax.div(u, per)
        a = lax.div(i1 + big - 1, big)
        t = lax.rem(u, per) + 4 * lax.div(i1, nc)
        return a * t + (1 - a) * ld

    def issue(ld):
        slot = lax.rem(ld, SLOTS)
        sem = ring_sem.at[slot]
        t = load_kind(ld)

        def start(src, dst):
            pltpu.make_async_copy(src, dst, sem).start()

        for d in range(4):
            @pl.when(t == d)
            def _():
                @each(n_ct)
                def _(ct):
                    c0 = pl.multiple_of(ct * DOT_N, DOT_N)
                    if d == 0:
                        cs = tile(q * n_ct + ct, DOT_N)
                        start(wo_ref.at[:, cs], ring.at[slot, tile(ct, kz), :])
                    else:
                        for k, piece in enumerate(wo_pieces):
                            bits = (dp, k % 2), (chip, k // 2 % 2), (core, k // 4)
                            n = piece.shape[1]
                            j = sum((own + x - 2 * own * x) * w for (own, x), w in zip(bits, (4, 2, 1)))
                            r0 = pl.multiple_of(ct * kz + j * n, n)
                            start(piece.at[d - 1, :, pl.ds(c0, DOT_N)], ring.at[slot, pl.ds(r0, n), :])

        @pl.when((t >= 4) & (t < 4 + nd))
        def _():
            cs = pl.ds(pl.multiple_of((t - 4) * 256, 256), 256)
            start(wg_ref.at[:, cs], ring.at[slot, :depth, :PAIR])
            start(wu_ref.at[:, cs], ring.at[slot, :depth, PAIR:])

        @pl.when(t >= 4 + nd)
        def _():
            cs = pl.ds(pl.multiple_of((t - 4 - nd) * DOT_N, DOT_N), DOT_N)
            start(wd_ref.at[:, cs], ring.at[slot, :ff, :])

    def take(ld, n_rows):
        slot = lax.rem(ld, SLOTS)
        whole = ring.at[slot, :n_rows, :]
        pltpu.make_async_copy(whole, whole, ring_sem.at[slot]).wait()
        pl.when(ld + SLOTS - 1 < total_loads)(lambda: issue(ld + SLOTS - 1))
        return slot

    def late(c, d):
        return obuf.at[c, d, :, tile(1, width)]

    def o_copy(c, d):
        return rdma(o_last[int(d > 1)].at[tile(c, H), :], late(c, d), o_send.at[c, d - 1], o_recv.at[c, d - 1], peers[d])

    def o_start(c):
        for d in (1, 2, 3):
            o_copy(c, d).start()

    def project(c, ld0):
        own_o = pltpu.make_async_copy(o_last[0].at[tile(c, H), :], late(c, 0), loc_sem.at[0])
        own_x = pltpu.make_async_copy(x_ref.at[tile(c * 2 + side, H), cols_at(z)], xs, loc_sem.at[1])
        own_o.start()
        own_x.start()
        for d in (1, 2, 3):
            o_copy(c, d).wait_recv()
        own_o.wait()
        own_x.wait()

        @each(n_ct)
        def _(ct):
            cs = tile(ct, DOT_N)
            ybuf[c, :, cs] = xs[:, cs].astype(F32)

        @each(4)
        def _(d):
            slot = take(ld0 + d, n_ct * kz)

            @each(n_ct)
            def _(ct):
                cs = tile(ct, DOT_N)
                w = ring[slot, tile(ct, kz), :]
                ybuf[c, :, cs] += jnp.dot(obuf[c, d], w, preferred_element_type=F32)

        sstat[c] = jnp.zeros((H, LANES), F32)

        @each(n_ct)
        def _(ct):
            yv = ybuf[c, :, tile(ct, DOT_N)]
            sstat[c] += jnp.broadcast_to(jnp.sum(yv * yv, axis=-1, keepdims=True), (H, LANES))

        swap_stat = rdma(sstat.at[c], rstat.at[c], st_send.at[c, 0], st_recv.at[c, 0], mate)
        swap_stat.start()
        swap_stat.wait_recv()
        inv = lax.rsqrt((sstat[c] + rstat[c])[:, 0:1] * (1.0 / depth) + NORM_EPS)

        @each(n_ct)
        def _(ct):
            cs = tile(ct, DOT_N)
            gs = tile(q * n_ct + ct, DOT_N)
            h2[c, rows_at(z), gs] = (ybuf[c, :, cs] * inv * gain_ref[:, gs].astype(F32)).astype(BF16)

    class Spread:
        def __init__(self, block, send, recv):
            self.block, self.send, self.recv = block, send, recv

        def copy(self, c, zz, s, r, dev):
            return rdma(self.block(c, zz), self.block(c, zz), self.send.at[c, s], self.recv.at[c, r], dev)

        def to_near(self, c):
            return self.copy(c, z, 0, 0, near)

        def to_outer(self, c):
            return self.copy(c, z, 0, 0, outer)

        def to_inner(self, c):
            return self.copy(c, z, 1, 1, inner)

        def end_to_inner(self, c):
            return self.copy(c, outer, 2, 2, inner)

        def inner_to_outer(self, c):
            return self.copy(c, inner, 3, 1, outer)

        def far_to_outer(self, c):
            return self.copy(c, far_end, 4, 2, outer)

        def start(self, c):
            pl.when(is_end)(lambda: self.to_near(c).start())

            @pl.when(is_mid)
            def _():
                self.to_outer(c).start()
                self.to_inner(c).start()

        def wait(self, c, r):
            self.copy(c, z, 0, r, mate).wait_recv()

        def serve(self, r, c):
            self.wait(c, r)
            (self.end_to_inner, self.inner_to_outer, self.far_to_outer)[r](c).start()

        def drain(self, c):
            @pl.when(is_end)
            def _():
                self.to_near(c).wait_send()

            @pl.when(is_mid)
            def _():
                for copy in (self.to_outer(c), self.to_inner(c), self.end_to_inner(c), self.inner_to_outer(c), self.far_to_outer(c)):
                    copy.wait_send()

    hidden = Spread(lambda c, zz: h2.at[c, rows_at(zz), cols_at(zz)], a1_send, a1_recv)

    done = Spread(lambda c, zz: xout_ref.at[tile(c * 2 + side_of(zz), H), cols_at(zz)], a2_send, a2_recv)

    def gate_up(c, ld0, active, after):
        @each(nd)
        def _(i):
            @pl.when(active)
            def _():
                slot = take(ld0 + i, depth)
                gu = jnp.dot(h2[c], ring[slot, :depth, :], preferred_element_type=F32)
                g, u = gu[:, :PAIR], gu[:, PAIR:]
                act[:, tile(i, PAIR)] = (g * (1.0 / (1.0 + jnp.exp(-g))) * u).astype(BF16)

            for k in range(4):
                pl.when(i == (k + 1) * nd // 4 - 1)(functools.partial(after, k + 1))

    def ps_copy(c, k_send, zz, k_recv, dev):
        return rdma(psum.at[lax.rem(c, 2), zz], land_ref.at[c, k_recv], rs_send.at[c, k_send], rs_recv.at[c, k_recv], dev)

    def sums_out(c):
        ends = (ps_copy(c, 0, far_end, 0, near), ps_copy(c, 1, inner, 2, near), ps_copy(c, 2, near, 3, near))
        mids = (ps_copy(c, 0, far_end, 1, inner), ps_copy(c, 1, outer, 0, outer), ps_copy(c, 2, inner, 4, inner))
        return ends, mids

    def wait_sums_out(c):
        ends, mids = sums_out(c)
        for flag, copies in ((is_end, ends), (is_mid, mids)):
            @pl.when(flag)
            def _():
                for copy in copies:
                    copy.wait_send()

    def down(c, ld0, part):
        ps = lax.rem(c, 2)
        ends, _ = sums_out(c)
        if part == 0:
            pl.when(c >= 2)(lambda: wait_sums_out(c - 2))

        @each(ne // 2)
        def _(i):
            slot = take(ld0 + part * (ne // 2) + i, ff)
            pv = jnp.dot(act[...], ring[slot, :ff, :], preferred_element_type=F32)
            cs = tile(i, DOT_N)
            psum[ps, part, :, cs] = pv[:H]
            psum[ps, 3 - part, :, cs] = pv[H:R]

        @pl.when(is_end)
        def _():
            for copy in (ends[:1], ends[1:])[part]:
                copy.start()

    def arrive(c, k, buf):
        ps_copy(c, 0, z, k, mate).wait_recv()
        copy = pltpu.make_async_copy(land_ref.at[c, k], stage.at[buf], loc_sem.at[2 + buf])
        copy.start()
        return copy

    def tiles(fn):
        @each(4)
        def _(i):
            fn(tile(i, H // 4))

    def pass_on(c, k, zz, send):
        arrive(c, k, 0).wait()

        def add(rs):
            psum[lax.rem(c, 2), zz, rs, :] += stage[0, rs, :]

        tiles(add)
        send.start()

    def finish(c, ks):
        for copy in [arrive(c, k, i) for i, k in enumerate(ks)]:
            copy.wait()

        def add(rs):
            v = psum[lax.rem(c, 2), z, rs, :] + stage[0, rs, :]
            if len(ks) == 2:
                v = v + stage[1, rs, :]
            r0 = pl.multiple_of((c * 2 + side) * H + rs.start, rs.size)
            xout_ref[pl.ds(r0, rs.size), cols_at(z)] = (ybuf[c, rs, :] + v).astype(BF16)

        tiles(add)
        done.start(c)

    def relay(k, c):
        pass_on(c, k, (far_end, outer, inner)[k], sums_out(c)[1][k])

    def hidden_wait(c):
        for r in range(3):
            hidden.wait(c, r)

    steps = {'O': o_start, 'hw': hidden_wait, 'f': lambda c: finish(c, (0,)), 'r4': lambda c: finish(c, (3, 4))}
    for r in range(3):
        steps['h' + 'abc'[r]] = functools.partial(hidden.serve, r)
        steps['x' + 'abc'[r]] = functools.partial(done.serve, r)
        steps['r' + '123'[r]] = functools.partial(relay, r)

    early = [pltpu.make_async_copy(src, obuf.at[:, d, :, tile(0, width)], loc_sem.at[5 + d]) for d, src in enumerate(o_first)]
    for copy in early:
        copy.start()
    each(SLOTS - 1)(issue)
    for copy in early:
        copy.wait()

    @each(AHEAD + nc + BEHIND)
    def _(t):
        j = t - AHEAD
        jj = j + 1
        active = (j >= 0) & (j < nc)

        def after(k):
            for flag, plan in ((is_mid, MID_PLAN[k]), (is_end, END_PLAN[k])):
                def run(plan=plan):
                    for name, ahead in plan:
                        c = j + ahead
                        pl.when((c >= 0) & (c < nc))(functools.partial(steps[name], c))

                if plan:
                    pl.when(flag)(run)

        @pl.when((jj >= 0) & (jj < nc))
        def _():
            project(jj, per * jj - (per - 4) * lax.div(jj + big - 1, big))
            hidden.start(jj)

        after(0)
        ld_d = per * jj - (per - 8) - 4 * lax.div(jj, nc)
        gate_up(j, ld_d, active, after)
        for part in range(2):
            pl.when(active)(lambda: down(j, ld_d + nd, part))
            after(5 + part)

    @each(nc)
    def _(c):
        @pl.when(is_end)
        def _():
            for r in range(3):
                done.wait(c, r)

        for d in (1, 2, 3):
            o_copy(c, d).wait_send()
        rdma(sstat.at[c], rstat.at[c], st_send.at[c, 0], st_recv.at[c, 0], mate).wait_send()
        hidden.drain(c)
        done.drain(c)
        pl.when(c >= nc - 2)(lambda: wait_sums_out(c))


def line_block(o_first, o_last, x, w_out, pieces, w_gate, w_up, w_down, gain):
    rows, depth = x.shape
    ff = w_gate.shape[1]
    width = o_last[0].shape[-1]
    kz = 2 * width
    nc = rows // ROWS_CH
    h, half = ROWS_CH // 2, depth // 2
    ring_rows = max(depth, ff, half // DOT_N * kz)
    sems = [pltpu.SemaphoreType.DMA((nc, n)) for n in (3, 3, 1, 1, 5, 3, 3, 5, 5, 3)]
    xout, _ = pl.pallas_call(
        functools.partial(line_kernel, nc=nc),
        in_specs=[HBM] * (11 + len(pieces)) + [VMEM],
        out_specs=[VMEM, HBM],
        out_shape=[pltpu.VMEM(x.shape, BF16), struct((nc, 5, h, half), F32)],
        scratch_shapes=[
            pltpu.VMEM((nc, 4, h, kz), BF16), pltpu.VMEM((nc, ROWS_CH, depth), BF16), pltpu.VMEM((nc, h, half), F32),
            pltpu.VMEM((SLOTS, ring_rows, DOT_N), BF16), pltpu.VMEM((2, 4, h, half), F32), pltpu.VMEM((ROWS_CH, ff), BF16),
            pltpu.VMEM((2, h, half), F32), pltpu.VMEM((h, half), BF16),
            *[pltpu.VMEM((nc, h, LANES), F32)] * 2, pltpu.SemaphoreType.DMA((SLOTS,)), pltpu.SemaphoreType.DMA((9,)), *sems,
        ],
        compiler_params=params(50, collective_id=1, has_side_effects=True),
        cost_estimate=cost(6 * x.size * ff, 2 * x.size),
        name="line_block",
    )(*(a.reshape(nc, h, width) for a in o_first), *o_last, x, w_out, *pieces, w_gate, w_up, w_down, gain.reshape(1, depth))
    return xout


def gather_w_out(w_out, tps):
    z, dp, cp = (lax.axis_index(a) for a in ('tp', 'dp', 'cp'))
    n, half = w_out.shape[0] // 8, w_out.shape[1] // 2
    q = (z + 1) // 2 % 2
    part = lax.dynamic_slice_in_dim(w_out, (dp * 4 + cp) * n, n, 0)
    same, other = (lax.dynamic_slice_in_dim(part, h * half, half, 1) for h in (q, 1 - q))
    return tuple(lax.ppermute(a, 'tp', [(i, i ^ d) for i in range(tps)]) for d, a in ((1, other), (2, other), (3, same)))


def solution(mesh):
    groups = mesh.shape['cp']
    tps = mesh.shape['tp']
    dps = mesh.shape['dp']

    def local_layer(x_loc, kp_loc, vp_loc, norm_attn, w_query, w_key, w_value, w_out, norm_mlp, w_gate, w_up, w_down):
        rows = x_loc.shape[0]
        pre_dev, kv_loc, head_dim = kp_loc.shape
        c2 = head_dim ** -0.5 * math.log2(math.e)
        me = lax.axis_index('cp')
        q_pos = block_positions(me, groups, rows // 2, pre_dev * groups)
        vals = vp_loc.reshape(pre_dev // LANES, LANES, kv_loc, head_dim).transpose(2, 0, 3, 1)
        own_pre = (kp_loc.transpose(1, 0, 2), vals.reshape(kv_loc, pre_dev, LANES))
        far_pre = swap(own_pre, 'cp', groups, 2)
        near_pre = swap(own_pre, 'cp', groups, 1)
        wo_z = gather_w_out(w_out, tps)
        cos_tab, sin_tab = rope_tables(q_pos, head_dim)
        q, own_suf, k_flat, v_flat = qkv(x_loc, norm_attn, w_query, w_key, w_value, cos_tab, sin_tab)
        far_suf, = swap((own_suf,), 'cp', groups, 2)
        near_suf, = swap((own_suf,), 'cp', groups, 1)
        o_first, o_last, wo_pieces = attend(q, own_pre, near_pre, far_pre, own_suf, near_suf, far_suf, wo_z, c2, groups, tps, dps)
        x_out = line_block(o_first, o_last, x_loc, w_out, wo_pieces, w_gate, w_up, w_down, norm_mlp)
        return x_out, k_flat.reshape(rows, kv_loc, head_dim), v_flat.reshape(rows, kv_loc, head_dim)

    row_spec = P(('dp', 'cp'), None)
    kv_spec = P(('dp', 'cp'), 'tp', None)
    col_spec = P(None, 'tp')
    row_split = P('tp', None)
    vec_spec = P(None)
    return jax.shard_map(local_layer, mesh=mesh, in_specs=(row_spec, kv_spec, kv_spec, vec_spec, col_spec, col_spec, col_spec, row_split, vec_spec, col_spec, col_spec, row_split), out_specs=(row_spec, kv_spec, kv_spec), check_vma=False)
```
